16 devices in a mesh: ep: 4 (over z, y), dp: 4 (over x, core).
Axes of the slice: x: 2, y: 2, z: 2, core: 2. Of those that a mesh axis runs over, the one named last changes fastest.
Arguments:
- tokens: bfloat16 [8192, 384], P(('dp', 'ep'))
- dy_out: bfloat16 [8192, 384], P(('dp', 'ep'))
- dense_w1: bfloat16 [384, 384], replicated
- route_idx1: int32 [8192, 4], P(('dp', 'ep'))
- route_gate1: float32 [8192, 4], P(('dp', 'ep'))
- w_gate1: bfloat16 [16, 384, 672], P('ep')
- w_up1: bfloat16 [16, 384, 672], P('ep')
- w_down1: bfloat16 [16, 672, 384], P('ep')
- dense_w2: bfloat16 [384, 384], replicated
- route_idx2: int32 [8192, 4], P(('dp', 'ep'))
- route_gate2: float32 [8192, 4], P(('dp', 'ep'))
- w_gate2: bfloat16 [16, 384, 672], P('ep')
- w_up2: bfloat16 [16, 384, 672], P('ep')
- w_down2: bfloat16 [16, 672, 384], P('ep')
Outputs:
- output 1: bfloat16 [8192, 384], P(('dp', 'ep'))
- output 2: bfloat16 [384, 384], P(('dp', 'ep'))
- output 3: bfloat16 [16, 384, 672], P('ep', 'dp')
- output 4: bfloat16 [16, 384, 672], P('ep', 'dp')
- output 5: bfloat16 [16, 672, 384], P('ep', None, 'dp')
- output 6: bfloat16 [384, 384], P(('dp', 'ep'))
- output 7: bfloat16 [16, 384, 672], P('ep', 'dp')
- output 8: bfloat16 [16, 384, 672], P('ep', 'dp')
- output 9: bfloat16 [16, 672, 384], P('ep', None, 'dp')
All inputs are finite; a program needn't handle non-finite values.
Results may differ from the reference program's by a relative error of at most 0.02.
Values are sent between devices in bfloat16 or wider.
A program may use at most 1 GiB of HBM per device.

```python
import jax
import jax.numpy as jnp

TOK = 512
D = 384
FF = 672
EXPERTS = 16
TOP = 4
SOURCES = 16
BASE = TOK * TOP // EXPERTS
CAPACITY = 2 * BASE


def draw_routing(key):
    key_tok, key_exp, key_shift = jax.random.split(key, 3)
    tok_order = jax.vmap(lambda src_key: jax.random.permutation(src_key, TOK))(jax.random.split(key_tok, SOURCES))
    exp_order = jax.vmap(lambda src_key: jax.random.permutation(src_key, EXPERTS))(jax.random.split(key_exp, SOURCES))
    shift = jax.random.randint(key_shift, (SOURCES, EXPERTS // 2), 0, BASE // 2 + 1, dtype=jnp.int32)
    shift = shift.at[:, 0].set(BASE)
    sizes = jnp.stack([BASE + shift, BASE - shift], axis=2).reshape(SOURCES, EXPERTS)
    block_end = jnp.cumsum(sizes, axis=1, dtype=jnp.int32)
    place = jnp.arange(TOP, dtype=jnp.int32)[None, None, :] * TOK + tok_order[:, :, None].astype(jnp.int32)
    block = jax.vmap(lambda end_row, place_row: jnp.searchsorted(end_row, place_row, side='right'))(block_end, place)
    expert = jnp.take_along_axis(exp_order, block.reshape(SOURCES, TOK * TOP), axis=1)
    return expert.reshape(SOURCES * TOK, TOP).astype(jnp.int32)


def setup_inputs(seed: int = 0) -> dict:
    keys = jax.random.split(jax.random.key(seed), 14)
    n_all = SOURCES * TOK

    def normal(key, shape, scale):
        return (scale * jax.random.normal(key, shape, jnp.float32)).astype(jnp.bfloat16)

    def gates(key):
        return jax.random.uniform(key, (n_all, TOP), jnp.float32, 0.5, 1.5) * TOP ** -0.5

    return {
        'tokens': normal(keys[0], (n_all, D), 1.0),
        'dy_out': normal(keys[1], (n_all, D), 1.0),
        'dense_w1': normal(keys[2], (D, D), 0.5 * D ** -0.5),
        'route_idx1': draw_routing(keys[3]),
        'route_gate1': gates(keys[4]),
        'w_gate1': normal(keys[5], (EXPERTS, D, FF), D ** -0.5),
        'w_up1': normal(keys[6], (EXPERTS, D, FF), D ** -0.5),
        'w_down1': normal(keys[7], (EXPERTS, FF, D), FF ** -0.5),
        'dense_w2': normal(keys[8], (D, D), 0.5 * D ** -0.5),
        'route_idx2': draw_routing(keys[9]),
        'route_gate2': gates(keys[10]),
        'w_gate2': normal(keys[11], (EXPERTS, D, FF), D ** -0.5),
        'w_up2': normal(keys[12], (EXPERTS, D, FF), D ** -0.5),
        'w_down2': normal(keys[13], (EXPERTS, FF, D), FF ** -0.5),
    }


def group_rows(route_idx, n_rows):
    flat_exp = route_idx.reshape(-1)
    n_copies = flat_exp.shape[0]
    order = jnp.argsort(flat_exp, stable=True).astype(jnp.int32)
    sorted_exp = jnp.take(flat_exp, order)
    counts = jnp.zeros((EXPERTS,), jnp.int32).at[flat_exp].add(1)
    starts = jnp.cumsum(counts, dtype=jnp.int32) - counts
    dest_row = (sorted_exp * n_rows + jnp.arange(n_copies, dtype=jnp.int32) - jnp.take(starts, sorted_exp)).astype(jnp.int32)
    return jnp.zeros((n_copies,), jnp.int32).at[order].set(dest_row).reshape(route_idx.shape)


def moe_layer(x_tok, dense_w, route_idx, route_gate, w_gate, w_up, w_down):
    n_all = x_tok.shape[0]
    n_rows = SOURCES * CAPACITY
    x_wide = x_tok.astype(jnp.float32)
    mixed = (x_wide + jnp.dot(x_wide, dense_w.astype(jnp.float32), preferred_element_type=jnp.float32)).astype(jnp.bfloat16)
    flat_pos = group_rows(route_idx, n_rows)
    tok_ids = jnp.broadcast_to(jnp.arange(n_all, dtype=jnp.int32)[:, None], route_idx.shape)
    row_tok = jnp.full((EXPERTS * n_rows,), n_all, jnp.int32).at[flat_pos.reshape(-1)].set(tok_ids.reshape(-1))
    buffer = jnp.take(mixed, row_tok, axis=0, mode='fill', fill_value=0).reshape(EXPERTS, n_rows, D).astype(jnp.float32)
    a_pre = jnp.einsum('erd,edf->erf', buffer, w_gate.astype(jnp.float32))
    b_pre = jnp.einsum('erd,edf->erf', buffer, w_up.astype(jnp.float32))
    hidden = (jax.nn.silu(a_pre) * b_pre).astype(jnp.bfloat16)
    expert_out = jnp.einsum('erf,efd->erd', hidden.astype(jnp.float32), w_down.astype(jnp.float32)).astype(jnp.bfloat16)
    picked = jnp.take(expert_out.reshape(EXPERTS * n_rows, D), flat_pos, axis=0).astype(jnp.float32)
    return (mixed.astype(jnp.float32) + jnp.sum(route_gate[:, :, None] * picked, axis=1)).astype(jnp.bfloat16)


def reference(tokens, dy_out, dense_w1, route_idx1, route_gate1, w_gate1, w_up1, w_down1, dense_w2, route_idx2, route_gate2, w_gate2, w_up2, w_down2):
    def forward(x_tok, dense_a, gate_a, up_a, down_a, dense_b, gate_b, up_b, down_b):
        mid_tok = moe_layer(x_tok, dense_a, route_idx1, route_gate1, gate_a, up_a, down_a)
        return moe_layer(mid_tok, dense_b, route_idx2, route_gate2, gate_b, up_b, down_b)

    y_out, pullback = jax.vjp(forward, tokens, dense_w1, w_gate1, w_up1, w_down1, dense_w2, w_gate2, w_up2, w_down2)
    (grad_tok, grad_dense1, grad_gate1, grad_up1, grad_down1, grad_dense2, grad_gate2, grad_up2, grad_down2) = pullback(dy_out)
    return (grad_tok, grad_dense1, grad_gate1, grad_up1, grad_down1, grad_dense2, grad_gate2, grad_up2, grad_down2)
```

```python
import functools

import jax
import jax.numpy as jnp
from jax import lax
from jax.experimental import pallas as pl
from jax.experimental.pallas import tpu as pltpu
from jax.sharding import PartitionSpec as P

BF16 = jnp.bfloat16
F32 = jnp.float32
N_EP = 4
N_LOC = 4
TOK = 512
D = 384
FF = 672
CAP = 256
SLOTS = 5 * CAP
VMEM = pl.BlockSpec(memory_space=pltpu.VMEM)
SMEM = pl.BlockSpec(memory_space=pltpu.SMEM)


def mm(a, b, dims=((1,), (0,))):
    return lax.dot_general(a, b, (dims, ((), ())), preferred_element_type=F32)


def route_kernel(pack_ref, rank_ref, gate_ref, off_ref):
    me = lax.axis_index('ep')
    before = (lax.broadcasted_iota(jnp.int32, (TOK, TOK), 0) < lax.broadcasted_iota(jnp.int32, (TOK, TOK), 1)).astype(BF16)
    for layer in range(2):
        running = [jnp.int32(0)] * N_LOC
        last = [jnp.int32(0)] * N_LOC
        for src in range(N_EP):
            ids = pack_ref[src, 4 * layer:4 * layer + 4, :]
            gates = pack_ref[src, 8 + 4 * layer:12 + 4 * layer, :]
            member, gate = [], []
            for exp in range(N_LOC):
                match = ids == (me * N_LOC + exp).astype(F32)
                member.append(jnp.sum(match.astype(F32), axis=0, keepdims=True))
                gate.append(jnp.sum(jnp.where(match, gates, 0.0), axis=0, keepdims=True))
            member = jnp.concatenate(member, axis=0)
            gate = jnp.concatenate(gate + [jnp.zeros((4, TOK), F32)], axis=0)
            rank = mm(member.astype(BF16), before)
            rank = jnp.where(member > 0.5, rank, -1.0).astype(jnp.int32)
            rank_ref[layer, src, 0:4, :] = rank
            gate_ref[layer, src * TOK:(src + 1) * TOK, :] = jnp.transpose(gate)
            for exp in range(N_LOC):
                count = jnp.max(rank[exp:exp + 1, :]) + 1
                off_ref[layer * N_LOC + exp, src] = running[exp]
                last[exp] = running[exp] + count
                running[exp] = running[exp] + (count + 15) // 16 * 16
        for exp in range(N_LOC):
            off_ref[layer * N_LOC + exp, 4] = (last[exp] + CAP - 1) // CAP
            for pad in range(5, 8):
                off_ref[layer * N_LOC + exp, pad] = 0


def route(pack_all):
    return pl.pallas_call(
        route_kernel,
        out_shape=(jax.ShapeDtypeStruct((2, N_EP, 8, TOK), jnp.int32),
                   jax.ShapeDtypeStruct((2, N_EP * TOK, 8), F32),
                   jax.ShapeDtypeStruct((8, 8), jnp.int32)),
        in_specs=[VMEM], out_specs=(VMEM, VMEM, SMEM),
        name='route')(pack_all)


def pick(rank_ref, src, exp):
    row = rank_ref[src, pl.ds(exp, 1), :]
    return (lax.broadcasted_iota(jnp.int32, (CAP, TOK), 0) == row).astype(BF16)


def gate_column(gate_ref, src, exp):
    block = gate_ref[src * TOK:(src + 1) * TOK, :]
    lane = lax.broadcasted_iota(jnp.int32, block.shape, 1)
    return jnp.sum(jnp.where(lane == exp, block, 0.0), axis=1, keepdims=True)


def offset(off_ref, row, src):
    return pl.multiple_of(off_ref[row, src], 16)


def forward_kernel(layer, off_ref, rank_ref, gate_ref, u_ref, wg_ref, wu_ref, wd_ref, out_ref, x_scr, o_scr, acc):
    exp = pl.program_id(0)
    row = layer * N_LOC + exp

    @pl.when(exp == 0)
    def _():
        acc[...] = jnp.zeros_like(acc)

    for src in range(N_EP):
        x_scr[pl.ds(offset(off_ref, row, src), CAP), :] = mm(pick(rank_ref, src, exp), u_ref[src * TOK:(src + 1) * TOK, :]).astype(BF16)
    x_scr[pl.ds(offset(off_ref, row, 3) + CAP, CAP), :] = jnp.zeros((CAP, D), BF16)

    @pl.loop(0, off_ref[row, 4])
    def _(blk):
        rows = pl.ds(pl.multiple_of(blk * CAP, CAP), CAP)
        x_blk = x_scr[rows, :]
        a_pre = mm(x_blk, wg_ref[0])
        b_pre = mm(x_blk, wu_ref[0])
        hidden = (jax.nn.silu(a_pre) * b_pre).astype(BF16)
        o_scr[rows, :] = mm(hidden, wd_ref[0]).astype(BF16)

    o_scr[pl.ds(pl.multiple_of(off_ref[row, 4] * CAP, CAP), CAP), :] = jnp.zeros((CAP, D), BF16)

    for src in range(N_EP):
        tok_out = mm(pick(rank_ref, src, exp), o_scr[pl.ds(offset(off_ref, row, src), CAP), :], ((0,), (0,)))
        acc[src * TOK:(src + 1) * TOK, :] += gate_column(gate_ref, src, exp) * tok_out

    @pl.when(exp == N_LOC - 1)
    def _():
        out_ref[...] = acc[...].astype(BF16)


def expert_forward(layer, off, rank, gate, u_all, w_gate, w_up, w_down):
    weight = pl.BlockSpec((1, D, FF), lambda e: (e, 0, 0))
    return pl.pallas_call(
        functools.partial(forward_kernel, layer),
        grid=(N_LOC,),
        out_shape=jax.ShapeDtypeStruct((N_EP * TOK, D), BF16),
        in_specs=[SMEM, VMEM, VMEM, VMEM, weight, weight, pl.BlockSpec((1, FF, D), lambda e: (e, 0, 0))],
        out_specs=VMEM,
        scratch_shapes=[pltpu.VMEM((SLOTS, D), BF16), pltpu.VMEM((SLOTS, D), BF16), pltpu.VMEM((N_EP * TOK, D), F32)],
        compiler_params=pltpu.CompilerParams(vmem_limit_bytes=56 * 1024 * 1024),
        cost_estimate=pl.CostEstimate(flops=14_000_000_000, bytes_accessed=10_000_000, transcendentals=0),
        name='expert_forward')(off, rank, gate, u_all, w_gate, w_up, w_down)


def backward_kernel(layer, off_ref, rank_ref, gate_ref, u_ref, dy_ref, wg_ref, wu_ref, wd_ref,
                    out_ref, gg_ref, gu_ref, gd_ref, x_scr, d_scr, gx_scr, acc, gg, gu, gd):
    exp = pl.program_id(0)
    row = layer * N_LOC + exp

    @pl.when(exp == 0)
    def _():
        acc[...] = jnp.zeros_like(acc)

    for src in range(N_EP):
        sel = pick(rank_ref, src, exp)
        toks = slice(src * TOK, (src + 1) * TOK)
        rows = pl.ds(offset(off_ref, row, src), CAP)
        x_scr[rows, :] = mm(sel, u_ref[toks, :]).astype(BF16)
        scaled = (gate_column(gate_ref, src, exp) * dy_ref[toks, :].astype(F32)).astype(BF16)
        d_scr[rows, :] = mm(sel, scaled).astype(BF16)
    tail = pl.ds(offset(off_ref, row, 3) + CAP, CAP)
    x_scr[tail, :] = jnp.zeros((CAP, D), BF16)
    d_scr[tail, :] = jnp.zeros((CAP, D), BF16)
    gg[...] = jnp.zeros_like(gg)
    gu[...] = jnp.zeros_like(gu)
    gd[...] = jnp.zeros_like(gd)

    @pl.loop(0, off_ref[row, 4])
    def _(blk):
        rows = pl.ds(pl.multiple_of(blk * CAP, CAP), CAP)
        x_blk = x_scr[rows, :]
        d_blk = d_scr[rows, :]
        a_pre = mm(x_blk, wg_ref[0])
        b_pre = mm(x_blk, wu_ref[0])
        grad_h = mm(d_blk, wd_ref[0], ((1,), (1,))).astype(BF16).astype(F32)
        sigma = jax.nn.sigmoid(a_pre)
        swish = a_pre * sigma
        hidden = (swish * b_pre).astype(BF16)
        grad_a = (grad_h * b_pre * sigma * (1.0 + a_pre * (1.0 - sigma))).astype(BF16)
        grad_b = (grad_h * swish).astype(BF16)
        gx_scr[rows, :] = (mm(grad_a, wg_ref[0], ((1,), (1,))) + mm(grad_b, wu_ref[0], ((1,), (1,)))).astype(BF16)
        gg[...] += mm(x_blk, grad_a, ((0,), (0,)))
        gu[...] += mm(x_blk, grad_b, ((0,), (0,)))
        gd[...] += mm(d_blk, hidden, ((0,), (0,)))

    gx_scr[pl.ds(pl.multiple_of(off_ref[row, 4] * CAP, CAP), CAP), :] = jnp.zeros((CAP, D), BF16)
    gg_ref[0] = gg[...].astype(BF16)
    gu_ref[0] = gu[...].astype(BF16)
    gd_ref[0] = gd[...].astype(BF16)

    for src in range(N_EP):
        acc[src * TOK:(src + 1) * TOK, :] += mm(pick(rank_ref, src, exp), gx_scr[pl.ds(offset(off_ref, row, src), CAP), :], ((0,), (0,)))

    @pl.when(exp == N_LOC - 1)
    def _():
        out_ref[...] = acc[...].astype(BF16)


def expert_backward(layer, off, rank, gate, u_all, dy_all, w_gate, w_up, w_down):
    weight = pl.BlockSpec((1, D, FF), lambda e: (e, 0, 0))
    grad = jax.ShapeDtypeStruct((N_LOC, D, FF), BF16)
    return pl.pallas_call(
        functools.partial(backward_kernel, layer),
        grid=(N_LOC,),
        out_shape=(jax.ShapeDtypeStruct((N_EP * TOK, D), BF16), grad, grad, grad),
        in_specs=[SMEM, VMEM, VMEM, VMEM, VMEM, weight, weight, pl.BlockSpec((1, FF, D), lambda e: (e, 0, 0))],
        out_specs=(VMEM, weight, weight, weight),
        scratch_shapes=[pltpu.VMEM((SLOTS, D), BF16)] * 3 + [pltpu.VMEM((N_EP * TOK, D), F32)] + [pltpu.VMEM((D, FF), F32)] * 3,
        compiler_params=pltpu.CompilerParams(vmem_limit_bytes=56 * 1024 * 1024),
        cost_estimate=pl.CostEstimate(flops=40_000_000_000, bytes_accessed=20_000_000, transcendentals=0),
        name='expert_backward')(off, rank, gate, u_all, dy_all, w_gate, w_up, w_down)


def remote(src, dst, sems, slot, target):
    send, recv = sems
    return pltpu.make_async_remote_copy(src_ref=src, dst_ref=dst, send_sem=send.at[slot], recv_sem=recv.at[slot],
                                        device_id=target, device_id_type=pl.DeviceIdType.MESH)


class Place:
    def __init__(self):
        ep, dp = lax.axis_index('ep'), lax.axis_index('dp')
        self.z, self.y = ep // 2, ep % 2
        self.x, self.c = dp // 2, dp % 2
        self.me = ep
        self.y_ep = self.z * 2 + 1 - self.y
        self.z_ep = (1 - self.z) * 2 + self.y
        self.d_ep = (1 - self.z) * 2 + 1 - self.y
        self.to_y, self.to_z = {'ep': self.y_ep}, {'ep': self.z_ep}
        self.to_c, self.to_x = {'dp': self.x * 2 + 1 - self.c}, {'dp': (1 - self.x) * 2 + self.c}


def greet(targets):
    barrier = pltpu.get_barrier_semaphore()
    for target in targets:
        pl.semaphore_signal(barrier, inc=1, device_id=target, device_id_type=pl.DeviceIdType.MESH)
    pl.semaphore_wait(barrier, len(targets))


HALF = TOK // 2
TOP_ROWS, LOW_ROWS = pl.ds(0, HALF), pl.ds(HALF, HALF)


class Spread:
    def __init__(self, at, own, every, sems):
        self.direct = [remote(own.at[TOP_ROWS], every.at[at.me, TOP_ROWS], sems, 0, at.to_y),
                       remote(own.at[LOW_ROWS], every.at[at.me, LOW_ROWS], sems, 1, at.to_z),
                       remote(own.at[LOW_ROWS], every.at[at.me, LOW_ROWS], sems, 2, at.to_y),
                       remote(own.at[TOP_ROWS], every.at[at.me, TOP_ROWS], sems, 3, at.to_z)]
        self.onward = [remote(every.at[at.y_ep, TOP_ROWS], every.at[at.y_ep, TOP_ROWS], sems, 4, at.to_z),
                       remote(every.at[at.z_ep, LOW_ROWS], every.at[at.z_ep, LOW_ROWS], sems, 5, at.to_y)]

    def start(self):
        for copy in self.direct:
            copy.start()

    def forward(self):
        for first, then in zip(self.direct, self.onward):
            first.wait_recv()
            then.start()

    def finish(self):
        for copy in self.direct[2:] + self.onward:
            copy.wait_recv()
        for copy in self.direct + self.onward:
            copy.wait_send()


class Collect:
    def __init__(self, at, part, got, mix_scr, sems):
        self.at, self.part, self.got, self.mix_scr = at, part, got, mix_scr
        self.direct = [remote(part.at[at.d_ep, TOP_ROWS], got.at[0], sems, 0, at.to_y),
                       remote(part.at[at.d_ep, LOW_ROWS], got.at[1], sems, 1, at.to_z),
                       remote(part.at[at.y_ep, TOP_ROWS], got.at[2], sems, 2, at.to_y),
                       remote(part.at[at.z_ep, LOW_ROWS], got.at[3], sems, 3, at.to_z)]
        self.summed = [remote(mix_scr.at[0], got.at[4], sems, 4, at.to_z),
                       remote(mix_scr.at[1], got.at[5], sems, 5, at.to_y)]

    def start(self):
        for copy in self.direct:
            copy.start()

    def forward(self):
        at = self.at
        for step, (ep, rows) in enumerate(((at.z_ep, TOP_ROWS), (at.y_ep, LOW_ROWS))):
            self.direct[step].wait_recv()
            self.mix_scr[step] = (self.part[ep, rows].astype(F32) + self.got[step].astype(F32)).astype(BF16)
            self.summed[step].start()

    def finish(self, base):
        for copy in self.direct[2:] + self.summed:
            copy.wait_recv()
        me, got = self.at.me, self.got
        top = self.part[me, TOP_ROWS].astype(F32) + got[2].astype(F32) + got[4].astype(F32)
        low = self.part[me, LOW_ROWS].astype(F32) + got[3].astype(F32) + got[5].astype(F32)
        return (base[TOP_ROWS].astype(F32) + top).astype(BF16), (base[LOW_ROWS].astype(F32) + low).astype(BF16)

    def drain(self):
        for copy in self.direct + self.summed:
            copy.wait_send()


N_GRAD = 3 * N_LOC
ROWS_DP = D // 4


class Reduce:
    def __init__(self, at, grads, outs, got_c, own, got_x, pair_sems, own_sem, x_sems):
        self.at, self.outs, self.got_c, self.own, self.got_x = at, outs, got_c, own, got_x
        self.pair, self.load, self.along = [], [], []
        for k in range(N_GRAD):
            grad = grads[k % 3].at[k // 3]
            self.pair.append(remote(grad.at[:, 1 - at.c], got_c.at[k], pair_sems, k, at.to_c))
            self.load.append(pltpu.make_async_copy(grad.at[:, at.c], own.at[k], own_sem.at[k]))
            self.along.append(remote(got_c.at[k, 1 - at.x], got_x.at[k], x_sems, k, at.to_x))

    def start(self):
        for pair, load in zip(self.pair, self.load):
            pair.start()
            load.start()

    def forward(self, ks):
        for k in ks:
            self.pair[k].wait_recv()
            self.load[k].wait()
            for side in range(2):
                self.got_c[k, side] = (self.got_c[k, side].astype(F32) + self.own[k, side].astype(F32)).astype(BF16)
            self.along[k].start()

    def finish(self):
        x = self.at.x
        for k in range(N_GRAD):
            self.along[k].wait_recv()
            self.outs[k % 3][k // 3] = (self.got_c[k, x].astype(F32) + self.got_x[k].astype(F32)).astype(BF16)
        for k in range(N_GRAD):
            self.pair[k].wait_send()
            self.along[k].wait_send()


REDUCE_SCRATCH = [pltpu.VMEM((N_GRAD, 2, ROWS_DP, FF), BF16), pltpu.VMEM((N_GRAD, 2, ROWS_DP, FF), BF16),
                  pltpu.VMEM((N_GRAD, ROWS_DP, FF), BF16)] + [pltpu.SemaphoreType.DMA((N_GRAD,))] * 5
COLLECT_SCRATCH = [pltpu.VMEM((6, HALF, D), BF16), pltpu.VMEM((2, HALF, D), BF16)] + [pltpu.SemaphoreType.DMA((6,))] * 2
SPREAD_SEMS = [pltpu.SemaphoreType.DMA((6,))] * 2
ANY = pl.BlockSpec(memory_space=pl.ANY)


def call(kernel, name, ident, ins, in_specs, outs, scratch):
    return pl.pallas_call(
        kernel, out_shape=outs, in_specs=in_specs, out_specs=jax.tree.map(lambda _: VMEM, outs), scratch_shapes=scratch,
        compiler_params=pltpu.CompilerParams(collective_id=ident, has_side_effects=True, vmem_limit_bytes=48 * 1024 * 1024),
        name=name)(*ins)


def block(*shape, dtype=BF16):
    return jax.ShapeDtypeStruct(shape, dtype)


def entry_kernel(u_ref, pack_ref, every, packs, s_send, s_recv, p_send, p_recv):
    at = Place()
    greet([at.to_y, at.to_z])
    small = [remote(pack_ref, packs.at[at.me], (p_send, p_recv), 0, at.to_y),
             remote(pack_ref, packs.at[at.me], (p_send, p_recv), 1, at.to_z),
             remote(packs.at[at.y_ep], packs.at[at.y_ep], (p_send, p_recv), 2, at.to_z)]
    small[0].start()
    small[1].start()
    spread = Spread(at, u_ref, every, (s_send, s_recv))
    spread.start()
    every[at.me] = u_ref[...]
    packs[at.me] = pack_ref[...]
    small[0].wait_recv()
    small[2].start()
    spread.forward()
    small[1].wait_recv()
    small[2].wait_recv()
    spread.finish()
    for copy in small:
        copy.wait_send()


def middle_kernel(part, u_ref, dense_ref, mid_ref, every, got, mix_scr, c_send, c_recv, u_scr, s_send, s_recv):
    at = Place()
    greet([at.to_y, at.to_z])
    collect = Collect(at, part, got, mix_scr, (c_send, c_recv))
    collect.start()
    collect.forward()
    top, low = collect.finish(u_ref)
    mid_ref[TOP_ROWS] = top
    mid_ref[LOW_ROWS] = low
    u_scr[TOP_ROWS] = (top.astype(F32) + mm(top, dense_ref[...])).astype(BF16)
    u_scr[LOW_ROWS] = (low.astype(F32) + mm(low, dense_ref[...])).astype(BF16)
    spread = Spread(at, u_scr, every, (s_send, s_recv))
    spread.start()
    every[at.me] = u_scr[...]
    collect.drain()
    spread.forward()
    spread.finish()


def dense_grad(x_ref, top, low):
    return mm(x_ref[TOP_ROWS], top, ((0,), (0,))) + mm(x_ref[LOW_ROWS], low, ((0,), (0,)))


def write_slabs(slabs, value):
    for k in range(16):
        slabs[k // 8, k // 4 % 2, k // 2 % 2, k % 2] = value[24 * k:24 * k + 24].astype(BF16)


def turn_kernel(part, dy_ref, dense_ref, mid_ref, ga, gb, gc, grad_ref, every, slabs, oa, ob, oc,
                got, mix_scr, c_send, c_recv, s_send, s_recv, got_c, own, got_x, pair_send, pair_recv, own_sem, x_send, x_recv, g_scr):
    at = Place()
    greet([at.to_y, at.to_z, at.to_c, at.to_x])
    collect = Collect(at, part, got, mix_scr, (c_send, c_recv))
    collect.start()
    reduce = Reduce(at, (ga, gb, gc), (oa, ob, oc), got_c, own, got_x, (pair_send, pair_recv), own_sem, (x_send, x_recv))
    reduce.start()
    reduce.forward(range(6))
    collect.forward()
    reduce.forward(range(6, N_GRAD))
    top, low = collect.finish(dy_ref)
    for rows, half in ((TOP_ROWS, top), (LOW_ROWS, low)):
        g_scr[rows] = (half.astype(F32) + mm(half, dense_ref[...], ((1,), (1,)))).astype(BF16)
    spread = Spread(at, g_scr, every, (s_send, s_recv))
    spread.start()
    grad_ref[...] = g_scr[...]
    every[at.me] = g_scr[...]
    write_slabs(slabs, dense_grad(mid_ref, top, low))
    collect.drain()
    spread.forward()
    spread.finish()
    reduce.finish()


def exit_kernel(part, dy_ref, dense_ref, tok_ref, slabs_two, ga, gb, gc, dx_ref, dense_out, oa, ob, oc,
                got, mix_scr, c_send, c_recv, got_c, own, got_x, pair_send, pair_recv, own_sem, x_send, x_recv,
                slab_c, slab_z, slab_y, slab_x, sum_c, sum_z, sum_y, s_send, s_recv, slabs_one):
    at = Place()
    greet([at.to_y, at.to_z, at.to_c, at.to_x])
    collect = Collect(at, part, got, mix_scr, (c_send, c_recv))
    collect.start()
    reduce = Reduce(at, (ga, gb, gc), (oa, ob, oc), got_c, own, got_x, (pair_send, pair_recv), own_sem, (x_send, x_recv))
    reduce.start()
    reduce.forward(range(6))
    collect.forward()
    reduce.forward(range(6, N_GRAD))
    top, low = collect.finish(dy_ref)
    write_slabs(slabs_one, dense_grad(tok_ref, top, low))
    sems = (s_send, s_recv)
    to_c = [remote(slabs.at[:, 1 - at.c], slab_c.at[k], sems, k, at.to_c) for k, slabs in enumerate((slabs_one, slabs_two))]
    for copy in to_c:
        copy.start()
    for rows, half in ((TOP_ROWS, top), (LOW_ROWS, low)):
        dx_ref[rows] = (half.astype(F32) + mm(half, dense_ref[...], ((1,), (1,)))).astype(BF16)
    for k, slabs in enumerate((slabs_one, slabs_two)):
        to_c[k].wait_recv()
        for side in range(2):
            sum_c[k, side] = (slabs[side, at.c].astype(F32) + slab_c[k, side].astype(F32)).astype(BF16)
    to_z = remote(sum_c.at[:, :, 1 - at.z], slab_z, sems, 2, at.to_z)
    to_z.start()
    to_z.wait_recv()
    for k in range(2):
        for side in range(2):
            sum_z[k, side] = (sum_c[k, side, at.z].astype(F32) + slab_z[k, side].astype(F32)).astype(BF16)
    to_y = remote(sum_z.at[:, :, 1 - at.y], slab_y, sems, 3, at.to_y)
    to_y.start()
    to_y.wait_recv()
    for k in range(2):
        for side in range(2):
            sum_y[side, k] = (sum_z[k, side, at.y].astype(F32) + slab_y[k, side].astype(F32)).astype(BF16)
    to_x = remote(sum_y.at[1 - at.x], slab_x, sems, 4, at.to_x)
    to_x.start()
    reduce.finish()
    to_x.wait_recv()
    dense_out[...] = (sum_y[at.x].astype(F32) + slab_x[...].astype(F32)).astype(BF16)
    collect.drain()
    for copy in to_c + [to_z, to_y, to_x]:
        copy.wait_send()


def by_owner(grad):
    return grad.reshape(N_LOC, 2, 2, ROWS_DP, FF)


REDUCED = (block(N_LOC, ROWS_DP, FF),) * 3


def mix(x_loc, dense_w):
    return (x_loc.astype(F32) + jnp.dot(x_loc, dense_w, preferred_element_type=F32)).astype(BF16)


def rows_of(every):
    return every.reshape(N_EP * TOK, D)


def per_source(part):
    return part.reshape(N_EP, TOK, D)


def solution(mesh):
    tok_spec = P(('dp', 'ep'), None)
    exp_spec = P('ep', None, None)
    layer_specs = (P(None, None), tok_spec, tok_spec, exp_spec, exp_spec, exp_spec)
    grad_specs = (P(('dp', 'ep'), None), P('ep', 'dp', None), P('ep', 'dp', None), P('ep', None, 'dp'))

    def local_step(tokens, dy_out, dense_w1, route_idx1, route_gate1, w_gate1, w_up1, w_down1, dense_w2, route_idx2, route_gate2, w_gate2, w_up2, w_down2):
        pack = jnp.concatenate([route_idx1.T.astype(F32), route_idx2.T.astype(F32), route_gate1.T, route_gate2.T], axis=0)
        mixed_one = mix(tokens, dense_w1)
        u_one, packs = call(entry_kernel, 'entry', 0, (mixed_one, pack), [VMEM, VMEM],
                            (block(N_EP, TOK, D), block(N_EP, 16, TOK, dtype=F32)),
                            SPREAD_SEMS + [pltpu.SemaphoreType.DMA((3,))] * 2)
        rank, gate, off = route(packs)
        dy_later, off = lax.optimization_barrier((dy_out, off))
        dy_all = lax.all_gather(dy_later, 'ep', axis=0, tiled=True)
        part = expert_forward(0, off, rank[0], gate[0], rows_of(u_one), w_gate1, w_up1, w_down1)
        mid_tok, u_two = call(middle_kernel, 'middle', 1, (per_source(part), mixed_one, dense_w2), [VMEM] * 3,
                              (block(TOK, D), block(N_EP, TOK, D)),
                              COLLECT_SCRATCH + [pltpu.VMEM((TOK, D), BF16)] + SPREAD_SEMS)
        part, *grads = expert_backward(1, off, rank[1], gate[1], rows_of(u_two), dy_all, w_gate2, w_up2, w_down2)
        grad_mid, dy_mid, slabs, *reduced_two = call(
            turn_kernel, 'turn', 2, (per_source(part), dy_out, dense_w2, mid_tok) + tuple(map(by_owner, grads)), [VMEM] * 4 + [ANY] * 3,
            (block(TOK, D), block(N_EP, TOK, D), block(2, 2, 2, 2, 24, D)) + REDUCED,
            COLLECT_SCRATCH + SPREAD_SEMS + REDUCE_SCRATCH + [pltpu.VMEM((TOK, D), BF16)])
        part, *grads = expert_backward(0, off, rank[0], gate[0], rows_of(u_one), rows_of(dy_mid), w_gate1, w_up1, w_down1)
        slab = lambda *lead: pltpu.VMEM(lead + (24, D), BF16)
        grad_tok, dense, *reduced_one = call(
            exit_kernel, 'exit', 3, (per_source(part), grad_mid, dense_w1, tokens, slabs) + tuple(map(by_owner, grads)), [VMEM] * 5 + [ANY] * 3,
            (block(TOK, D), block(2, 24, D)) + REDUCED,
            COLLECT_SCRATCH + REDUCE_SCRATCH
            + [slab(2, 2, 2, 2), slab(2, 2, 2), slab(2, 2), slab(2), slab(2, 2, 2, 2), slab(2, 2, 2), slab(2, 2)]
            + [pltpu.SemaphoreType.DMA((5,))] * 2 + [slab(2, 2, 2, 2)])

        def grads_of(k, reduced):
            return (dense[k], reduced[0], reduced[1], jnp.swapaxes(reduced[2], 1, 2))

        return (grad_tok,) + grads_of(0, reduced_one) + grads_of(1, reduced_two)

    return jax.shard_map(local_step, mesh=mesh, in_specs=(tok_spec, tok_spec) + layer_specs + layer_specs,
                         out_specs=(tok_spec,) + grad_specs + grad_specs, check_vma=False)
```

```python
import functools

import jax
import jax.numpy as jnp
from jax import lax
from jax.experimental import pallas as pl
from jax.experimental.pallas import tpu as pltpu
from jax.sharding import PartitionSpec as P

BF16 = jnp.bfloat16
F32 = jnp.float32
N_EP = 4
N_LOC = 4
TOK = 512
D = 384
FF = 672
CAP = 256
SLOTS = 5 * CAP
ROWS_DP = D // 4
VMEM = pl.BlockSpec(memory_space=pltpu.VMEM)
SMEM = pl.BlockSpec(memory_space=pltpu.SMEM)


def block(*shape, dtype=BF16):
    return jax.ShapeDtypeStruct(shape, dtype)


def mm(a, b, dims=((1,), (0,))):
    return lax.dot_general(a, b, (dims, ((), ())), preferred_element_type=F32)


NT = ((1,), (1,))
TN = ((0,), (0,))


def route_into(packs, rank_ref, gate_ref, off_ref, me):
    before = (lax.broadcasted_iota(jnp.int32, (TOK, TOK), 0) < lax.broadcasted_iota(jnp.int32, (TOK, TOK), 1)).astype(BF16)
    for layer in range(2):
        running = [jnp.int32(0)] * N_LOC
        last = [jnp.int32(0)] * N_LOC
        for src in range(N_EP):
            ids = packs[src, 4 * layer:4 * layer + 4, :]
            gates = packs[src, 8 + 4 * layer:12 + 4 * layer, :]
            member, gate = [], []
            for exp in range(N_LOC):
                match = ids == (me * N_LOC + exp).astype(F32)
                member.append(jnp.sum(match.astype(F32), axis=0, keepdims=True))
                gate.append(jnp.sum(jnp.where(match, gates, 0.0), axis=0, keepdims=True))
            member = jnp.concatenate(member, axis=0)
            gate = jnp.concatenate(gate + [jnp.zeros((4, TOK), F32)], axis=0)
            rank = mm(member.astype(BF16), before)
            rank = jnp.where(member > 0.5, rank, -1.0).astype(jnp.int32)
            rank_ref[layer, src, 0:4, :] = rank
            gate_ref[layer, src] = jnp.transpose(gate)
            for exp in range(N_LOC):
                count = jnp.max(rank[exp:exp + 1, :]) + 1
                off_ref[layer * N_LOC + exp, src] = running[exp]
                last[exp] = running[exp] + count
                running[exp] = running[exp] + (count + 15) // 16 * 16
        for exp in range(N_LOC):
            off_ref[layer * N_LOC + exp, 4] = (last[exp] + CAP - 1) // CAP
            for pad in range(5, 8):
                off_ref[layer * N_LOC + exp, pad] = 0


def pick(layer, rank_ref, src, exp):
    row = rank_ref[layer, src, pl.ds(exp, 1), :]
    return (lax.broadcasted_iota(jnp.int32, (CAP, TOK), 0) == row).astype(BF16)


def gate_column(layer, gate_ref, src, exp):
    slab = gate_ref[layer, src]
    lane = lax.broadcasted_iota(jnp.int32, slab.shape, 1)
    return jnp.sum(jnp.where(lane == exp, slab, 0.0), axis=1, keepdims=True)


def offset(off_ref, row, src):
    return pl.multiple_of(off_ref[row, src], 16)


def forward_kernel(layer, off_ref, rank_ref, gate_ref, u_ref, wg_ref, wu_ref, wd_ref, out_ref, x_scr, o_scr, acc):
    acc[...] = jnp.zeros_like(acc)

    @pl.loop(0, N_LOC)
    def _(exp):
        row = layer * N_LOC + exp
        for src in range(N_EP):
            x_scr[pl.ds(offset(off_ref, row, src), CAP), :] = mm(pick(layer, rank_ref, src, exp), u_ref[src]).astype(BF16)
        x_scr[pl.ds(offset(off_ref, row, 3) + CAP, CAP), :] = jnp.zeros((CAP, D), BF16)

        @pl.loop(0, off_ref[row, 4])
        def _(blk):
            rows = pl.ds(pl.multiple_of(blk * CAP, CAP), CAP)
            x_blk = x_scr[rows, :]
            a_pre = mm(x_blk, wg_ref[exp], NT)
            b_pre = mm(x_blk, wu_ref[exp], NT)
            hidden = (jax.nn.silu(a_pre) * b_pre).astype(BF16)
            o_scr[rows, :] = mm(hidden, wd_ref[exp]).astype(BF16)

        o_scr[pl.ds(pl.multiple_of(off_ref[row, 4] * CAP, CAP), CAP), :] = jnp.zeros((CAP, D), BF16)
        for src in range(N_EP):
            tok_out = mm(pick(layer, rank_ref, src, exp), o_scr[pl.ds(offset(off_ref, row, src), CAP), :], TN)
            acc[src] += gate_column(layer, gate_ref, src, exp) * tok_out

    out_ref[...] = acc[...].astype(BF16)


def plain(kernel, name, ins, outs, scratch, flops):
    return pl.pallas_call(
        kernel, out_shape=outs, in_specs=[SMEM] + [VMEM] * (len(ins) - 1), out_specs=jax.tree.map(lambda _: VMEM, outs),
        scratch_shapes=scratch, compiler_params=pltpu.CompilerParams(vmem_limit_bytes=24 * 1024 * 1024),
        cost_estimate=pl.CostEstimate(flops=flops, bytes_accessed=10_000_000, transcendentals=0), name=name)(*ins)


def expert_forward(layer, routes, u_all, weights):
    return plain(functools.partial(forward_kernel, layer), 'expert_forward', routes + (u_all,) + weights, block(N_EP, TOK, D),
                 [pltpu.VMEM((SLOTS, D), BF16)] * 2 + [pltpu.VMEM((N_EP, TOK, D), F32)], 14_000_000_000)


def backward_kernel(layer, first, count, n_dy, carried, off_ref, rank_ref, gate_ref, u_ref, *refs):
    dy_refs, refs = refs[:n_dy], refs[n_dy:]
    before, refs = refs[:carried], refs[carried:]
    wg_ref, wu_ref, wd_ref, out_ref, gg_ref, gu_ref, gd_ref, x_scr, d_scr, gx_scr, acc, gg, gu, gd = refs
    acc[...] = before[0][...] if carried else jnp.zeros_like(acc)

    @pl.loop(first, first + count)
    def _(exp):
        row = layer * N_LOC + exp
        for src in range(N_EP):
            sel = pick(layer, rank_ref, src, exp)
            rows = pl.ds(offset(off_ref, row, src), CAP)
            x_scr[rows, :] = mm(sel, u_ref[src]).astype(BF16)
            dy = dy_refs[src][...] if n_dy > 1 else dy_refs[0][src]
            scaled = (gate_column(layer, gate_ref, src, exp) * dy.astype(F32)).astype(BF16)
            d_scr[rows, :] = mm(sel, scaled).astype(BF16)
        tail = pl.ds(offset(off_ref, row, 3) + CAP, CAP)
        x_scr[tail, :] = jnp.zeros((CAP, D), BF16)
        d_scr[tail, :] = jnp.zeros((CAP, D), BF16)
        gg[...] = jnp.zeros_like(gg)
        gu[...] = jnp.zeros_like(gu)
        gd[...] = jnp.zeros_like(gd)

        @pl.loop(0, off_ref[row, 4])
        def _(blk):
            rows = pl.ds(pl.multiple_of(blk * CAP, CAP), CAP)
            x_blk = x_scr[rows, :]
            d_blk = d_scr[rows, :]
            a_pre = mm(x_blk, wg_ref[exp], NT)
            b_pre = mm(x_blk, wu_ref[exp], NT)
            grad_h = mm(d_blk, wd_ref[exp], NT).astype(BF16).astype(F32)
            sigma = jax.nn.sigmoid(a_pre)
            swish = a_pre * sigma
            hidden = (swish * b_pre).astype(BF16)
            grad_a = (grad_h * b_pre * sigma * (1.0 + a_pre * (1.0 - sigma))).astype(BF16)
            grad_b = (grad_h * swish).astype(BF16)
            gx_scr[rows, :] = (mm(grad_a, wg_ref[exp]) + mm(grad_b, wu_ref[exp])).astype(BF16)
            gg[...] += mm(x_blk, grad_a, TN)
            gu[...] += mm(x_blk, grad_b, TN)
            gd[...] += mm(d_blk, hidden, TN)

        gx_scr[pl.ds(pl.multiple_of(off_ref[row, 4] * CAP, CAP), CAP), :] = jnp.zeros((CAP, D), BF16)
        for grad_ref, grad in ((gg_ref, gg), (gu_ref, gu), (gd_ref, gd)):
            for owner in range(4):
                grad_ref[exp - first, owner // 2, owner % 2] = grad[ROWS_DP * owner:ROWS_DP * owner + ROWS_DP].astype(BF16)
        for src in range(N_EP):
            acc[src] += mm(pick(layer, rank_ref, src, exp), gx_scr[pl.ds(offset(off_ref, row, src), CAP), :], TN)

    out_ref[...] = acc[...].astype(out_ref.dtype)


def expert_backward(layer, first, count, routes, u_all, dys, weights, carried=(), out_type=BF16):
    grad = block(count, 2, 2, ROWS_DP, FF)
    return plain(functools.partial(backward_kernel, layer, first, count, len(dys), len(carried)), 'expert_backward',
                 routes + (u_all,) + dys + carried + weights, (block(N_EP, TOK, D, dtype=out_type), grad, grad, grad),
                 [pltpu.VMEM((SLOTS, D), BF16)] * 3 + [pltpu.VMEM((N_EP, TOK, D), F32)] + [pltpu.VMEM((D, FF), F32)] * 3,
                 9_000_000_000 * count)


def remote(src, dst, sems, slot, target):
    send, recv = sems
    return pltpu.make_async_remote_copy(src_ref=src, dst_ref=dst, send_sem=send.at[slot], recv_sem=recv.at[slot],
                                        device_id=target, device_id_type=pl.DeviceIdType.MESH)


class Place:
    def __init__(self):
        ep, dp = lax.axis_index('ep'), lax.axis_index('dp')
        self.me = ep
        self.z, self.y = ep // 2, ep % 2
        self.x, self.c = dp // 2, dp % 2
        self.to_y, self.to_z = {'ep': self.z * 2 + 1 - self.y}, {'ep': (1 - self.z) * 2 + self.y}
        self.to_c, self.to_x = {'dp': self.x * 2 + 1 - self.c}, {'dp': (1 - self.x) * 2 + self.c}


def greet(targets):
    barrier = pltpu.get_barrier_semaphore()
    for target in targets:
        pl.semaphore_signal(barrier, inc=1, device_id=target, device_id_type=pl.DeviceIdType.MESH)
    pl.semaphore_wait(barrier, len(targets))


HALF = TOK // 2
TOP_ROWS, LOW_ROWS = pl.ds(0, HALF), pl.ds(HALF, HALF)


class Spread:
    def __init__(self, at, own, every, sems):
        self.direct = [remote(own.at[TOP_ROWS], every.at[1, TOP_ROWS], sems, 0, at.to_y),
                       remote(own.at[LOW_ROWS], every.at[2, LOW_ROWS], sems, 1, at.to_z),
                       remote(own.at[LOW_ROWS], every.at[1, LOW_ROWS], sems, 2, at.to_y),
                       remote(own.at[TOP_ROWS], every.at[2, TOP_ROWS], sems, 3, at.to_z)]
        self.onward = [remote(every.at[1, TOP_ROWS], every.at[3, TOP_ROWS], sems, 4, at.to_z),
                       remote(every.at[2, LOW_ROWS], every.at[3, LOW_ROWS], sems, 5, at.to_y)]

    def start(self):
        for copy in self.direct:
            copy.start()

    def forward(self):
        for first, then in zip(self.direct, self.onward):
            first.wait_recv()
            then.start()

    def finish(self):
        for copy in self.direct[2:] + self.onward:
            copy.wait_recv()
        for copy in self.direct + self.onward:
            copy.wait_send()


class Collect:
    def __init__(self, at, part, got, mix_scr, sems):
        self.part, self.got, self.mix_scr = part, got, mix_scr
        self.direct = [remote(part.at[3, TOP_ROWS], got.at[0], sems, 0, at.to_y),
                       remote(part.at[3, LOW_ROWS], got.at[1], sems, 1, at.to_z),
                       remote(part.at[1, TOP_ROWS], got.at[2], sems, 2, at.to_y),
                       remote(part.at[2, LOW_ROWS], got.at[3], sems, 3, at.to_z)]
        self.summed = [remote(mix_scr.at[0], got.at[4], sems, 4, at.to_z),
                       remote(mix_scr.at[1], got.at[5], sems, 5, at.to_y)]

    def start(self):
        for copy in self.direct:
            copy.start()

    def forward(self):
        for step, (slot, rows) in enumerate(((2, TOP_ROWS), (1, LOW_ROWS))):
            self.direct[step].wait_recv()
            self.mix_scr[step] = (self.part[slot, rows].astype(F32) + self.got[step].astype(F32)).astype(BF16)
            self.summed[step].start()

    def finish(self, base):
        for copy in self.direct[2:] + self.summed:
            copy.wait_recv()
        got = self.got
        top = self.part[0, TOP_ROWS].astype(F32) + got[2].astype(F32) + got[4].astype(F32)
        low = self.part[0, LOW_ROWS].astype(F32) + got[3].astype(F32) + got[5].astype(F32)
        return (base[TOP_ROWS].astype(F32) + top).astype(BF16), (base[LOW_ROWS].astype(F32) + low).astype(BF16)

    def drain(self):
        for copy in self.direct + self.summed:
            copy.wait_send()


class Halve:
    def __init__(self, at, grads, first, got, sems):
        self.at, self.grads, self.first, self.got = at, grads, first, got
        self.pair = [remote(grads[k // 2].at[first + k % 2, :, 1 - at.c], got.at[k], sems, k, at.to_c) for k in range(6)]

    def start(self):
        for copy in self.pair:
            copy.start()

    def total(self, mat, side):
        return jnp.concatenate([self.grads[mat][self.first + exp, side, self.at.c].astype(F32) + self.got[2 * mat + exp, side].astype(F32)
                                for exp in range(2)], axis=1).astype(BF16)

    def wait(self, mat):
        for exp in range(2):
            self.pair[2 * mat + exp].wait_recv()

    def drain(self):
        for copy in self.pair:
            copy.wait_send()


def store_pair(out, first, keep, got):
    total = (keep.astype(F32) + got.astype(F32)).astype(BF16)
    for exp in range(2):
        out[first + exp] = total[:, FF * exp:FF * exp + FF]


class Across:
    def __init__(self, at, halve, keep, send, got, sems):
        self.at, self.halve, self.keep, self.send, self.got = at, halve, keep, send, got
        self.along = [remote(send.at[mat], got.at[mat], sems, mat, at.to_x) for mat in range(3)]

    def forward(self, mat):
        self.halve.wait(mat)
        self.send[mat] = self.halve.total(mat, 1 - self.at.x)
        self.along[mat].start()
        self.keep[mat] = self.halve.total(mat, self.at.x)

    def finish(self, outs, first):
        for mat in range(3):
            self.along[mat].wait_recv()
            store_pair(outs[mat], first, self.keep[mat], self.got[mat])
        for copy in self.along:
            copy.wait_send()


def sems(count):
    return [pltpu.SemaphoreType.DMA((count,))] * 2


PACKED = (3, ROWS_DP, 2 * FF)
COLLECT_SCRATCH = [pltpu.VMEM((6, HALF, D), BF16), pltpu.VMEM((2, HALF, D), BF16)] + sems(6)
HALVE_SCRATCH = [pltpu.VMEM((6, 2, ROWS_DP, FF), BF16)] + sems(6)
ACROSS_SCRATCH = [pltpu.VMEM(PACKED, BF16)] * 3 + sems(3)


def call(kernel, name, ident, ins, outs, scratch):
    return pl.pallas_call(
        kernel, out_shape=outs, in_specs=[VMEM] * len(ins), scratch_shapes=scratch,
        out_specs=jax.tree.map(lambda o: SMEM if o.shape == (8, 8) else VMEM, outs),
        compiler_params=pltpu.CompilerParams(collective_id=ident, has_side_effects=True, vmem_limit_bytes=24 * 1024 * 1024),
        cost_estimate=pl.CostEstimate(flops=10_000_000_000, bytes_accessed=4_000_000, transcendentals=0), name=name)(*ins)


def entry_kernel(u_ref, pack_ref, every, rank_ref, gate_ref, off_ref, packs, s_send, s_recv, p_send, p_recv):
    at = Place()
    greet([at.to_y, at.to_z])
    small = [remote(pack_ref, packs.at[1], (p_send, p_recv), 0, at.to_y),
             remote(pack_ref, packs.at[2], (p_send, p_recv), 1, at.to_z),
             remote(packs.at[1], packs.at[3], (p_send, p_recv), 2, at.to_z)]
    small[0].start()
    small[1].start()
    spread = Spread(at, u_ref, every, (s_send, s_recv))
    spread.start()
    every[0] = u_ref[...]
    packs[0] = pack_ref[...]
    small[0].wait_recv()
    small[2].start()
    spread.forward()
    small[1].wait_recv()
    small[2].wait_recv()
    route_into(packs, rank_ref, gate_ref, off_ref, at.me)
    spread.finish()
    for copy in small:
        copy.wait_send()


def middle_kernel(part, u_ref, dense_ref, mid_ref, every, got, mix_scr, c_send, c_recv, u_scr, s_send, s_recv):
    at = Place()
    greet([at.to_y, at.to_z])
    collect = Collect(at, part, got, mix_scr, (c_send, c_recv))
    collect.start()
    collect.forward()
    top, low = collect.finish(u_ref)
    for rows, half in ((TOP_ROWS, top), (LOW_ROWS, low)):
        u_scr[rows] = (half.astype(F32) + mm(half, dense_ref[...])).astype(BF16)
    spread = Spread(at, u_scr, every, (s_send, s_recv))
    spread.start()
    mid_ref[TOP_ROWS] = top
    mid_ref[LOW_ROWS] = low
    every[0] = u_scr[...]
    collect.drain()
    spread.forward()
    spread.finish()


def dense_grad(x_ref, top, low):
    return mm(x_ref[TOP_ROWS], top, TN) + mm(x_ref[LOW_ROWS], low, TN)


def write_slabs(slabs, value):
    for k in range(16):
        slabs[k // 8, k // 4 % 2, k // 2 % 2, k % 2] = value[24 * k:24 * k + 24].astype(BF16)


def turn_kernel(part, dy_ref, dense_ref, mid_ref, ga, gb, gc, grad_ref, every, slabs, oa, ob, oc, later_keep, later_send,
                got, mix_scr, c_send, c_recv, s_send, s_recv, got_a, a_send, a_recv, got_b, b_send, b_recv,
                keep, send, got_x, x_send, x_recv, g_scr):
    at = Place()
    greet([at.to_y, at.to_z, at.to_c, at.to_x])
    collect = Collect(at, part, got, mix_scr, (c_send, c_recv))
    collect.start()
    now = Halve(at, (ga, gb, gc), 0, got_a, (a_send, a_recv))
    later = Halve(at, (ga, gb, gc), 2, got_b, (b_send, b_recv))
    now.start()
    later.start()
    across = Across(at, now, keep, send, got_x, (x_send, x_recv))
    for mat in range(3):
        across.forward(mat)
    collect.forward()
    for mat in range(3):
        later.wait(mat)
        later_send[mat] = later.total(mat, 1 - at.x)
        later_keep[mat] = later.total(mat, at.x)
    top, low = collect.finish(dy_ref)
    for rows, half in ((TOP_ROWS, top), (LOW_ROWS, low)):
        g_scr[rows] = (half.astype(F32) + mm(half, dense_ref[...], NT)).astype(BF16)
    spread = Spread(at, g_scr, every, (s_send, s_recv))
    spread.start()
    grad_ref[...] = g_scr[...]
    every[0] = g_scr[...]
    write_slabs(slabs, dense_grad(mid_ref, top, low))
    collect.drain()
    spread.forward()
    now.drain()
    later.drain()
    across.finish((oa, ob, oc), 0)
    spread.finish()


def pair_kernel(ga, gb, gc, later_keep, later_send, got_b, b_send, b_recv):
    at = Place()
    greet([at.to_c])
    later = Halve(at, (ga, gb, gc), 0, got_b, (b_send, b_recv))
    later.start()
    for mat in range(3):
        later.wait(mat)
        later_send[mat] = later.total(mat, 1 - at.x)
        later_keep[mat] = later.total(mat, at.x)
    later.drain()


def exit_kernel(part, dy_ref, dense_ref, tok_ref, slabs_two, ga, gb, gc, two_keep, two_got, one_keep, one_got, da, db, dc,
                dx_ref, dense_one, dense_two, oa, ob, oc, ta, tb, tc,
                got, mix_scr, c_send, c_recv, got_a, a_send, a_recv, keep, send, got_x, x_send, x_recv,
                slab_c, slab_z, slab_y, slab_x, sum_c, sum_z, sum_y, s_send, s_recv, slabs_one):
    at = Place()
    greet([at.to_y, at.to_z, at.to_c, at.to_x])
    collect = Collect(at, part, got, mix_scr, (c_send, c_recv))
    collect.start()
    now = Halve(at, (ga, gb, gc), 0, got_a, (a_send, a_recv))
    now.start()
    across = Across(at, now, keep, send, got_x, (x_send, x_recv))
    for mat in range(3):
        across.forward(mat)
    collect.forward()
    for mat, (out, done) in enumerate(((ta, da), (tb, db), (tc, dc))):
        store_pair(out, 2, two_keep[mat], two_got[mat])
        out[0:2] = done[...]
    for mat, out in enumerate((oa, ob, oc)):
        store_pair(out, 0, one_keep[mat], one_got[mat])
    top, low = collect.finish(dy_ref)
    write_slabs(slabs_one, dense_grad(tok_ref, top, low))
    pair = (s_send, s_recv)
    to_c = [remote(slabs.at[:, 1 - at.c], slab_c.at[k], pair, k, at.to_c) for k, slabs in enumerate((slabs_one, slabs_two))]
    for copy in to_c:
        copy.start()
    for rows, half in ((TOP_ROWS, top), (LOW_ROWS, low)):
        dx_ref[rows] = (half.astype(F32) + mm(half, dense_ref[...], NT)).astype(BF16)
    for k, slabs in enumerate((slabs_one, slabs_two)):
        to_c[k].wait_recv()
        for side in range(2):
            sum_c[k, side] = (slabs[side, at.c].astype(F32) + slab_c[k, side].astype(F32)).astype(BF16)
    to_z = remote(sum_c.at[:, :, 1 - at.z], slab_z, pair, 2, at.to_z)
    to_z.start()
    to_z.wait_recv()
    for k in range(2):
        for side in range(2):
            sum_z[k, side] = (sum_c[k, side, at.z].astype(F32) + slab_z[k, side].astype(F32)).astype(BF16)
    to_y = remote(sum_z.at[:, :, 1 - at.y], slab_y, pair, 3, at.to_y)
    to_y.start()
    to_y.wait_recv()
    for k in range(2):
        for side in range(2):
            sum_y[side, k] = (sum_z[k, side, at.y].astype(F32) + slab_y[k, side].astype(F32)).astype(BF16)
    to_x = remote(sum_y.at[1 - at.x], slab_x, pair, 4, at.to_x)
    to_x.start()
    across.finish((oa, ob, oc), 2)
    to_x.wait_recv()
    for k, out in enumerate((dense_one, dense_two)):
        out[...] = (sum_y[at.x, k].astype(F32) + slab_x[k].astype(F32)).astype(BF16)
    collect.drain()
    now.drain()
    for copy in to_c + [to_z, to_y, to_x]:
        copy.wait_send()


def store_kernel(*refs):
    count = len(refs) // 2
    copies = [pltpu.make_async_copy(refs[k], refs[count + k], refs[-1].at[k]) for k in range(count)]
    for copy in copies:
        copy.start()
    for copy in copies:
        copy.wait()


def store_all(values):
    return pl.pallas_call(
        store_kernel, out_shape=[block(*value.shape) for value in values], in_specs=[VMEM] * len(values),
        out_specs=[pl.BlockSpec(memory_space=pl.ANY)] * len(values), scratch_shapes=[pltpu.SemaphoreType.DMA((len(values),))],
        compiler_params=pltpu.CompilerParams(vmem_limit_bytes=1024 * 1024),
        cost_estimate=pl.CostEstimate(flops=1_000_000_000, bytes_accessed=4_000_000, transcendentals=0), name='store')(*values)


def mix(x_loc, dense_w):
    return (x_loc.astype(F32) + jnp.dot(x_loc, dense_w, preferred_element_type=F32)).astype(BF16)


def stored(w_gate, w_up, w_down):
    return jnp.swapaxes(w_gate, 1, 2), jnp.swapaxes(w_up, 1, 2), w_down


def along_x(sent):
    return lax.ppermute(sent, 'dp', [(0, 2), (2, 0), (1, 3), (3, 1)])


def solution(mesh):
    tok_spec = P(('dp', 'ep'), None)
    exp_spec = P('ep', None, None)
    layer_specs = (P(None, None), tok_spec, tok_spec, exp_spec, exp_spec, exp_spec)
    grad_specs = (P(('dp', 'ep'), None), P('ep', 'dp', None), P('ep', 'dp', None), P('ep', None, 'dp'))

    def local_step(tokens, dy_out, dense_w1, route_idx1, route_gate1, w_gate1, w_up1, w_down1, dense_w2, route_idx2, route_gate2, w_gate2, w_up2, w_down2):
        weights_one, weights_two = stored(w_gate1, w_up1, w_down1), stored(w_gate2, w_up2, w_down2)
        tok_block, all_block = block(TOK, D), block(N_EP, TOK, D)
        pack = jnp.concatenate([route_idx1.T.astype(F32), route_idx2.T.astype(F32), route_gate1.T, route_gate2.T], axis=0)
        mixed_one = mix(tokens, dense_w1)
        u_one, rank, gate, off = call(
            entry_kernel, 'entry', 0, (mixed_one, pack),
            (all_block, block(2, N_EP, 8, TOK, dtype=jnp.int32), block(2, N_EP, TOK, 8, dtype=F32), block(8, 8, dtype=jnp.int32)),
            [pltpu.VMEM((N_EP, 16, TOK), F32)] + sems(6) + sems(3))
        routes = (off, rank, gate)
        dy_later, u_one = lax.optimization_barrier((dy_out, u_one))
        dy_all = (dy_out,) + tuple(lax.ppermute(dy_later, 'ep', [(k, k ^ flip) for k in range(N_EP)]) for flip in (1, 2, 3))
        part = expert_forward(0, routes, u_one, weights_one)
        mid_tok, u_two = call(middle_kernel, 'middle', 1, (part, mixed_one, dense_w2), (tok_block, all_block),
                              COLLECT_SCRATCH + [pltpu.VMEM((TOK, D), BF16)] + sems(6))
        part, *grads = expert_backward(1, 0, 4, routes, u_two, dy_all, weights_two)
        grad_mid, dy_mid, slabs, *done_two, keep_two, send_two = call(
            turn_kernel, 'turn', 2, (part, dy_out, dense_w2, mid_tok) + tuple(grads),
            (tok_block, all_block, block(2, 2, 2, 2, 24, D)) + (block(2, ROWS_DP, FF),) * 3 + (block(*PACKED),) * 2,
            COLLECT_SCRATCH + sems(6) + HALVE_SCRATCH * 2 + ACROSS_SCRATCH + [pltpu.VMEM((TOK, D), BF16)])
        got_two = along_x(send_two)
        part, *grads = expert_backward(0, 0, 2, routes, u_one, (dy_mid,), weights_one, out_type=F32)
        got_two, grads = lax.optimization_barrier((got_two, grads))
        keep_one, send_one = call(pair_kernel, 'pair', 4, tuple(grads), (block(*PACKED),) * 2, HALVE_SCRATCH)
        got_one = along_x(send_one)
        part, *grads = expert_backward(0, 2, 2, routes, u_one, (dy_mid,), weights_one, carried=(part,))
        slab = lambda *lead: pltpu.VMEM(lead + (24, D), BF16)
        grad_tok, dense_one, dense_two, *reduced = store_all(call(
            exit_kernel, 'exit', 3, (part, grad_mid, dense_w1, tokens, slabs) + tuple(grads) + (keep_two, got_two, keep_one, got_one) + tuple(done_two),
            (tok_block, block(24, D), block(24, D)) + (block(N_LOC, ROWS_DP, FF),) * 6,
            COLLECT_SCRATCH + HALVE_SCRATCH + ACROSS_SCRATCH
            + [slab(2, 2, 2, 2), slab(2, 2, 2), slab(2, 2), slab(2), slab(2, 2, 2, 2), slab(2, 2, 2), slab(2, 2)]
            + sems(5) + [slab(2, 2, 2, 2)]))

        def shaped(gate_up_down):
            return gate_up_down[0], gate_up_down[1], jnp.swapaxes(gate_up_down[2], 1, 2)

        return (grad_tok, dense_one) + shaped(reduced[:3]) + (dense_two,) + shaped(reduced[3:])

    return jax.shard_map(local_step, mesh=mesh, in_specs=(tok_spec, tok_spec) + layer_specs + layer_specs,
                         out_specs=(tok_spec,) + grad_specs + grad_specs, check_vma=False)
```

```python
import functools

import jax
import jax.numpy as jnp
from jax import lax
from jax.experimental import pallas as pl
from jax.experimental.pallas import tpu as pltpu
from jax.sharding import PartitionSpec as P

BF16 = jnp.bfloat16
F32 = jnp.float32
N_EP = 4
N_LOC = 4
TOK = 512
D = 384
FF = 672
CAP = 256
SLOTS = 5 * CAP
ROWS_DP = D // 4
VMEM = pl.BlockSpec(memory_space=pltpu.VMEM)
SMEM = pl.BlockSpec(memory_space=pltpu.SMEM)


def block(*shape, dtype=BF16):
    return jax.ShapeDtypeStruct(shape, dtype)


def mm(a, b, dims=((1,), (0,))):
    return lax.dot_general(a, b, (dims, ((), ())), preferred_element_type=F32)


NT = ((1,), (1,))
TN = ((0,), (0,))


def route_into(packs, rank_ref, gate_ref, off_ref, me):
    before = (lax.broadcasted_iota(jnp.int32, (TOK, TOK), 0) < lax.broadcasted_iota(jnp.int32, (TOK, TOK), 1)).astype(BF16)
    for layer in range(2):
        running = [jnp.int32(0)] * N_LOC
        last = [jnp.int32(0)] * N_LOC
        for src in range(N_EP):
            ids = packs[src, 4 * layer:4 * layer + 4, :]
            gates = packs[src, 8 + 4 * layer:12 + 4 * layer, :]
            member, gate = [], []
            for exp in range(N_LOC):
                match = ids == (me * N_LOC + exp).astype(F32)
                member.append(jnp.sum(match.astype(F32), axis=0, keepdims=True))
                gate.append(jnp.sum(jnp.where(match, gates, 0.0), axis=0, keepdims=True))
            member = jnp.concatenate(member, axis=0)
            gate = jnp.concatenate(gate + [jnp.zeros((4, TOK), F32)], axis=0)
            rank = mm(member.astype(BF16), before)
            rank = jnp.where(member > 0.5, rank, -1.0).astype(jnp.int32)
            rank_ref[layer, src, 0:4, :] = rank
            gate_ref[layer, src] = jnp.transpose(gate)
            for exp in range(N_LOC):
                count = jnp.max(rank[exp:exp + 1, :]) + 1
                off_ref[layer * N_LOC + exp, src] = running[exp]
                last[exp] = running[exp] + count
                running[exp] = running[exp] + (count + 15) // 16 * 16
        for exp in range(N_LOC):
            halves = (last[exp] + CAP // 2 - 1) // (CAP // 2)
            off_ref[layer * N_LOC + exp, 4] = halves // 2
            off_ref[layer * N_LOC + exp, 5] = halves % 2
            off_ref[layer * N_LOC + exp, 6] = halves * (CAP // 2)
            off_ref[layer * N_LOC + exp, 7] = (halves + 1) // 2


def pick(layer, rank_ref, src, exp):
    row = rank_ref[layer, src, pl.ds(exp, 1), :]
    return (lax.broadcasted_iota(jnp.int32, (CAP, TOK), 0) == row).astype(BF16)


def gate_column(layer, gate_ref, src, exp):
    slab = gate_ref[layer, src]
    lane = lax.broadcasted_iota(jnp.int32, slab.shape, 1)
    return jnp.sum(jnp.where(lane == exp, slab, 0.0), axis=1, keepdims=True)


def offset(off_ref, row, src):
    return pl.multiple_of(off_ref[row, src], 16)


def scatter_gated(layer, rank_ref, gate_ref, o_ref, src):
    total = None
    for exp in range(N_LOC):
        term = gate_column(layer, gate_ref, src, exp) * mm(pick(layer, rank_ref, src, exp), o_ref[exp, src], TN)
        total = term if total is None else total + term
    return total.astype(BF16)


def scatter_plain(layer, rank_ref, g_refs, src):
    sel = jnp.concatenate([pick(layer, rank_ref, src, exp) for exp in range(N_LOC)], axis=0)
    per = N_LOC // len(g_refs)
    rows = [g_refs[exp // per][exp % per, src] for exp in range(N_LOC)]
    return mm(sel, jnp.concatenate(rows, axis=0), TN).astype(BF16)


def gather_rows(layer, rank_ref, pad_ref, src, toks):
    @pl.loop(0, N_LOC)
    def _(exp):
        pad_ref[exp, src] = mm(pick(layer, rank_ref, src, exp), toks[...]).astype(BF16)


def gather_scaled(layer, rank_ref, gate_ref, pad_ref, src, toks):
    @pl.loop(0, N_LOC)
    def _(exp):
        scaled = (gate_column(layer, gate_ref, src, exp) * toks[...].astype(F32)).astype(BF16)
        pad_ref[exp, src] = mm(pick(layer, rank_ref, src, exp), scaled).astype(BF16)


def packed(off_ref, row, pad_ref, exp, scr):
    for src in range(N_EP):
        scr[pl.ds(offset(off_ref, row, src), CAP), :] = pad_ref[exp, src]
    scr[pl.ds(offset(off_ref, row, 3) + CAP, CAP), :] = jnp.zeros((CAP, D), BF16)


def over_rows(off_ref, row, step):
    @pl.loop(0, off_ref[row, 4])
    def _(blk):
        step(pl.ds(pl.multiple_of(blk * CAP, CAP), CAP))

    @pl.when(off_ref[row, 5] == 1)
    def _():
        step(pl.ds(pl.multiple_of(off_ref[row, 4] * CAP, CAP), CAP // 2))


def tail_of(off_ref, row, size):
    return pl.ds(pl.multiple_of(off_ref[row, 6], CAP // 2), size)


def unpacked(off_ref, row, scr, out_ref, exp):
    for src in range(N_EP):
        out_ref[exp, src] = scr[pl.ds(offset(off_ref, row, src), CAP), :]


def forward_kernel(layer, off_ref, x_ref, wg_ref, wu_ref, wd_ref, out_ref, x_scr, o_scr):
    @pl.loop(0, N_LOC)
    def _(exp):
        row = layer * N_LOC + exp
        packed(off_ref, row, x_ref, exp, x_scr)

        def step(rows):
            x_blk = x_scr[rows, :]
            a_pre = mm(x_blk, wg_ref[exp], NT)
            b_pre = mm(x_blk, wu_ref[exp], NT)
            hidden = (jax.nn.silu(a_pre) * b_pre).astype(BF16)
            o_scr[rows, :] = mm(hidden, wd_ref[exp]).astype(BF16)

        over_rows(off_ref, row, step)
        o_scr[tail_of(off_ref, row, CAP), :] = jnp.zeros((CAP, D), BF16)
        unpacked(off_ref, row, o_scr, out_ref, exp)


def plain(kernel, name, ins, outs, scratch, grant, flops):
    return pl.pallas_call(
        kernel, out_shape=outs, in_specs=[SMEM] + [VMEM] * (len(ins) - 1), out_specs=jax.tree.map(lambda _: VMEM, outs),
        scratch_shapes=scratch, compiler_params=pltpu.CompilerParams(vmem_limit_bytes=grant * 1024 * 1024),
        cost_estimate=pl.CostEstimate(flops=flops, bytes_accessed=10_000_000, transcendentals=0), name=name)(*ins)


def expert_forward(layer, off, x_pad, weights):
    return plain(functools.partial(forward_kernel, layer), 'expert_forward', (off, x_pad) + weights, block(N_LOC, N_EP, CAP, D),
                 [pltpu.VMEM((SLOTS, D), BF16)] * 2, 8, 10_000_000_000)


def backward_kernel(layer, first, count, off_ref, x_ref, d_ref, wg_ref, wu_ref, wd_ref, out_ref, grad_ref, left, right, gx_scr):
    x_scr, d_scr = left.at[0], left.at[1]

    @pl.loop(first, first + count)
    def _(exp):
        row = layer * N_LOC + exp
        packed(off_ref, row, x_ref, exp, x_scr)
        packed(off_ref, row, d_ref, exp, d_scr)

        def step(rows):
            x_blk = x_scr[rows, :]
            a_pre = mm(x_blk, wg_ref[exp], NT)
            b_pre = mm(x_blk, wu_ref[exp], NT)
            grad_h = mm(d_scr[rows, :], wd_ref[exp], NT).astype(BF16).astype(F32)
            sigma = jax.nn.sigmoid(a_pre)
            swish = a_pre * sigma
            grad_a = (grad_h * b_pre * sigma * (1.0 + a_pre * (1.0 - sigma))).astype(BF16)
            grad_b = (grad_h * swish).astype(BF16)
            right[0, rows, :] = grad_a
            right[1, rows, :] = grad_b
            right[2, rows, :] = (swish * b_pre).astype(BF16)
            gx_scr[rows, :] = (mm(grad_a, wg_ref[exp]) + mm(grad_b, wu_ref[exp])).astype(BF16)

        over_rows(off_ref, row, step)
        gx_scr[tail_of(off_ref, row, CAP), :] = jnp.zeros((CAP, D), BF16)
        unpacked(off_ref, row, gx_scr, out_ref, exp - first)
        right[:, tail_of(off_ref, row, CAP // 2), :] = jnp.zeros((3, CAP // 2, FF), BF16)

        def weight_grads(depth):
            @pl.loop(0, 3)
            def _(mat):
                grad = mm(left[mat // 2, 0:depth, :], right[mat, 0:depth, :], TN).astype(BF16)
                for owner in range(4):
                    grad_ref[exp - first, mat, owner // 2, owner % 2] = grad[ROWS_DP * owner:ROWS_DP * owner + ROWS_DP]

        for blocks in range(1, 5):
            pl.when(off_ref[row, 7] == blocks)(functools.partial(weight_grads, blocks * CAP))

        @pl.when(off_ref[row, 7] == 0)
        def _():
            grad_ref[exp - first] = jnp.zeros(grad_ref.shape[1:], BF16)


def expert_backward(layer, first, count, off, x_pad, d_pad, weights):
    return plain(functools.partial(backward_kernel, layer, first, count), 'expert_backward',
                 (off, x_pad, d_pad) + weights, (block(count, N_EP, CAP, D), block(count, 3, 2, 2, ROWS_DP, FF)),
                 [pltpu.VMEM((2, SLOTS, D), BF16), pltpu.VMEM((3, N_EP * CAP + CAP // 2, FF), BF16), pltpu.VMEM((SLOTS, D), BF16)], 14, 9_000_000_000 * count)


def remote(src, dst, sems, slot, target):
    send, recv = sems
    return pltpu.make_async_remote_copy(src_ref=src, dst_ref=dst, send_sem=send.at[slot], recv_sem=recv.at[slot],
                                        device_id=target, device_id_type=pl.DeviceIdType.MESH)


class Place:
    def __init__(self):
        ep, dp = lax.axis_index('ep'), lax.axis_index('dp')
        self.me = ep
        self.z, self.y = ep // 2, ep % 2
        self.x, self.c = dp // 2, dp % 2
        self.to_y, self.to_z = {'ep': self.z * 2 + 1 - self.y}, {'ep': (1 - self.z) * 2 + self.y}
        self.to_d = {'ep': (1 - self.z) * 2 + 1 - self.y}
        self.to_c, self.to_x = {'dp': self.x * 2 + 1 - self.c}, {'dp': (1 - self.x) * 2 + self.c}


def greet(targets):
    barrier = pltpu.get_barrier_semaphore()
    for target in targets:
        pl.semaphore_signal(barrier, inc=1, device_id=target, device_id_type=pl.DeviceIdType.MESH)
    pl.semaphore_wait(barrier, len(targets))


HALF = TOK // 2
TOP_ROWS, LOW_ROWS = pl.ds(0, HALF), pl.ds(HALF, HALF)


class Spread:
    def __init__(self, at, own, every, sems):
        self.direct = [remote(own.at[TOP_ROWS], every.at[1, TOP_ROWS], sems, 0, at.to_y),
                       remote(own.at[LOW_ROWS], every.at[2, LOW_ROWS], sems, 1, at.to_z),
                       remote(own.at[LOW_ROWS], every.at[1, LOW_ROWS], sems, 2, at.to_y),
                       remote(own.at[TOP_ROWS], every.at[2, TOP_ROWS], sems, 3, at.to_z)]
        self.onward = [remote(every.at[1, TOP_ROWS], every.at[3, TOP_ROWS], sems, 4, at.to_z),
                       remote(every.at[2, LOW_ROWS], every.at[3, LOW_ROWS], sems, 5, at.to_y)]

    def start(self):
        for copy in self.direct:
            copy.start()

    def forward(self):
        for first, then in zip(self.direct, self.onward):
            first.wait_recv()
            then.start()

    def arrived(self, slot):
        for copy in ((), self.direct[2:3], self.direct[3:4], self.onward)[slot]:
            copy.wait_recv()

    def finish(self):
        for copy in self.direct + self.onward:
            copy.wait_send()


class Collect:
    def __init__(self, at, part, got, mix_scr, sems):
        self.part, self.got, self.mix_scr = part, got, mix_scr
        self.direct = [remote(part.at[3, TOP_ROWS], got.at[0], sems, 0, at.to_y),
                       remote(part.at[3, LOW_ROWS], got.at[1], sems, 1, at.to_z),
                       remote(part.at[1, TOP_ROWS], got.at[2], sems, 2, at.to_y),
                       remote(part.at[2, LOW_ROWS], got.at[3], sems, 3, at.to_z)]
        self.summed = [remote(mix_scr.at[0], got.at[4], sems, 4, at.to_z),
                       remote(mix_scr.at[1], got.at[5], sems, 5, at.to_y)]

    def start(self, slot_sum):
        self.part[3] = slot_sum(3)
        self.direct[0].start()
        self.direct[1].start()
        self.part[1] = slot_sum(1)
        self.direct[2].start()
        self.part[2] = slot_sum(2)
        self.direct[3].start()

    def forward(self):
        for step, (slot, rows) in enumerate(((2, TOP_ROWS), (1, LOW_ROWS))):
            self.direct[step].wait_recv()
            self.mix_scr[step] = (self.part[slot, rows].astype(F32) + self.got[step].astype(F32)).astype(BF16)
            self.summed[step].start()

    def finish(self, base):
        for copy in self.direct[2:] + self.summed:
            copy.wait_recv()
        got = self.got
        top = self.part[0, TOP_ROWS].astype(F32) + got[2].astype(F32) + got[4].astype(F32)
        low = self.part[0, LOW_ROWS].astype(F32) + got[3].astype(F32) + got[5].astype(F32)
        return (base[TOP_ROWS].astype(F32) + top).astype(BF16), (base[LOW_ROWS].astype(F32) + low).astype(BF16)

    def summed_gone(self):
        for copy in self.summed:
            copy.wait_send()

    def drain(self):
        for copy in self.direct:
            copy.wait_send()


class Halve:
    def __init__(self, at, grads, first, got, sems):
        self.at, self.grads, self.first, self.got = at, grads, first, got
        self.pair = [remote(grads.at[first + k % 2, k // 2, :, 1 - at.c], got.at[k], sems, k, at.to_c) for k in range(6)]

    def start(self):
        for copy in self.pair:
            copy.start()

    def total(self, mat, side):
        return jnp.concatenate([self.grads[self.first + exp, mat, side, self.at.c].astype(F32) + self.got[2 * mat + exp, side].astype(F32)
                                for exp in range(2)], axis=1).astype(BF16)

    def wait(self, mat):
        for exp in range(2):
            self.pair[2 * mat + exp].wait_recv()

    def drain(self):
        for copy in self.pair:
            copy.wait_send()


def store_pair(out, first, keep, got):
    total = (keep.astype(F32) + got.astype(F32)).astype(BF16)
    for exp in range(2):
        out[first + exp] = total[:, FF * exp:FF * exp + FF]


class Across:
    def __init__(self, at, halve, keep, send, got, sems):
        self.at, self.halve, self.keep, self.send, self.got = at, halve, keep, send, got
        self.along = [remote(send.at[mat], got.at[mat], sems, mat, at.to_x) for mat in range(3)]

    def forward(self, mat):
        self.halve.wait(mat)
        self.send[mat] = self.halve.total(mat, 1 - self.at.x)
        self.along[mat].start()
        self.keep[mat] = self.halve.total(mat, self.at.x)

    def finish(self, outs, first):
        for mat in range(3):
            self.along[mat].wait_recv()
            store_pair(outs[mat], first, self.keep[mat], self.got[mat])
        for copy in self.along:
            copy.wait_send()


def sems(count):
    return [pltpu.SemaphoreType.DMA((count,))] * 2


PACKED = (3, ROWS_DP, 2 * FF)
COLLECT_SCRATCH = [pltpu.VMEM((N_EP, TOK, D), BF16), pltpu.VMEM((6, HALF, D), BF16), pltpu.VMEM((2, HALF, D), BF16)] + sems(6)
HALVE_SCRATCH = [pltpu.VMEM((6, 2, ROWS_DP, FF), BF16)] + sems(6)
ACROSS_SCRATCH = [pltpu.VMEM(PACKED, BF16)] * 3 + sems(3)


ANY = pl.BlockSpec(memory_space=pl.ANY)


def call(kernel, name, ident, ins, outs, scratch, grant):
    return pl.pallas_call(
        kernel, out_shape=outs, scratch_shapes=scratch,
        in_specs=[SMEM if value.shape == (8, 8) else VMEM for value in ins],
        out_specs=jax.tree.map(lambda o: SMEM if o.shape == (8, 8) else VMEM, outs),
        compiler_params=pltpu.CompilerParams(collective_id=ident, has_side_effects=True, vmem_limit_bytes=grant * 1024 * 1024),
        cost_estimate=pl.CostEstimate(flops=10_000_000_000, bytes_accessed=4_000_000, transcendentals=0), name=name)(*ins)


def entry_kernel(own, pack_ref, x_pad, rank_ref, gate_ref, off_ref, packs, every, s_send, s_recv, p_send, p_recv):
    at = Place()
    greet([at.to_y, at.to_z])
    small = [remote(pack_ref, packs.at[1], (p_send, p_recv), 0, at.to_y),
             remote(pack_ref, packs.at[2], (p_send, p_recv), 1, at.to_z),
             remote(packs.at[1], packs.at[3], (p_send, p_recv), 2, at.to_z)]
    small[0].start()
    small[1].start()
    spread = Spread(at, own, every, (s_send, s_recv))
    spread.start()
    packs[0] = pack_ref[...]
    small[0].wait_recv()
    small[2].start()
    small[1].wait_recv()
    small[2].wait_recv()
    route_into(packs, rank_ref, gate_ref, off_ref, at.me)
    spread.forward()
    gather_rows(0, rank_ref, x_pad, 0, own)
    for src in range(1, N_EP):
        spread.arrived(src)
        gather_rows(0, rank_ref, x_pad, src, every.at[src])
    spread.finish()
    for copy in small:
        copy.wait_send()


def middle_kernel(o_ref, u_ref, dense_ref, rank_ref, gate_ref, dy_own, dy_y, dy_z, mid_ref, x_pad, d_pad,
                  part, got, mix_scr, c_send, c_recv, u_scr, every, s_send, s_recv, dy_d, d_send, d_recv):
    at = Place()
    greet([at.to_y, at.to_z])
    collect = Collect(at, part, got, mix_scr, (c_send, c_recv))

    def slot_sum(src):
        return scatter_gated(0, rank_ref, gate_ref, o_ref, src)

    collect.start(slot_sum)
    collect.forward()
    onward = [remote(dy_y.at[TOP_ROWS], dy_d.at[TOP_ROWS], (d_send, d_recv), 0, at.to_z),
              remote(dy_z.at[LOW_ROWS], dy_d.at[LOW_ROWS], (d_send, d_recv), 1, at.to_y)]
    part[0] = slot_sum(0)
    for src, dy_ref in ((0, dy_own), (1, dy_y)):
        gather_scaled(1, rank_ref, gate_ref, d_pad, src, dy_ref)
    collect.summed_gone()
    for copy in onward:
        copy.start()
    top, low = collect.finish(u_ref)
    for rows, half in ((TOP_ROWS, top), (LOW_ROWS, low)):
        u_scr[rows] = (half.astype(F32) + mm(half, dense_ref[...])).astype(BF16)
    spread = Spread(at, u_scr, every, (s_send, s_recv))
    spread.start()
    mid_ref[TOP_ROWS] = top
    mid_ref[LOW_ROWS] = low
    gather_rows(1, rank_ref, x_pad, 0, u_scr)
    gather_scaled(1, rank_ref, gate_ref, d_pad, 2, dy_z)
    spread.forward()
    for copy in onward:
        copy.wait_recv()
    gather_scaled(1, rank_ref, gate_ref, d_pad, 3, dy_d)
    collect.drain()
    for copy in onward:
        copy.wait_send()
    for src in range(1, N_EP):
        spread.arrived(src)
        gather_rows(1, rank_ref, x_pad, src, every.at[src])
    spread.finish()


def dense_grad(x_ref, top, low):
    return mm(x_ref[TOP_ROWS], top, TN) + mm(x_ref[LOW_ROWS], low, TN)


def write_slabs(slabs, value):
    for k in range(16):
        slabs[k // 8, k // 4 % 2, k // 2 % 2, k % 2] = value[24 * k:24 * k + 24].astype(BF16)


class DenseReduce:
    def __init__(self, at, slabs, got_c, sum_c, got_p, sum_p, got_x, sems):
        self.at, self.slabs, self.got_c, self.sum_c, self.got_p, self.sum_p, self.got_x = at, slabs, got_c, sum_c, got_p, sum_p, got_x
        self.pair = remote(slabs.at[:, 1 - at.c], got_c, sems, 0, at.to_c)
        self.plane = [remote(sum_c.at[:, z, y], got_p.at[k], sems, 1 + k, to) for k, (z, y, to) in enumerate((
            (at.z, 1 - at.y, at.to_y), (1 - at.z, at.y, at.to_z), (1 - at.z, 1 - at.y, at.to_d)))]
        self.along = remote(sum_p.at[1 - at.x], got_x, sems, 4, at.to_x)

    def start(self):
        self.pair.start()

    def to_plane(self):
        self.pair.wait_recv()
        for side in range(2):
            self.sum_c[side] = (self.slabs[side, self.at.c].astype(F32) + self.got_c[side].astype(F32)).astype(BF16)
        for copy in self.plane:
            copy.start()

    def to_x(self):
        for copy in self.plane:
            copy.wait_recv()
        for side in range(2):
            total = self.sum_c[side, self.at.z, self.at.y].astype(F32)
            for k in range(3):
                total = total + self.got_p[k, side].astype(F32)
            self.sum_p[side] = total.astype(BF16)
        self.along.start()

    def finish(self, out):
        self.along.wait_recv()
        out[...] = (self.sum_p[self.at.x].astype(F32) + self.got_x[...].astype(F32)).astype(BF16)
        for copy in [self.pair, self.along] + self.plane:
            copy.wait_send()


def dense_scratch():
    slab = lambda *lead: pltpu.VMEM(lead + (24, D), BF16)
    return [slab(2, 2, 2), slab(2, 2, 2), slab(3, 2), slab(2), slab()] + sems(5)


def turn_kernel(gx_ref, dy_ref, dense_ref, mid_ref, rank_ref, gate_ref, grads,
                grad_ref, d_pad, slabs, oa, ob, oc, later_keep, later_send,
                part, got, mix_scr, c_send, c_recv, s_send, s_recv, got_a, a_send, a_recv, got_b, b_send, b_recv,
                keep, send, got_x, x_send, x_recv, g_scr, every):
    at = Place()
    greet([at.to_y, at.to_z, at.to_c, at.to_x])
    now = Halve(at, grads, 0, got_a, (a_send, a_recv))
    later = Halve(at, grads, 2, got_b, (b_send, b_recv))
    now.start()
    collect = Collect(at, part, got, mix_scr, (c_send, c_recv))

    def slot_sum(src):
        return scatter_plain(1, rank_ref, (gx_ref,), src)

    collect.start(slot_sum)
    later.start()
    across = Across(at, now, keep, send, got_x, (x_send, x_recv))
    across.forward(0)
    collect.forward()
    across.forward(1)
    across.forward(2)
    part[0] = slot_sum(0)
    for mat in range(3):
        later.wait(mat)
        later_send[mat] = later.total(mat, 1 - at.x)
        later_keep[mat] = later.total(mat, at.x)
    top, low = collect.finish(dy_ref)
    for rows, half in ((TOP_ROWS, top), (LOW_ROWS, low)):
        g_scr[rows] = (half.astype(F32) + mm(half, dense_ref[...], NT)).astype(BF16)
    spread = Spread(at, g_scr, every, (s_send, s_recv))
    spread.start()
    grad_ref[...] = g_scr[...]
    gather_scaled(0, rank_ref, gate_ref, d_pad, 0, g_scr)
    write_slabs(slabs, dense_grad(mid_ref, top, low))
    spread.forward()
    collect.summed_gone()
    collect.drain()
    now.drain()
    later.drain()
    for src in range(1, N_EP):
        spread.arrived(src)
        if src == 3:
            across.finish((oa, ob, oc), 0)
        gather_scaled(0, rank_ref, gate_ref, d_pad, src, every.at[src])
    spread.finish()


def pair_kernel(grads, later_keep, later_send, got_b, b_send, b_recv):
    at = Place()
    greet([at.to_c])
    later = Halve(at, grads, 0, got_b, (b_send, b_recv))
    later.start()
    for mat in range(3):
        later.wait(mat)
        later_send[mat] = later.total(mat, 1 - at.x)
        later_keep[mat] = later.total(mat, at.x)
    later.drain()


def exit_kernel(gx_a, gx_b, dy_ref, dense_ref, tok_ref, slabs_two, rank_ref, grads, two_keep, two_got, da, db, dc,
                dx_ref, dense_one, dense_two, oa, ob, oc, ta, tb, tc,
                part, got, mix_scr, c_send, c_recv, got_a, a_send, a_recv, keep, send, got_x, x_send, x_recv, slabs_one, *dense):
    at = Place()
    greet([at.to_y, at.to_z, at.to_d, at.to_c, at.to_x])
    now = Halve(at, grads, 0, got_a, (a_send, a_recv))
    now.start()
    half = len(dense) // 2
    first, second = [DenseReduce(at, slabs, *dense[k * half:k * half + 5], dense[k * half + 5:k * half + 7])
                     for k, slabs in enumerate((slabs_one, slabs_two))]
    second.start()
    collect = Collect(at, part, got, mix_scr, (c_send, c_recv))

    def slot_sum(src):
        return scatter_plain(0, rank_ref, (gx_a, gx_b), src)

    collect.start(slot_sum)
    across = Across(at, now, keep, send, got_x, (x_send, x_recv))
    across.forward(0)
    collect.forward()
    second.to_plane()
    across.forward(1)
    across.forward(2)
    part[0] = slot_sum(0)
    for mat, (out, done) in enumerate(((ta, da), (tb, db), (tc, dc))):
        store_pair(out, 2, two_keep[mat], two_got[mat])
        out[0:2] = done[...]
    top, low = collect.finish(dy_ref)
    write_slabs(slabs_one, dense_grad(tok_ref, top, low))
    first.start()
    second.to_x()
    for rows, part_rows in ((TOP_ROWS, top), (LOW_ROWS, low)):
        dx_ref[rows] = (part_rows.astype(F32) + mm(part_rows, dense_ref[...], NT)).astype(BF16)
    first.to_plane()
    collect.summed_gone()
    collect.drain()
    now.drain()
    first.to_x()
    across.finish((oa, ob, oc), 0)
    second.finish(dense_two)
    first.finish(dense_one)


def store_kernel(count, keep, got, *refs):
    values, outs, made, sem = refs[:count], refs[count:2 * count], refs[-2], refs[-1]
    copies = [pltpu.make_async_copy(values[k], outs[k] if k < count - 3 else outs[k].at[2:4], sem.at[k]) for k in range(count)]
    for copy in copies:
        copy.start()
    for mat in range(3):
        store_pair(made.at[mat], 0, keep[mat], got[mat])
        copies.append(pltpu.make_async_copy(made.at[mat], outs[count - 3 + mat].at[0:2], sem.at[count + mat]))
        copies[-1].start()
    for copy in copies:
        copy.wait()


def store_all(keep, got, values):
    count = len(values)
    outs = [block(*value.shape) for value in values[:-3]] + [block(N_LOC, ROWS_DP, FF)] * 3
    return pl.pallas_call(
        functools.partial(store_kernel, count),
        out_shape=outs, in_specs=[VMEM] * (2 + count), out_specs=[ANY] * count,
        scratch_shapes=[pltpu.VMEM((3, 2, ROWS_DP, FF), BF16), pltpu.SemaphoreType.DMA((count + 3,))],
        compiler_params=pltpu.CompilerParams(vmem_limit_bytes=4 * 1024 * 1024),
        cost_estimate=pl.CostEstimate(flops=1_000_000_000, bytes_accessed=4_000_000, transcendentals=0), name='store')(keep, got, *values)


def stored(w_gate, w_up, w_down):
    return jnp.swapaxes(w_gate, 1, 2), jnp.swapaxes(w_up, 1, 2), w_down


def along_x(sent):
    return lax.ppermute(sent, 'dp', [(0, 2), (2, 0), (1, 3), (3, 1)])


def solution(mesh):
    tok_spec = P(('dp', 'ep'), None)
    exp_spec = P('ep', None, None)
    layer_specs = (P(None, None), tok_spec, tok_spec, exp_spec, exp_spec, exp_spec)
    grad_specs = (P(('dp', 'ep'), None), P('ep', 'dp', None), P('ep', 'dp', None), P('ep', None, 'dp'))

    def local_step(tokens, dy_out, dense_w1, route_idx1, route_gate1, w_gate1, w_up1, w_down1, dense_w2, route_idx2, route_gate2, w_gate2, w_up2, w_down2):
        weights_one, weights_two = stored(w_gate1, w_up1, w_down1), stored(w_gate2, w_up2, w_down2)
        tok_block, all_block = block(TOK, D), block(N_EP, TOK, D)
        padded = block(N_LOC, N_EP, CAP, D)
        every = pltpu.VMEM((N_EP, TOK, D), BF16)
        own = pltpu.VMEM((TOK, D), BF16)
        pack = jnp.concatenate([route_idx1.T.astype(F32), route_idx2.T.astype(F32), route_gate1.T, route_gate2.T], axis=0)
        mixed_one = (tokens.astype(F32) + jnp.dot(tokens, dense_w1, preferred_element_type=F32)).astype(BF16)
        x_one, rank, gate, off = call(
            entry_kernel, 'entry', 0, (mixed_one, pack),
            (padded, block(2, N_EP, 8, TOK, dtype=jnp.int32), block(2, N_EP, TOK, 8, dtype=F32), block(8, 8, dtype=jnp.int32)),
            [pltpu.VMEM((N_EP, 16, TOK), F32), every] + sems(6) + sems(3), 12)
        dy_later, x_one = lax.optimization_barrier((dy_out, x_one))
        dy_all = (dy_out,) + tuple(lax.ppermute(dy_later, 'ep', [(k, k ^ flip) for k in range(N_EP)]) for flip in (1, 2))
        outs = expert_forward(0, off, x_one, weights_one)
        mid_tok, x_two, d_two = call(middle_kernel, 'middle', 1, (outs, mixed_one, dense_w2, rank, gate) + dy_all,
                                     (tok_block, padded, padded), COLLECT_SCRATCH + [own, every] + sems(6) + [own] + sems(2), 12)
        gx, grads = expert_backward(1, 0, 4, off, x_two, d_two, weights_two)
        grad_mid, d_one, slabs, *done_two, keep_two, send_two = call(
            turn_kernel, 'turn', 2, (gx, dy_out, dense_w2, mid_tok, rank, gate, grads),
            (tok_block, padded, block(2, 2, 2, 2, 24, D)) + (block(2, ROWS_DP, FF),) * 3 + (block(*PACKED),) * 2,
            COLLECT_SCRATCH + sems(6) + HALVE_SCRATCH * 2 + ACROSS_SCRATCH + [own, every], 18)
        got_two = along_x(send_two)
        gx_a, grads = expert_backward(0, 0, 2, off, x_one, d_one, weights_one)
        keep_one, send_one = call(pair_kernel, 'pair', 4, (grads,), (block(*PACKED),) * 2, HALVE_SCRATCH, 6)
        got_two, d_one = lax.optimization_barrier((got_two, d_one))
        got_one = along_x(send_one)
        gx_b, grads = expert_backward(0, 2, 2, off, x_one, d_one, weights_one)
        grad_tok, dense_one, dense_two, *reduced = call(
            exit_kernel, 'exit', 3, (gx_a, gx_b, grad_mid, dense_w1, tokens, slabs, rank, grads, keep_two, got_two) + tuple(done_two),
            (tok_block, block(24, D), block(24, D)) + (block(2, ROWS_DP, FF),) * 3 + (block(N_LOC, ROWS_DP, FF),) * 3,
            COLLECT_SCRATCH + HALVE_SCRATCH + ACROSS_SCRATCH + [pltpu.VMEM((2, 2, 2, 2, 24, D), BF16)] + dense_scratch() * 2, 18)
        grad_tok, dense_one, dense_two, *reduced = store_all(keep_one, got_one, (grad_tok, dense_one, dense_two) + tuple(reduced[3:]) + tuple(reduced[:3]))

        def shaped(gate_up_down):
            return gate_up_down[0], gate_up_down[1], jnp.swapaxes(gate_up_down[2], 1, 2)

        return (grad_tok, dense_one) + shaped(reduced[3:]) + (dense_two,) + shaped(reduced[:3])

    return jax.shard_map(local_step, mesh=mesh, in_specs=(tok_spec, tok_spec) + layer_specs + layer_specs,
                         out_specs=(tok_spec,) + grad_specs + grad_specs, check_vma=False)
```

```python
import functools

import jax
import jax.numpy as jnp
from jax import lax
from jax.experimental import pallas as pl
from jax.experimental.pallas import tpu as pltpu
from jax.sharding import PartitionSpec as P

BF16 = jnp.bfloat16
F32 = jnp.float32
N_EP = 4
N_LOC = 4
TOK = 512
D = 384
FF = 672
CAP = 256
SLOTS = 5 * CAP
ROWS_DP = D // 4
VMEM = pl.BlockSpec(memory_space=pltpu.VMEM)
SMEM = pl.BlockSpec(memory_space=pltpu.SMEM)


def block(*shape, dtype=BF16):
    return jax.ShapeDtypeStruct(shape, dtype)


def mm(a, b, dims=((1,), (0,))):
    return lax.dot_general(a, b, (dims, ((), ())), preferred_element_type=F32)


NT = ((1,), (1,))
TN = ((0,), (0,))


def route_into(packs, rank_ref, gate_ref, off_ref, me):
    before = (lax.broadcasted_iota(jnp.int32, (TOK, TOK), 0) < lax.broadcasted_iota(jnp.int32, (TOK, TOK), 1)).astype(BF16)
    for layer in range(2):
        running = [jnp.int32(0)] * N_LOC
        last = [jnp.int32(0)] * N_LOC
        for src in range(N_EP):
            ids = packs[src, 4 * layer:4 * layer + 4, :]
            gates = packs[src, 8 + 4 * layer:12 + 4 * layer, :]
            member, gate = [], []
            for exp in range(N_LOC):
                match = ids == (me * N_LOC + exp).astype(F32)
                member.append(jnp.sum(match.astype(F32), axis=0, keepdims=True))
                gate.append(jnp.sum(jnp.where(match, gates, 0.0), axis=0, keepdims=True))
            member = jnp.concatenate(member, axis=0)
            gate = jnp.concatenate(gate + [jnp.zeros((4, TOK), F32)], axis=0)
            rank = mm(member.astype(BF16), before)
            rank = jnp.where(member > 0.5, rank, -1.0).astype(jnp.int32)
            rank_ref[layer, src, 0:4, :] = rank
            gate_ref[layer, src] = jnp.transpose(gate)
            for exp in range(N_LOC):
                count = jnp.max(rank[exp:exp + 1, :]) + 1
                off_ref[layer * N_LOC + exp, src] = running[exp]
                last[exp] = running[exp] + count
                running[exp] = running[exp] + (count + 15) // 16 * 16
        for exp in range(N_LOC):
            halves = (last[exp] + CAP // 2 - 1) // (CAP // 2)
            off_ref[layer * N_LOC + exp, 4] = halves // 2
            off_ref[layer * N_LOC + exp, 5] = halves % 2
            off_ref[layer * N_LOC + exp, 6] = halves * (CAP // 2)
            off_ref[layer * N_LOC + exp, 7] = jnp.maximum((halves + 1) // 2, 2)


def pick(layer, rank_ref, src, exp):
    row = rank_ref[layer, src, pl.ds(exp, 1), :]
    return (lax.broadcasted_iota(jnp.int32, (CAP, TOK), 0) == row).astype(BF16)


def gate_column(layer, gate_ref, src, exp):
    slab = gate_ref[layer, src]
    lane = lax.broadcasted_iota(jnp.int32, slab.shape, 1)
    return jnp.sum(jnp.where(lane == exp, slab, 0.0), axis=1, keepdims=True)


def offset(off_ref, row, src):
    return pl.multiple_of(off_ref[row, src], 16)


def scatter_gated(layer, rank_ref, gate_ref, o_ref, src):
    total = None
    for exp in range(N_LOC):
        term = gate_column(layer, gate_ref, src, exp) * mm(pick(layer, rank_ref, src, exp), o_ref[exp, src], TN)
        total = term if total is None else total + term
    return total.astype(BF16)


def scatter_plain(layer, rank_ref, g_refs, src):
    sel = jnp.concatenate([pick(layer, rank_ref, src, exp) for exp in range(N_LOC)], axis=0)
    per = N_LOC // len(g_refs)
    rows = [g_refs[exp // per][exp % per, src] for exp in range(N_LOC)]
    return mm(sel, jnp.concatenate(rows, axis=0), TN).astype(BF16)


def gather_rows(layer, rank_ref, pad_ref, src, toks):
    @pl.loop(0, N_LOC)
    def _(exp):
        pad_ref[exp, src] = mm(pick(layer, rank_ref, src, exp), toks[...]).astype(BF16)


def gather_scaled(layer, rank_ref, gate_ref, pad_ref, src, toks):
    @pl.loop(0, N_LOC)
    def _(exp):
        scaled = (gate_column(layer, gate_ref, src, exp) * toks[...].astype(F32)).astype(BF16)
        pad_ref[exp, src] = mm(pick(layer, rank_ref, src, exp), scaled).astype(BF16)


def packed(off_ref, row, pad_ref, exp, scr):
    for src in range(N_EP):
        scr[pl.ds(offset(off_ref, row, src), CAP), :] = pad_ref[exp, src]
    scr[pl.ds(offset(off_ref, row, 3) + CAP, CAP), :] = jnp.zeros((CAP, D), BF16)


def over_rows(off_ref, row, step):
    @pl.loop(0, off_ref[row, 4])
    def _(blk):
        step(pl.ds(pl.multiple_of(blk * CAP, CAP), CAP))

    @pl.when(off_ref[row, 5] == 1)
    def _():
        step(pl.ds(pl.multiple_of(off_ref[row, 4] * CAP, CAP), CAP // 2))


def tail_of(off_ref, row, size):
    return pl.ds(pl.multiple_of(off_ref[row, 6], CAP // 2), size)


def unpacked(off_ref, row, scr, out_ref, exp):
    for src in range(N_EP):
        out_ref[exp, src] = scr[pl.ds(offset(off_ref, row, src), CAP), :]


def forward_kernel(layer, off_ref, x_ref, wg_ref, wu_ref, wd_ref, out_ref, x_scr, o_scr):
    @pl.loop(0, N_LOC)
    def _(exp):
        row = layer * N_LOC + exp
        packed(off_ref, row, x_ref, exp, x_scr)

        def step(rows):
            x_blk = x_scr[rows, :]
            a_pre = mm(x_blk, wg_ref[exp], NT)
            b_pre = mm(x_blk, wu_ref[exp], NT)
            hidden = (jax.nn.silu(a_pre) * b_pre).astype(BF16)
            o_scr[rows, :] = mm(hidden, wd_ref[exp]).astype(BF16)

        over_rows(off_ref, row, step)
        o_scr[tail_of(off_ref, row, CAP), :] = jnp.zeros((CAP, D), BF16)
        unpacked(off_ref, row, o_scr, out_ref, exp)


def plain(kernel, name, ins, outs, scratch, grant, flops):
    return pl.pallas_call(
        kernel, out_shape=outs, in_specs=[SMEM] + [VMEM] * (len(ins) - 1), out_specs=jax.tree.map(lambda _: VMEM, outs),
        scratch_shapes=scratch, compiler_params=pltpu.CompilerParams(vmem_limit_bytes=grant * 1024 * 1024),
        cost_estimate=pl.CostEstimate(flops=flops, bytes_accessed=10_000_000, transcendentals=0), name=name)(*ins)


def expert_forward(layer, off, x_pad, weights):
    return plain(functools.partial(forward_kernel, layer), 'expert_forward', (off, x_pad) + weights, block(N_LOC, N_EP, CAP, D),
                 [pltpu.VMEM((SLOTS, D), BF16)] * 2, 8, 10_000_000_000)


def backward_kernel(layer, first, count, done, off_ref, x_ref, d_ref, wg_ref, wu_ref, wd_ref, out_ref, *refs):
    grad_ref = refs[0] if done else None
    left, right, gx_scr = refs[-3:]

    @pl.loop(first, first + count)
    def _(exp):
        row = layer * N_LOC + exp
        slot = jnp.maximum(exp - first - done, 0)
        x_scr, d_scr = left.at[slot, 0], left.at[slot, 1]
        packed(off_ref, row, x_ref, exp, x_scr)
        packed(off_ref, row, d_ref, exp, d_scr)

        def step(rows):
            x_blk = x_scr[rows, :]
            a_pre = mm(x_blk, wg_ref[exp], NT)
            b_pre = mm(x_blk, wu_ref[exp], NT)
            grad_h = mm(d_scr[rows, :], wd_ref[exp], NT).astype(BF16).astype(F32)
            sigma = jax.nn.sigmoid(a_pre)
            swish = a_pre * sigma
            grad_a = (grad_h * b_pre * sigma * (1.0 + a_pre * (1.0 - sigma))).astype(BF16)
            grad_b = (grad_h * swish).astype(BF16)
            right[slot, 0, rows, :] = grad_a
            right[slot, 1, rows, :] = grad_b
            right[slot, 2, rows, :] = (swish * b_pre).astype(BF16)
            gx_scr[rows, :] = (mm(grad_a, wg_ref[exp]) + mm(grad_b, wu_ref[exp])).astype(BF16)

        over_rows(off_ref, row, step)
        gx_scr[tail_of(off_ref, row, CAP), :] = jnp.zeros((CAP, D), BF16)
        unpacked(off_ref, row, gx_scr, out_ref, exp - first)
        depth, half = off_ref[row, 7], CAP // 2
        made_here = exp < first + done

        @pl.loop(off_ref[row, 4] * 2 + off_ref[row, 5], jnp.where(made_here, depth * 2, N_EP * 2))
        def _(k):
            rows = pl.ds(pl.multiple_of(k * half, half), half)
            right[slot, :, rows, :] = jnp.zeros((3, half, FF), BF16)
            left[slot, :, rows, :] = jnp.zeros((2, half, D), BF16)

        if done:
            for blocks in range(2, 5):
                pl.when(jnp.logical_and(made_here, depth == blocks))(
                    functools.partial(weight_grads, left, right, slot, grad_ref, exp - first, blocks * CAP))


def weight_grads(left, right, slot, grad_ref, exp, depth):
    @pl.loop(0, 3)
    def _(mat):
        grad = mm(left[slot, mat // 2, 0:depth, :], right[slot, mat, 0:depth, :], TN).astype(BF16)
        for owner in range(4):
            grad_ref[exp, mat, owner // 2, owner % 2] = grad[ROWS_DP * owner:ROWS_DP * owner + ROWS_DP]


def grads_shape(count):
    return (count, 3, 2, 2, ROWS_DP, FF)


def expert_backward(layer, first, count, done, off, x_pad, d_pad, weights):
    slots = max(count - done, 1)
    factors = ((slots, 2, SLOTS, D), (slots, 3, N_EP * CAP, FF))
    outs = (block(count, N_EP, CAP, D),) + ((block(*grads_shape(done)),) if done else ())
    scratch = [pltpu.VMEM((SLOTS, D), BF16)]
    if count > done:
        outs += tuple(block(*shape) for shape in factors)
    else:
        scratch = [pltpu.VMEM(shape, BF16) for shape in factors] + scratch
    return plain(functools.partial(backward_kernel, layer, first, count, done), 'expert_backward',
                 (off, x_pad, d_pad) + weights, outs, scratch, 12 if count == done else 6, 9_000_000_000 * count)


def remote(src, dst, sems, slot, target):
    send, recv = sems
    return pltpu.make_async_remote_copy(src_ref=src, dst_ref=dst, send_sem=send.at[slot], recv_sem=recv.at[slot],
                                        device_id=target, device_id_type=pl.DeviceIdType.MESH)


class Place:
    def __init__(self):
        ep, dp = lax.axis_index('ep'), lax.axis_index('dp')
        self.me = ep
        self.z, self.y = ep // 2, ep % 2
        self.x, self.c = dp // 2, dp % 2
        self.to_y, self.to_z = {'ep': self.z * 2 + 1 - self.y}, {'ep': (1 - self.z) * 2 + self.y}
        self.to_d = {'ep': (1 - self.z) * 2 + 1 - self.y}
        self.to_c, self.to_x = {'dp': self.x * 2 + 1 - self.c}, {'dp': (1 - self.x) * 2 + self.c}


def greet(targets):
    barrier = pltpu.get_barrier_semaphore()
    for target in targets:
        pl.semaphore_signal(barrier, inc=1, device_id=target, device_id_type=pl.DeviceIdType.MESH)
    pl.semaphore_wait(barrier, len(targets))


HALF = TOK // 2
QUARTER = TOK // 4
SETS = (pl.ds(0, HALF), pl.ds(HALF, HALF))


class Spread:
    def __init__(self, at, own, every, sems, k):
        top, low = pl.ds(HALF * k, QUARTER), pl.ds(HALF * k + QUARTER, QUARTER)
        first = 6 * k
        self.direct = [remote(own.at[top], every.at[1, top], sems, first, at.to_y),
                       remote(own.at[low], every.at[2, low], sems, first + 1, at.to_z),
                       remote(own.at[low], every.at[1, low], sems, first + 2, at.to_y),
                       remote(own.at[top], every.at[2, top], sems, first + 3, at.to_z)]
        self.onward = [remote(every.at[1, top], every.at[3, top], sems, first + 4, at.to_z),
                       remote(every.at[2, low], every.at[3, low], sems, first + 5, at.to_y)]

    def start(self):
        for copy in self.direct:
            copy.start()

    def forward(self):
        for first, then in zip(self.direct, self.onward):
            first.wait_recv()
            then.start()

    def arrived(self, slot):
        for copy in ((), self.direct[2:3], self.direct[3:4], self.onward)[slot]:
            copy.wait_recv()

    def finish(self):
        for copy in self.direct + self.onward:
            copy.wait_send()


class Both:
    def __init__(self, first, second):
        self.sets = (first, second)

    def __getattr__(self, name):
        def each(*args):
            for one in self.sets:
                getattr(one, name)(*args)
        return each


class Collect:
    def __init__(self, at, part, got, mix_scr, sems, k):
        self.part, self.got, self.mix_scr, self.k = part, got, mix_scr, k
        self.top, self.low = pl.ds(HALF * k, QUARTER), pl.ds(HALF * k + QUARTER, QUARTER)
        self.first = first = 6 * k
        self.direct = [remote(part.at[3, self.top], got.at[first], sems, first, at.to_y),
                       remote(part.at[3, self.low], got.at[first + 1], sems, first + 1, at.to_z),
                       remote(part.at[1, self.top], got.at[first + 2], sems, first + 2, at.to_y),
                       remote(part.at[2, self.low], got.at[first + 3], sems, first + 3, at.to_z)]
        self.summed = [remote(mix_scr.at[2 * k], got.at[first + 4], sems, first + 4, at.to_z),
                       remote(mix_scr.at[2 * k + 1], got.at[first + 5], sems, first + 5, at.to_y)]

    def far(self):
        self.direct[0].start()
        self.direct[1].start()

    def near_y(self):
        self.direct[2].start()

    def near_z(self):
        self.direct[3].start()

    def forward(self):
        for step, (slot, rows) in enumerate(((2, self.top), (1, self.low))):
            self.direct[step].wait_recv()
            self.mix_scr[2 * self.k + step] = (self.part[slot, rows].astype(F32) + self.got[self.first + step].astype(F32)).astype(BF16)
            self.summed[step].start()

    def finish(self, base):
        for copy in self.direct[2:] + self.summed:
            copy.wait_recv()
        got, first = self.got, self.first
        top = self.part[0, self.top].astype(F32) + got[first + 2].astype(F32) + got[first + 4].astype(F32)
        low = self.part[0, self.low].astype(F32) + got[first + 3].astype(F32) + got[first + 5].astype(F32)
        return (base[SETS[self.k]].astype(F32) + jnp.concatenate([top, low], axis=0)).astype(BF16)

    def summed_gone(self):
        for copy in self.summed:
            copy.wait_send()

    def drain(self):
        for copy in self.direct:
            copy.wait_send()


def start_collect(at, part, got, mix_scr, sems, slot_sum):
    both = Both(*[Collect(at, part, got, mix_scr, sems, k) for k in range(2)])
    part[3] = slot_sum(3)
    both.far()
    part[1] = slot_sum(1)
    both.near_y()
    part[2] = slot_sum(2)
    both.near_z()
    return both


def spread_of(at, own, every, sems):
    return Both(*[Spread(at, own, every, sems, k) for k in range(2)])


class Halve:
    def __init__(self, at, grads, first, got, sems):
        self.at, self.grads, self.first, self.got = at, grads, first, got
        self.pair = [remote(grads.at[first + k % 2, k // 2, :, 1 - at.c], got.at[k], sems, k, at.to_c) for k in range(6)]

    def start(self, exp):
        for copy in self.pair[exp::2]:
            copy.start()

    def total(self, mat, side):
        return jnp.concatenate([self.grads[self.first + exp, mat, side, self.at.c].astype(F32) + self.got[2 * mat + exp, side].astype(F32)
                                for exp in range(2)], axis=1).astype(BF16)

    def wait(self, mat):
        for exp in range(2):
            self.pair[2 * mat + exp].wait_recv()

    def drain(self):
        for copy in self.pair:
            copy.wait_send()


def store_pair(out, first, keep, got):
    total = (keep.astype(F32) + got.astype(F32)).astype(BF16)
    for exp in range(2):
        out[first + exp] = total[:, FF * exp:FF * exp + FF]


class Across:
    def __init__(self, at, halve, keep, send, got, sems):
        self.at, self.halve, self.keep, self.send, self.got = at, halve, keep, send, got
        self.along = [remote(send.at[mat], got.at[mat], sems, mat, at.to_x) for mat in range(3)]

    def forward(self, mat):
        self.halve.wait(mat)
        self.send[mat] = self.halve.total(mat, 1 - self.at.x)
        self.along[mat].start()
        self.keep[mat] = self.halve.total(mat, self.at.x)

    def finish(self, outs, first):
        for mat in range(3):
            self.along[mat].wait_recv()
            store_pair(outs[mat], first, self.keep[mat], self.got[mat])
        for copy in self.along:
            copy.wait_send()


def sems(count):
    return [pltpu.SemaphoreType.DMA((count,))] * 2


PACKED = (3, ROWS_DP, 2 * FF)
COLLECT_SCRATCH = [pltpu.VMEM((N_EP, TOK, D), BF16), pltpu.VMEM((12, QUARTER, D), BF16), pltpu.VMEM((4, QUARTER, D), BF16)] + sems(12)
HALVE_SCRATCH = [pltpu.VMEM((6, 2, ROWS_DP, FF), BF16)] + sems(6)
ACROSS_SCRATCH = [pltpu.VMEM(PACKED, BF16)] * 3 + sems(3)


ANY = pl.BlockSpec(memory_space=pl.ANY)


def call(kernel, name, ident, ins, outs, scratch, grant):
    return pl.pallas_call(
        kernel, out_shape=outs, scratch_shapes=scratch,
        in_specs=[SMEM if value.shape == (8, 8) else VMEM for value in ins],
        out_specs=jax.tree.map(lambda o: SMEM if o.shape == (8, 8) else VMEM, outs),
        compiler_params=pltpu.CompilerParams(collective_id=ident, has_side_effects=True, vmem_limit_bytes=grant * 1024 * 1024),
        cost_estimate=pl.CostEstimate(flops=10_000_000_000, bytes_accessed=4_000_000, transcendentals=0), name=name)(*ins)


def entry_kernel(own, pack_ref, x_pad, rank_ref, gate_ref, off_ref, packs, every, s_send, s_recv, p_send, p_recv):
    at = Place()
    greet([at.to_y, at.to_z])
    small = [remote(pack_ref, packs.at[1], (p_send, p_recv), 0, at.to_y),
             remote(pack_ref, packs.at[2], (p_send, p_recv), 1, at.to_z),
             remote(packs.at[1], packs.at[3], (p_send, p_recv), 2, at.to_z)]
    small[0].start()
    small[1].start()
    spread = spread_of(at, own, every, (s_send, s_recv))
    spread.start()
    packs[0] = pack_ref[...]
    small[0].wait_recv()
    small[2].start()
    small[1].wait_recv()
    small[2].wait_recv()
    route_into(packs, rank_ref, gate_ref, off_ref, at.me)
    spread.forward()
    gather_rows(0, rank_ref, x_pad, 0, own)
    for src in range(1, N_EP):
        spread.arrived(src)
        gather_rows(0, rank_ref, x_pad, src, every.at[src])
    spread.finish()
    for copy in small:
        copy.wait_send()


def middle_kernel(o_ref, u_ref, dense_ref, rank_ref, gate_ref, dy_own, dy_y, dy_z, mid_ref, x_pad, d_pad,
                  part, got, mix_scr, c_send, c_recv, u_scr, every, s_send, s_recv, dy_d, d_send, d_recv):
    at = Place()
    greet([at.to_y, at.to_z])

    def slot_sum(src):
        return scatter_gated(0, rank_ref, gate_ref, o_ref, src)

    collect = start_collect(at, part, got, mix_scr, (c_send, c_recv), slot_sum)
    collect.forward()
    onward = [remote(dy_y.at[SETS[0]], dy_d.at[SETS[0]], (d_send, d_recv), 0, at.to_z),
              remote(dy_z.at[SETS[1]], dy_d.at[SETS[1]], (d_send, d_recv), 1, at.to_y)]
    part[0] = slot_sum(0)
    for src, dy_ref in ((0, dy_own), (1, dy_y)):
        gather_scaled(1, rank_ref, gate_ref, d_pad, src, dy_ref)
    collect.summed_gone()
    for copy in onward:
        copy.start()
    spread = spread_of(at, u_scr, every, (s_send, s_recv))
    for k, rows in enumerate(SETS):
        mid = collect.sets[k].finish(u_ref)
        u_scr[rows] = (mid.astype(F32) + mm(mid, dense_ref[...])).astype(BF16)
        spread.sets[k].start()
        mid_ref[rows] = mid
    gather_rows(1, rank_ref, x_pad, 0, u_scr)
    gather_scaled(1, rank_ref, gate_ref, d_pad, 2, dy_z)
    spread.forward()
    for copy in onward:
        copy.wait_recv()
    gather_scaled(1, rank_ref, gate_ref, d_pad, 3, dy_d)
    collect.drain()
    for copy in onward:
        copy.wait_send()
    for src in range(1, N_EP):
        spread.arrived(src)
        gather_rows(1, rank_ref, x_pad, src, every.at[src])
    spread.finish()


def dense_grad(x_ref, halves):
    return mm(x_ref[SETS[0]], halves[0], TN) + mm(x_ref[SETS[1]], halves[1], TN)


def write_slabs(slabs, value):
    for k in range(16):
        slabs[k // 8, k // 4 % 2, k // 2 % 2, k % 2] = value[24 * k:24 * k + 24].astype(BF16)


class DenseReduce:
    def __init__(self, at, slabs, got_c, sum_c, got_p, sum_p, got_x, sems):
        self.at, self.slabs, self.got_c, self.sum_c, self.got_p, self.sum_p, self.got_x = at, slabs, got_c, sum_c, got_p, sum_p, got_x
        self.pair = remote(slabs.at[:, 1 - at.c], got_c, sems, 0, at.to_c)
        self.plane = [remote(sum_c.at[:, z, y], got_p.at[k], sems, 1 + k, to) for k, (z, y, to) in enumerate((
            (at.z, 1 - at.y, at.to_y), (1 - at.z, at.y, at.to_z), (1 - at.z, 1 - at.y, at.to_d)))]
        self.along = remote(sum_p.at[1 - at.x], got_x, sems, 4, at.to_x)

    def start(self):
        self.pair.start()

    def to_plane(self):
        self.pair.wait_recv()
        for side in range(2):
            self.sum_c[side] = (self.slabs[side, self.at.c].astype(F32) + self.got_c[side].astype(F32)).astype(BF16)
        for copy in self.plane:
            copy.start()

    def to_x(self):
        for copy in self.plane:
            copy.wait_recv()
        for side in range(2):
            total = self.sum_c[side, self.at.z, self.at.y].astype(F32)
            for k in range(3):
                total = total + self.got_p[k, side].astype(F32)
            self.sum_p[side] = total.astype(BF16)
        self.along.start()

    def finish(self, out):
        self.along.wait_recv()
        out[...] = (self.sum_p[self.at.x].astype(F32) + self.got_x[...].astype(F32)).astype(BF16)
        for copy in [self.pair, self.along] + self.plane:
            copy.wait_send()


def dense_scratch():
    slab = lambda *lead: pltpu.VMEM(lead + (24, D), BF16)
    return [slab(2, 2, 2), slab(2, 2, 2), slab(3, 2), slab(2), slab()] + sems(5)


def turn_kernel(gx_ref, dy_ref, dense_ref, mid_ref, rank_ref, gate_ref, grads, left, right,
                grad_ref, d_pad, slabs, oa, ob, oc, later_keep, later_send,
                part, got, mix_scr, c_send, c_recv, s_send, s_recv, got_a, a_send, a_recv, got_b, b_send, b_recv,
                keep, send, got_x, x_send, x_recv, g_scr, every, later_grads):
    at = Place()
    greet([at.to_y, at.to_z, at.to_c, at.to_x])
    now = Halve(at, grads, 0, got_a, (a_send, a_recv))
    later = Halve(at, later_grads, 0, got_b, (b_send, b_recv))
    now.start(0)
    now.start(1)

    def slot_sum(src):
        return scatter_plain(1, rank_ref, (gx_ref,), src)

    collect = start_collect(at, part, got, mix_scr, (c_send, c_recv), slot_sum)
    across = Across(at, now, keep, send, got_x, (x_send, x_recv))
    across.forward(0)
    collect.forward()
    across.forward(1)
    across.forward(2)
    part[0] = slot_sum(0)
    for exp in range(2):
        weight_grads(left, right, exp, later_grads, exp, N_EP * CAP)
        later.start(exp)
    spread = spread_of(at, g_scr, every, (s_send, s_recv))
    halves = []
    for k, rows in enumerate(SETS):
        halves.append(collect.sets[k].finish(dy_ref))
        g_scr[rows] = (halves[k].astype(F32) + mm(halves[k], dense_ref[...], NT)).astype(BF16)
        spread.sets[k].start()
        grad_ref[rows] = g_scr[rows]
    gather_scaled(0, rank_ref, gate_ref, d_pad, 0, g_scr)
    write_slabs(slabs, dense_grad(mid_ref, halves))
    spread.forward()
    for mat in range(3):
        later.wait(mat)
        later_send[mat] = later.total(mat, 1 - at.x)
        later_keep[mat] = later.total(mat, at.x)
    collect.summed_gone()
    collect.drain()
    now.drain()
    later.drain()
    for src in range(1, N_EP):
        spread.arrived(src)
        if src == 3:
            across.finish((oa, ob, oc), 0)
        gather_scaled(0, rank_ref, gate_ref, d_pad, src, every.at[src])
    spread.finish()


def pair_kernel(grads, later_keep, later_send, got_b, b_send, b_recv):
    at = Place()
    greet([at.to_c])
    later = Halve(at, grads, 0, got_b, (b_send, b_recv))
    later.start(0)
    later.start(1)
    for mat in range(3):
        later.wait(mat)
        later_send[mat] = later.total(mat, 1 - at.x)
        later_keep[mat] = later.total(mat, at.x)
    later.drain()


def exit_kernel(gx_a, gx_b, dy_ref, dense_ref, tok_ref, slabs_two, rank_ref, grads, two_keep, two_got, da, db, dc,
                dx_ref, dense_one, dense_two, oa, ob, oc, ta, tb, tc,
                part, got, mix_scr, c_send, c_recv, got_a, a_send, a_recv, keep, send, got_x, x_send, x_recv, slabs_one, *dense):
    at = Place()
    greet([at.to_y, at.to_z, at.to_d, at.to_c, at.to_x])
    now = Halve(at, grads, 0, got_a, (a_send, a_recv))
    now.start(0)
    now.start(1)
    half = len(dense) // 2
    first, second = [DenseReduce(at, slabs, *dense[k * half:k * half + 5], dense[k * half + 5:k * half + 7])
                     for k, slabs in enumerate((slabs_one, slabs_two))]
    second.start()

    def slot_sum(src):
        return scatter_plain(0, rank_ref, (gx_a, gx_b), src)

    collect = start_collect(at, part, got, mix_scr, (c_send, c_recv), slot_sum)
    across = Across(at, now, keep, send, got_x, (x_send, x_recv))
    across.forward(0)
    collect.forward()
    second.to_plane()
    across.forward(1)
    across.forward(2)
    part[0] = slot_sum(0)
    for mat, (out, done) in enumerate(((ta, da), (tb, db), (tc, dc))):
        store_pair(out, 2, two_keep[mat], two_got[mat])
        out[0:2] = done[...]
    halves = [one.finish(dy_ref) for one in collect.sets]
    write_slabs(slabs_one, dense_grad(tok_ref, halves))
    first.start()
    second.to_x()
    for rows, half_rows in zip(SETS, halves):
        dx_ref[rows] = (half_rows.astype(F32) + mm(half_rows, dense_ref[...], NT)).astype(BF16)
    first.to_plane()
    collect.summed_gone()
    collect.drain()
    now.drain()
    first.to_x()
    across.finish((oa, ob, oc), 0)
    second.finish(dense_two)
    first.finish(dense_one)


def store_kernel(count, keep, got, *refs):
    values, outs, made, sem = refs[:count], refs[count:2 * count], refs[-2], refs[-1]
    copies = [pltpu.make_async_copy(values[k], outs[k] if k < count - 3 else outs[k].at[2:4], sem.at[k]) for k in range(count)]
    for copy in copies:
        copy.start()
    for mat in range(3):
        store_pair(made.at[mat], 0, keep[mat], got[mat])
        copies.append(pltpu.make_async_copy(made.at[mat], outs[count - 3 + mat].at[0:2], sem.at[count + mat]))
        copies[-1].start()
    for copy in copies:
        copy.wait()


def store_all(keep, got, values):
    count = len(values)
    outs = [block(*value.shape) for value in values[:-3]] + [block(N_LOC, ROWS_DP, FF)] * 3
    return pl.pallas_call(
        functools.partial(store_kernel, count),
        out_shape=outs, in_specs=[VMEM] * (2 + count), out_specs=[ANY] * count,
        scratch_shapes=[pltpu.VMEM((3, 2, ROWS_DP, FF), BF16), pltpu.SemaphoreType.DMA((count + 3,))],
        compiler_params=pltpu.CompilerParams(vmem_limit_bytes=4 * 1024 * 1024),
        cost_estimate=pl.CostEstimate(flops=1_000_000_000, bytes_accessed=4_000_000, transcendentals=0), name='store')(keep, got, *values)


def stored(w_gate, w_up, w_down):
    return jnp.swapaxes(w_gate, 1, 2), jnp.swapaxes(w_up, 1, 2), w_down


def along_x(sent):
    return lax.ppermute(sent, 'dp', [(0, 2), (2, 0), (1, 3), (3, 1)])


def solution(mesh):
    tok_spec = P(('dp', 'ep'), None)
    exp_spec = P('ep', None, None)
    layer_specs = (P(None, None), tok_spec, tok_spec, exp_spec, exp_spec, exp_spec)
    grad_specs = (P(('dp', 'ep'), None), P('ep', 'dp', None), P('ep', 'dp', None), P('ep', None, 'dp'))

    def local_step(tokens, dy_out, dense_w1, route_idx1, route_gate1, w_gate1, w_up1, w_down1, dense_w2, route_idx2, route_gate2, w_gate2, w_up2, w_down2):
        weights_one, weights_two = stored(w_gate1, w_up1, w_down1), stored(w_gate2, w_up2, w_down2)
        tok_block, all_block = block(TOK, D), block(N_EP, TOK, D)
        padded = block(N_LOC, N_EP, CAP, D)
        every = pltpu.VMEM((N_EP, TOK, D), BF16)
        own = pltpu.VMEM((TOK, D), BF16)
        pack = jnp.concatenate([route_idx1.T.astype(F32), route_idx2.T.astype(F32), route_gate1.T, route_gate2.T], axis=0)
        mixed_one = (tokens.astype(F32) + jnp.dot(tokens, dense_w1, preferred_element_type=F32)).astype(BF16)
        x_one, rank, gate, off = call(
            entry_kernel, 'entry', 0, (mixed_one, pack),
            (padded, block(2, N_EP, 8, TOK, dtype=jnp.int32), block(2, N_EP, TOK, 8, dtype=F32), block(8, 8, dtype=jnp.int32)),
            [pltpu.VMEM((N_EP, 16, TOK), F32), every] + sems(12) + sems(3), 12)
        dy_later, x_one = lax.optimization_barrier((dy_out, x_one))
        dy_all = (dy_out,) + tuple(lax.ppermute(dy_later, 'ep', [(k, k ^ flip) for k in range(N_EP)]) for flip in (1, 2))
        outs = expert_forward(0, off, x_one, weights_one)
        mid_tok, x_two, d_two = call(middle_kernel, 'middle', 1, (outs, mixed_one, dense_w2, rank, gate) + dy_all,
                                     (tok_block, padded, padded), COLLECT_SCRATCH + [own, every] + sems(12) + [own] + sems(2), 9)
        gx, grads, left, right = expert_backward(1, 0, 4, 2, off, x_two, d_two, weights_two)
        grad_mid, d_one, slabs, *done_two, keep_two, send_two = call(
            turn_kernel, 'turn', 2, (gx, dy_out, dense_w2, mid_tok, rank, gate, grads, left, right),
            (tok_block, padded, block(2, 2, 2, 2, 24, D)) + (block(2, ROWS_DP, FF),) * 3 + (block(*PACKED),) * 2,
            COLLECT_SCRATCH + sems(12) + HALVE_SCRATCH * 2 + ACROSS_SCRATCH + [own, every, pltpu.VMEM(grads_shape(2), BF16)], 17)
        got_two = along_x(send_two)
        gx_a, grads = expert_backward(0, 0, 2, 2, off, x_one, d_one, weights_one)
        keep_one, send_one = call(pair_kernel, 'pair', 4, (grads,), (block(*PACKED),) * 2, HALVE_SCRATCH, 6)
        got_two, d_one = lax.optimization_barrier((got_two, d_one))
        got_one = along_x(send_one)
        gx_b, grads = expert_backward(0, 2, 2, 2, off, x_one, d_one, weights_one)
        grad_tok, dense_one, dense_two, *reduced = call(
            exit_kernel, 'exit', 3, (gx_a, gx_b, grad_mid, dense_w1, tokens, slabs, rank, grads, keep_two, got_two) + tuple(done_two),
            (tok_block, block(24, D), block(24, D)) + (block(2, ROWS_DP, FF),) * 3 + (block(N_LOC, ROWS_DP, FF),) * 3,
            COLLECT_SCRATCH + HALVE_SCRATCH + ACROSS_SCRATCH + [pltpu.VMEM((2, 2, 2, 2, 24, D), BF16)] + dense_scratch() * 2, 14)
        grad_tok, dense_one, dense_two, *reduced = store_all(keep_one, got_one, (grad_tok, dense_one, dense_two) + tuple(reduced[3:]) + tuple(reduced[:3]))

        def shaped(gate_up_down):
            return gate_up_down[0], gate_up_down[1], jnp.swapaxes(gate_up_down[2], 1, 2)

        return (grad_tok, dense_one) + shaped(reduced[3:]) + (dense_two,) + shaped(reduced[:3])

    return jax.shard_map(local_step, mesh=mesh, in_specs=(tok_spec, tok_spec) + layer_specs + layer_specs,
                         out_specs=(tok_spec,) + grad_specs + grad_specs, check_vma=False)
```

```python
import functools

import jax
import jax.numpy as jnp
from jax import lax
from jax.experimental import pallas as pl
from jax.experimental.pallas import tpu as pltpu
from jax.sharding import PartitionSpec as P

BF16 = jnp.bfloat16
F32 = jnp.float32
N_EP = 4
N_LOC = 4
TOK = 512
D = 384
FF = 672
CAP = 256
SLOTS = 5 * CAP
HALF = TOK // 2
QUARTER = TOK // 4
SETS = (pl.ds(0, HALF), pl.ds(HALF, HALF))
ALL = pl.ds(0, TOK)
ROWS_DP = D // 4
VMEM = pl.BlockSpec(memory_space=pltpu.VMEM)
SMEM = pl.BlockSpec(memory_space=pltpu.SMEM)


def block(*shape, dtype=BF16):
    return jax.ShapeDtypeStruct(shape, dtype)


def mm(a, b, dims=((1,), (0,))):
    return lax.dot_general(a, b, (dims, ((), ())), preferred_element_type=F32)


NT = ((1,), (1,))
TN = ((0,), (0,))


def route_into(packs, rank_ref, gate_ref, off_ref, me):
    before = (lax.broadcasted_iota(jnp.int32, (TOK, TOK), 0) < lax.broadcasted_iota(jnp.int32, (TOK, TOK), 1)).astype(BF16)
    for layer in range(2):
        running = [jnp.int32(0)] * N_LOC
        last = [jnp.int32(0)] * N_LOC
        for src in range(N_EP):
            ids = packs[src, 4 * layer:4 * layer + 4, :]
            gates = packs[src, 8 + 4 * layer:12 + 4 * layer, :]
            member, gate = [], []
            for exp in range(N_LOC):
                match = ids == (me * N_LOC + exp).astype(F32)
                member.append(jnp.sum(match.astype(F32), axis=0, keepdims=True))
                gate.append(jnp.sum(jnp.where(match, gates, 0.0), axis=0, keepdims=True))
            member = jnp.concatenate(member, axis=0)
            gate = jnp.concatenate(gate + [jnp.zeros((4, TOK), F32)], axis=0)
            rank = mm(member.astype(BF16), before)
            rank = jnp.where(member > 0.5, rank, -1.0).astype(jnp.int32)
            rank_ref[layer, src, 0:4, :] = rank
            gate_ref[layer, src] = jnp.transpose(gate)
            for exp in range(N_LOC):
                count = jnp.max(rank[exp:exp + 1, :]) + 1
                off_ref[layer * N_LOC + exp, src] = running[exp]
                last[exp] = running[exp] + count
                running[exp] = running[exp] + (count + 15) // 16 * 16
        for exp in range(N_LOC):
            halves = (last[exp] + CAP // 2 - 1) // (CAP // 2)
            off_ref[layer * N_LOC + exp, 4] = halves // 2
            off_ref[layer * N_LOC + exp, 5] = halves % 2
            off_ref[layer * N_LOC + exp, 6] = halves * (CAP // 2)
            off_ref[layer * N_LOC + exp, 7] = jnp.maximum((halves + 1) // 2, 2)


def pick(layer, rank_ref, src, exp, toks=ALL):
    row = rank_ref[layer, src, pl.ds(exp, 1), toks]
    return (lax.broadcasted_iota(jnp.int32, (CAP, toks.size), 0) == row).astype(BF16)


def gate_column(layer, gate_ref, src, exp, toks=ALL):
    slab = gate_ref[layer, src, toks]
    lane = lax.broadcasted_iota(jnp.int32, slab.shape, 1)
    return jnp.sum(jnp.where(lane == exp, slab, 0.0), axis=1, keepdims=True)


def offset(off_ref, row, src):
    return pl.multiple_of(off_ref[row, src], 16)


def scatter_gated(layer, rank_ref, gate_ref, o_ref, src, toks):
    total = None
    for exp in range(N_LOC):
        term = gate_column(layer, gate_ref, src, exp, toks) * mm(pick(layer, rank_ref, src, exp, toks), o_ref[exp, src], TN)
        total = term if total is None else total + term
    return total.astype(BF16)


def scatter_plain(layer, rank_ref, g_refs, src, toks):
    sel = jnp.concatenate([pick(layer, rank_ref, src, exp, toks) for exp in range(N_LOC)], axis=0)
    per = N_LOC // len(g_refs)
    rows = [g_refs[exp // per][exp % per, src] for exp in range(N_LOC)]
    return mm(sel, jnp.concatenate(rows, axis=0), TN).astype(BF16)


def gather_rows(layer, rank_ref, pad_ref, src, block_ref, toks=ALL, gate_ref=None, more=False):
    @pl.loop(0, N_LOC)
    def _(exp):
        rows = block_ref[toks]
        if gate_ref is not None:
            rows = (gate_column(layer, gate_ref, src, exp, toks) * rows.astype(F32)).astype(BF16)
        picked = mm(pick(layer, rank_ref, src, exp, toks), rows)
        if more:
            picked = pad_ref[exp, src].astype(F32) + picked
        pad_ref[exp, src] = picked.astype(BF16)


def gather_others(spread, layer, rank_ref, pad_ref, every, gate_ref=None):
    for src in (1, 2):
        spread.arrived(src)
        gather_rows(layer, rank_ref, pad_ref, src, every.at[src], ALL, gate_ref)
    for k, toks in enumerate(SETS):
        spread.sets[k].arrived(3)
        gather_rows(layer, rank_ref, pad_ref, 3, every.at[3], toks, gate_ref, k == 1)


def packed(off_ref, row, pad_ref, exp, scr):
    for src in range(N_EP):
        scr[pl.ds(offset(off_ref, row, src), CAP), :] = pad_ref[exp, src]
    scr[pl.ds(offset(off_ref, row, 3) + CAP, CAP), :] = jnp.zeros((CAP, D), BF16)


def over_rows(off_ref, row, step):
    @pl.loop(0, off_ref[row, 4])
    def _(blk):
        step(pl.ds(pl.multiple_of(blk * CAP, CAP), CAP))

    @pl.when(off_ref[row, 5] == 1)
    def _():
        step(pl.ds(pl.multiple_of(off_ref[row, 4] * CAP, CAP), CAP // 2))


def tail_of(off_ref, row, size):
    return pl.ds(pl.multiple_of(off_ref[row, 6], CAP // 2), size)


def unpacked(off_ref, row, scr, out_ref, exp):
    for src in range(N_EP):
        out_ref[exp, src] = scr[pl.ds(offset(off_ref, row, src), CAP), :]


def forward_kernel(layer, off_ref, x_ref, wg_ref, wu_ref, wd_ref, out_ref, x_scr, o_scr):
    @pl.loop(0, N_LOC)
    def _(exp):
        row = layer * N_LOC + exp
        packed(off_ref, row, x_ref, exp, x_scr)

        def step(rows):
            x_blk = x_scr[rows, :]
            a_pre = mm(x_blk, wg_ref[exp], NT)
            b_pre = mm(x_blk, wu_ref[exp], NT)
            hidden = (jax.nn.silu(a_pre) * b_pre).astype(BF16)
            o_scr[rows, :] = mm(hidden, wd_ref[exp]).astype(BF16)

        over_rows(off_ref, row, step)
        o_scr[tail_of(off_ref, row, CAP), :] = jnp.zeros((CAP, D), BF16)
        unpacked(off_ref, row, o_scr, out_ref, exp)


def plain(kernel, name, ins, outs, scratch, grant, flops):
    return pl.pallas_call(
        kernel, out_shape=outs, in_specs=[SMEM] + [VMEM] * (len(ins) - 1), out_specs=jax.tree.map(lambda _: VMEM, outs),
        scratch_shapes=scratch, compiler_params=pltpu.CompilerParams(vmem_limit_bytes=grant * 1024 * 1024),
        cost_estimate=pl.CostEstimate(flops=flops, bytes_accessed=10_000_000, transcendentals=0), name=name)(*ins)


def expert_forward(layer, off, x_pad, weights):
    return plain(functools.partial(forward_kernel, layer), 'expert_forward', (off, x_pad) + weights, block(N_LOC, N_EP, CAP, D),
                 [pltpu.VMEM((SLOTS, D), BF16)] * 2, 8, 10_000_000_000)


def backward_kernel(layer, first, count, done, off_ref, x_ref, d_ref, wg_ref, wu_ref, wd_ref, out_ref, *refs):
    grad_ref = refs[0] if done else None
    left, right, gx_scr = refs[-3:]

    @pl.loop(first, first + count)
    def _(exp):
        row = layer * N_LOC + exp
        slot = jnp.maximum(exp - first - done, 0)
        x_scr, d_scr = left.at[slot, 0], left.at[slot, 1]
        packed(off_ref, row, x_ref, exp, x_scr)
        packed(off_ref, row, d_ref, exp, d_scr)

        def step(rows):
            x_blk = x_scr[rows, :]
            a_pre = mm(x_blk, wg_ref[exp], NT)
            b_pre = mm(x_blk, wu_ref[exp], NT)
            grad_h = mm(d_scr[rows, :], wd_ref[exp], NT).astype(BF16).astype(F32)
            sigma = jax.nn.sigmoid(a_pre)
            swish = a_pre * sigma
            grad_a = (grad_h * b_pre * sigma * (1.0 + a_pre * (1.0 - sigma))).astype(BF16)
            grad_b = (grad_h * swish).astype(BF16)
            right[slot, 0, rows, :] = grad_a
            right[slot, 1, rows, :] = grad_b
            right[slot, 2, rows, :] = (swish * b_pre).astype(BF16)
            gx_scr[rows, :] = (mm(grad_a, wg_ref[exp]) + mm(grad_b, wu_ref[exp])).astype(BF16)

        over_rows(off_ref, row, step)
        gx_scr[tail_of(off_ref, row, CAP), :] = jnp.zeros((CAP, D), BF16)
        unpacked(off_ref, row, gx_scr, out_ref, exp - first)
        depth, half = off_ref[row, 7], CAP // 2
        made_here = exp < first + done

        @pl.loop(off_ref[row, 4] * 2 + off_ref[row, 5], jnp.where(made_here, depth * 2, N_EP * 2))
        def _(k):
            rows = pl.ds(pl.multiple_of(k * half, half), half)
            right[slot, :, rows, :] = jnp.zeros((3, half, FF), BF16)
            left[slot, :, rows, :] = jnp.zeros((2, half, D), BF16)

        if done:
            for blocks in range(2, 5):
                pl.when(jnp.logical_and(made_here, depth == blocks))(
                    functools.partial(weight_grads, left, right, slot, grad_ref, exp - first, blocks * CAP))


def weight_grads(left, right, slot, grad_ref, exp, depth):
    @pl.loop(0, 3)
    def _(mat):
        grad = mm(left[slot, mat // 2, 0:depth, :], right[slot, mat, 0:depth, :], TN).astype(BF16)
        for owner in range(4):
            grad_ref[exp, mat, owner // 2, owner % 2] = grad[ROWS_DP * owner:ROWS_DP * owner + ROWS_DP]


def grads_shape(count):
    return (count, 3, 2, 2, ROWS_DP, FF)


def expert_backward(layer, first, count, done, off, x_pad, d_pad, weights):
    slots = max(count - done, 1)
    factors = ((slots, 2, SLOTS, D), (slots, 3, N_EP * CAP, FF))
    outs = (block(count, N_EP, CAP, D),) + ((block(*grads_shape(done)),) if done else ())
    scratch = [pltpu.VMEM((SLOTS, D), BF16)]
    if count > done:
        outs += tuple(block(*shape) for shape in factors)
    else:
        scratch = [pltpu.VMEM(shape, BF16) for shape in factors] + scratch
    return plain(functools.partial(backward_kernel, layer, first, count, done), 'expert_backward',
                 (off, x_pad, d_pad) + weights, outs, scratch, 12 if count == done else 6, 9_000_000_000 * count)


def remote(src, dst, sems, slot, target):
    send, recv = sems
    return pltpu.make_async_remote_copy(src_ref=src, dst_ref=dst, send_sem=send.at[slot], recv_sem=recv.at[slot],
                                        device_id=target, device_id_type=pl.DeviceIdType.MESH)


class Place:
    def __init__(self):
        ep, dp = lax.axis_index('ep'), lax.axis_index('dp')
        self.me = ep
        self.z, self.y = ep // 2, ep % 2
        self.x, self.c = dp // 2, dp % 2
        self.to_y, self.to_z = {'ep': self.z * 2 + 1 - self.y}, {'ep': (1 - self.z) * 2 + self.y}
        self.to_d = {'ep': (1 - self.z) * 2 + 1 - self.y}
        self.to_c, self.to_x = {'dp': self.x * 2 + 1 - self.c}, {'dp': (1 - self.x) * 2 + self.c}


def greet(targets):
    barrier = pltpu.get_barrier_semaphore()
    for target in targets:
        pl.semaphore_signal(barrier, inc=1, device_id=target, device_id_type=pl.DeviceIdType.MESH)
    return functools.partial(pl.semaphore_wait, barrier, len(targets))


class Spread:
    def __init__(self, at, own, every, sems, k):
        top, low = pl.ds(HALF * k, QUARTER), pl.ds(HALF * k + QUARTER, QUARTER)
        first = 6 * k
        self.direct = [remote(own.at[top], every.at[1, top], sems, first, at.to_y),
                       remote(own.at[low], every.at[2, low], sems, first + 1, at.to_z),
                       remote(own.at[low], every.at[1, low], sems, first + 2, at.to_y),
                       remote(own.at[top], every.at[2, top], sems, first + 3, at.to_z)]
        self.onward = [remote(every.at[1, top], every.at[3, top], sems, first + 4, at.to_z),
                       remote(every.at[2, low], every.at[3, low], sems, first + 5, at.to_y)]

    def start(self):
        for copy in self.direct:
            copy.start()

    def forward(self):
        for first, then in zip(self.direct, self.onward):
            first.wait_recv()
            then.start()

    def arrived(self, slot):
        for copy in ((), self.direct[2:3], self.direct[3:4], self.onward)[slot]:
            copy.wait_recv()

    def finish(self):
        for copy in self.direct + self.onward:
            copy.wait_send()


class Both:
    def __init__(self, first, second):
        self.sets = (first, second)

    def __getattr__(self, name):
        def each(*args):
            for one in self.sets:
                getattr(one, name)(*args)
        return each


class Collect:
    def __init__(self, at, part, got, mix_scr, sems, k):
        self.part, self.got, self.mix_scr, self.k = part, got, mix_scr, k
        self.top, self.low = pl.ds(HALF * k, QUARTER), pl.ds(HALF * k + QUARTER, QUARTER)
        self.first = first = 6 * k
        self.direct = [remote(part.at[3, self.top], got.at[first], sems, first, at.to_y),
                       remote(part.at[3, self.low], got.at[first + 1], sems, first + 1, at.to_z),
                       remote(part.at[1, self.top], got.at[first + 2], sems, first + 2, at.to_y),
                       remote(part.at[2, self.low], got.at[first + 3], sems, first + 3, at.to_z)]
        self.summed = [remote(mix_scr.at[2 * k], got.at[first + 4], sems, first + 4, at.to_z),
                       remote(mix_scr.at[2 * k + 1], got.at[first + 5], sems, first + 5, at.to_y)]

    def far(self):
        self.direct[0].start()
        self.direct[1].start()

    def near_y(self):
        self.direct[2].start()

    def near_z(self):
        self.direct[3].start()

    def forward(self):
        for step, (slot, rows) in enumerate(((2, self.top), (1, self.low))):
            self.direct[step].wait_recv()
            self.mix_scr[2 * self.k + step] = (self.part[slot, rows].astype(F32) + self.got[self.first + step].astype(F32)).astype(BF16)
            self.summed[step].start()

    def finish(self, base):
        for copy in self.direct[2:] + self.summed:
            copy.wait_recv()
        got, first = self.got, self.first
        top = self.part[0, self.top].astype(F32) + got[first + 2].astype(F32) + got[first + 4].astype(F32)
        low = self.part[0, self.low].astype(F32) + got[first + 3].astype(F32) + got[first + 5].astype(F32)
        return (base[SETS[self.k]].astype(F32) + jnp.concatenate([top, low], axis=0)).astype(BF16)

    def summed_gone(self):
        for copy in self.summed:
            copy.wait_send()

    def drain(self):
        for copy in self.direct:
            copy.wait_send()


def start_collect(at, part, got, mix_scr, sems, slot_sum, await_peers):
    both = Both(*[Collect(at, part, got, mix_scr, sems, k) for k in range(2)])
    for k, toks in enumerate(SETS):
        part[3, toks] = slot_sum(3, toks)
        if k == 0:
            await_peers()
        both.sets[k].far()
    sum_slot(part, 1, slot_sum)
    both.near_y()
    sum_slot(part, 2, slot_sum)
    both.near_z()
    return both


def sum_slot(part, slot, slot_sum):
    @pl.loop(0, 2)
    def _(k):
        toks = pl.ds(pl.multiple_of(k * HALF, HALF), HALF)
        part[slot, toks] = slot_sum(slot, toks)


def spread_of(at, own, every, sems):
    return Both(*[Spread(at, own, every, sems, k) for k in range(2)])


class Halve:
    def __init__(self, at, grads, got, sems):
        self.at, self.grads, self.got = at, grads, got
        self.pair = [remote(grads[k // 3].at[k % 3, :, 1 - at.c], got.at[k], sems, k, at.to_c) for k in range(6)]

    def start(self, exp):
        for copy in self.pair[3 * exp:3 * exp + 3]:
            copy.start()

    def wait(self, exp):
        for copy in self.pair[3 * exp:3 * exp + 3]:
            copy.wait_recv()

    def total(self, exp, side):
        return jnp.concatenate([self.grads[exp][mat, side, self.at.c].astype(F32) + self.got[3 * exp + mat, side].astype(F32)
                                for mat in range(3)], axis=1).astype(BF16)

    def drain(self):
        for copy in self.pair:
            copy.wait_send()


def store_expert(outs, exp, keep, got):
    total = (keep.astype(F32) + got.astype(F32)).astype(BF16)
    for mat, out in enumerate(outs):
        out[exp] = total[:, FF * mat:FF * mat + FF]


class Across:
    def __init__(self, at, halve, keep, send, got, sems):
        self.at, self.halve, self.keep, self.send, self.got = at, halve, keep, send, got
        self.along = [remote(send.at[exp], got.at[exp], sems, exp, at.to_x) for exp in range(2)]

    def forward(self, exp):
        self.halve.wait(exp)
        self.send[exp] = self.halve.total(exp, 1 - self.at.x)
        self.along[exp].start()
        self.keep[exp] = self.halve.total(exp, self.at.x)

    def finish(self, outs, first):
        for exp in range(2):
            self.along[exp].wait_recv()
            store_expert(outs, first + exp, self.keep[exp], self.got[exp])
        for copy in self.along:
            copy.wait_send()


def leave_totals(at, halve, keep, send):
    for exp in range(2):
        halve.wait(exp)
        send[exp] = halve.total(exp, 1 - at.x)
        keep[exp] = halve.total(exp, at.x)


def sems(count):
    return [pltpu.SemaphoreType.DMA((count,))] * 2


PACKED = (2, ROWS_DP, 3 * FF)
COLLECT_SCRATCH = [pltpu.VMEM((N_EP, TOK, D), BF16), pltpu.VMEM((12, QUARTER, D), BF16), pltpu.VMEM((4, QUARTER, D), BF16)] + sems(12)
HALVE_SCRATCH = [pltpu.VMEM((6, 2, ROWS_DP, FF), BF16)] + sems(6)
ACROSS_SCRATCH = [pltpu.VMEM(PACKED, BF16)] * 3 + sems(2)


ANY = pl.BlockSpec(memory_space=pl.ANY)


def call(kernel, name, ident, ins, outs, scratch, grant):
    return pl.pallas_call(
        kernel, out_shape=outs, scratch_shapes=scratch,
        in_specs=[SMEM if value.shape == (8, 8) else VMEM for value in ins],
        out_specs=jax.tree.map(lambda o: SMEM if o.shape == (8, 8) else VMEM, outs),
        compiler_params=pltpu.CompilerParams(collective_id=ident, has_side_effects=True, vmem_limit_bytes=grant * 1024 * 1024),
        cost_estimate=pl.CostEstimate(flops=10_000_000_000, bytes_accessed=4_000_000, transcendentals=0), name=name)(*ins)


def entry_kernel(own, pack_ref, x_pad, rank_ref, gate_ref, off_ref, packs, every, s_send, s_recv, p_send, p_recv):
    at = Place()
    greet([at.to_y, at.to_z])()
    small = [remote(pack_ref, packs.at[1], (p_send, p_recv), 0, at.to_y),
             remote(pack_ref, packs.at[2], (p_send, p_recv), 1, at.to_z),
             remote(packs.at[1], packs.at[3], (p_send, p_recv), 2, at.to_z)]
    small[0].start()
    small[1].start()
    spread = spread_of(at, own, every, (s_send, s_recv))
    spread.start()
    packs[0] = pack_ref[...]
    small[0].wait_recv()
    small[2].start()
    small[1].wait_recv()
    small[2].wait_recv()
    route_into(packs, rank_ref, gate_ref, off_ref, at.me)
    spread.forward()
    gather_rows(0, rank_ref, x_pad, 0, own)
    gather_others(spread, 0, rank_ref, x_pad, every)
    spread.finish()
    for copy in small:
        copy.wait_send()


def middle_kernel(o_ref, u_ref, dense_ref, rank_ref, gate_ref, dy_own, dy_y, dy_z, mid_ref, x_pad, d_pad,
                  part, got, mix_scr, c_send, c_recv, u_scr, every, s_send, s_recv, dy_d, d_send, d_recv):
    at = Place()
    await_peers = greet([at.to_y, at.to_z])
    onward = [remote(dy_y.at[SETS[0]], dy_d.at[SETS[0]], (d_send, d_recv), 0, at.to_z),
              remote(dy_z.at[SETS[1]], dy_d.at[SETS[1]], (d_send, d_recv), 1, at.to_y)]

    def begin():
        await_peers()
        for copy in onward:
            copy.start()

    def slot_sum(src, toks):
        return scatter_gated(0, rank_ref, gate_ref, o_ref, src, toks)

    collect = start_collect(at, part, got, mix_scr, (c_send, c_recv), slot_sum, begin)
    gather_rows(1, rank_ref, d_pad, 0, dy_own, ALL, gate_ref)
    collect.forward()
    sum_slot(part, 0, slot_sum)
    gather_rows(1, rank_ref, d_pad, 1, dy_y, ALL, gate_ref)
    spread = spread_of(at, u_scr, every, (s_send, s_recv))
    for k, rows in enumerate(SETS):
        mid = collect.sets[k].finish(u_ref)
        u_scr[rows] = (mid.astype(F32) + mm(mid, dense_ref[...])).astype(BF16)
        spread.sets[k].start()
        mid_ref[rows] = mid
    gather_rows(1, rank_ref, x_pad, 0, u_scr)
    gather_rows(1, rank_ref, d_pad, 2, dy_z, ALL, gate_ref)
    spread.forward()
    for copy in onward:
        copy.wait_recv()
    gather_rows(1, rank_ref, d_pad, 3, dy_d, ALL, gate_ref)
    collect.summed_gone()
    collect.drain()
    for copy in onward:
        copy.wait_send()
    gather_others(spread, 1, rank_ref, x_pad, every)
    spread.finish()


def dense_grad(x_ref, halves):
    return mm(x_ref[SETS[0]], halves[0], TN) + mm(x_ref[SETS[1]], halves[1], TN)


def write_slabs(slabs, value):
    for k in range(16):
        slabs[k // 8, k // 4 % 2, k // 2 % 2, k % 2] = value[24 * k:24 * k + 24].astype(BF16)


class DenseReduce:
    def __init__(self, at, slabs, got_c, sum_c, got_p, sum_p, got_x, sems):
        self.at, self.slabs, self.got_c, self.sum_c, self.got_p, self.sum_p, self.got_x = at, slabs, got_c, sum_c, got_p, sum_p, got_x
        self.pair = remote(slabs.at[:, 1 - at.c], got_c, sems, 0, at.to_c)
        self.plane = [remote(sum_c.at[:, z, y], got_p.at[k], sems, 1 + k, to) for k, (z, y, to) in enumerate((
            (at.z, 1 - at.y, at.to_y), (1 - at.z, at.y, at.to_z), (1 - at.z, 1 - at.y, at.to_d)))]
        self.along = remote(sum_p.at[1 - at.x], got_x, sems, 4, at.to_x)

    def start(self):
        self.pair.start()

    def to_plane(self):
        self.pair.wait_recv()
        for side in range(2):
            self.sum_c[side] = (self.slabs[side, self.at.c].astype(F32) + self.got_c[side].astype(F32)).astype(BF16)
        for copy in self.plane:
            copy.start()

    def to_x(self):
        for copy in self.plane:
            copy.wait_recv()
        for side in range(2):
            total = self.sum_c[side, self.at.z, self.at.y].astype(F32)
            for k in range(3):
                total = total + self.got_p[k, side].astype(F32)
            self.sum_p[side] = total.astype(BF16)
        self.along.start()

    def finish(self, out):
        self.along.wait_recv()
        out[...] = (self.sum_p[self.at.x].astype(F32) + self.got_x[...].astype(F32)).astype(BF16)
        for copy in [self.pair, self.along] + self.plane:
            copy.wait_send()


def dense_scratch():
    slab = lambda *lead: pltpu.VMEM(lead + (24, D), BF16)
    return [slab(2, 2, 2), slab(2, 2, 2), slab(3, 2), slab(2), slab()] + sems(5)


def turn_kernel(gx_ref, dy_ref, dense_ref, mid_ref, rank_ref, gate_ref, grads, left, right,
                grad_ref, d_pad, slabs, oa, ob, oc, later_keep, later_send,
                part, got, mix_scr, c_send, c_recv, s_send, s_recv, got_a, a_send, a_recv, got_b, b_send, b_recv,
                keep, send, got_x, x_send, x_recv, g_scr, every, later_grads):
    at = Place()
    await_peers = greet([at.to_y, at.to_z, at.to_c, at.to_x])
    now = Halve(at, (grads.at[0], grads.at[1]), got_a, (a_send, a_recv))
    later = Halve(at, (later_grads.at[0], later_grads.at[1]), got_b, (b_send, b_recv))

    def begin():
        await_peers()
        now.start(0)
        now.start(1)

    def slot_sum(src, toks):
        return scatter_plain(1, rank_ref, (gx_ref,), src, toks)

    collect = start_collect(at, part, got, mix_scr, (c_send, c_recv), slot_sum, begin)
    across = Across(at, now, keep, send, got_x, (x_send, x_recv))
    across.forward(0)
    collect.forward()
    across.forward(1)
    sum_slot(part, 0, slot_sum)
    for exp in range(2):
        weight_grads(left, right, exp, later_grads, exp, N_EP * CAP)
        later.start(exp)
    spread = spread_of(at, g_scr, every, (s_send, s_recv))
    halves = []
    for k, rows in enumerate(SETS):
        halves.append(collect.sets[k].finish(dy_ref))
        g_scr[rows] = (halves[k].astype(F32) + mm(halves[k], dense_ref[...], NT)).astype(BF16)
        spread.sets[k].start()
        grad_ref[rows] = g_scr[rows]
    gather_rows(0, rank_ref, d_pad, 0, g_scr, ALL, gate_ref)
    write_slabs(slabs, dense_grad(mid_ref, halves))
    spread.forward()
    leave_totals(at, later, later_keep, later_send)
    collect.summed_gone()
    collect.drain()
    now.drain()
    later.drain()
    across.finish((oa, ob, oc), 0)
    gather_others(spread, 0, rank_ref, d_pad, every, gate_ref)
    spread.finish()


def pair_kernel(grads, later_keep, later_send, got_b, b_send, b_recv):
    at = Place()
    greet([at.to_c])()
    later = Halve(at, (grads.at[0], grads.at[1]), got_b, (b_send, b_recv))
    later.start(0)
    later.start(1)
    leave_totals(at, later, later_keep, later_send)
    later.drain()


def exit_kernel(gx_a, gx_b, dy_ref, dense_ref, tok_ref, slabs_two, rank_ref, grads, left, right, two_keep, two_got, da, db, dc,
                dx_ref, dense_one, dense_two, oa, ob, oc, ta, tb, tc,
                part, got, mix_scr, c_send, c_recv, got_a, a_send, a_recv, keep, send, got_x, x_send, x_recv, slabs_one, last_grads, *dense):
    at = Place()
    await_peers = greet([at.to_y, at.to_z, at.to_d, at.to_c, at.to_x])
    now = Halve(at, (grads.at[0], last_grads.at[0]), got_a, (a_send, a_recv))
    half = len(dense) // 2
    first, second = [DenseReduce(at, slabs, *dense[k * half:k * half + 5], dense[k * half + 5:k * half + 7])
                     for k, slabs in enumerate((slabs_one, slabs_two))]

    def begin():
        await_peers()
        now.start(0)
        second.start()

    def slot_sum(src, toks):
        return scatter_plain(0, rank_ref, (gx_a, gx_b), src, toks)

    collect = start_collect(at, part, got, mix_scr, (c_send, c_recv), slot_sum, begin)
    across = Across(at, now, keep, send, got_x, (x_send, x_recv))
    across.forward(0)
    weight_grads(left, right, 0, last_grads, 0, N_EP * CAP)
    now.start(1)
    collect.forward()
    second.to_plane()
    across.forward(1)
    sum_slot(part, 0, slot_sum)
    for exp in range(2):
        store_expert((ta, tb, tc), 2 + exp, two_keep[exp], two_got[exp])
    for out, done in ((ta, da), (tb, db), (tc, dc)):
        out[0:2] = done[...]
    halves = [one.finish(dy_ref) for one in collect.sets]
    write_slabs(slabs_one, dense_grad(tok_ref, halves))
    first.start()
    second.to_x()
    for rows, half_rows in zip(SETS, halves):
        dx_ref[rows] = (half_rows.astype(F32) + mm(half_rows, dense_ref[...], NT)).astype(BF16)
    first.to_plane()
    collect.summed_gone()
    collect.drain()
    now.drain()
    first.to_x()
    across.finish((oa, ob, oc), 0)
    second.finish(dense_two)
    first.finish(dense_one)


def store_kernel(count, keep, got, *refs):
    values, outs, made, sem = refs[:count], refs[count:2 * count], refs[-2], refs[-1]
    copies = [pltpu.make_async_copy(values[k], outs[k] if k < count - 3 else outs[k].at[2:4], sem.at[k]) for k in range(count)]
    for copy in copies:
        copy.start()
    for exp in range(2):
        store_expert([made.at[mat] for mat in range(3)], exp, keep[exp], got[exp])
    for mat in range(3):
        copies.append(pltpu.make_async_copy(made.at[mat], outs[count - 3 + mat].at[0:2], sem.at[count + mat]))
        copies[-1].start()
    for copy in copies:
        copy.wait()


def store_all(keep, got, values):
    count = len(values)
    outs = [block(*value.shape) for value in values[:-3]] + [block(N_LOC, ROWS_DP, FF)] * 3
    return pl.pallas_call(
        functools.partial(store_kernel, count),
        out_shape=outs, in_specs=[VMEM] * (2 + count), out_specs=[ANY] * count,
        scratch_shapes=[pltpu.VMEM((3, 2, ROWS_DP, FF), BF16), pltpu.SemaphoreType.DMA((count + 3,))],
        compiler_params=pltpu.CompilerParams(vmem_limit_bytes=4 * 1024 * 1024),
        cost_estimate=pl.CostEstimate(flops=1_000_000_000, bytes_accessed=4_000_000, transcendentals=0), name='store')(keep, got, *values)


def stored(w_gate, w_up, w_down):
    return jnp.swapaxes(w_gate, 1, 2), jnp.swapaxes(w_up, 1, 2), w_down


def along_x(sent):
    return lax.ppermute(sent, 'dp', [(0, 2), (2, 0), (1, 3), (3, 1)])


def solution(mesh):
    tok_spec = P(('dp', 'ep'), None)
    exp_spec = P('ep', None, None)
    layer_specs = (P(None, None), tok_spec, tok_spec, exp_spec, exp_spec, exp_spec)
    grad_specs = (P(('dp', 'ep'), None), P('ep', 'dp', None), P('ep', 'dp', None), P('ep', None, 'dp'))

    def local_step(tokens, dy_out, dense_w1, route_idx1, route_gate1, w_gate1, w_up1, w_down1, dense_w2, route_idx2, route_gate2, w_gate2, w_up2, w_down2):
        weights_one, weights_two = stored(w_gate1, w_up1, w_down1), stored(w_gate2, w_up2, w_down2)
        tok_block, all_block = block(TOK, D), block(N_EP, TOK, D)
        padded = block(N_LOC, N_EP, CAP, D)
        every = pltpu.VMEM((N_EP, TOK, D), BF16)
        own = pltpu.VMEM((TOK, D), BF16)
        pack = jnp.concatenate([route_idx1.T.astype(F32), route_idx2.T.astype(F32), route_gate1.T, route_gate2.T], axis=0)
        mixed_one = (tokens.astype(F32) + jnp.dot(tokens, dense_w1, preferred_element_type=F32)).astype(BF16)
        x_one, rank, gate, off = call(
            entry_kernel, 'entry', 0, (mixed_one, pack),
            (padded, block(2, N_EP, 8, TOK, dtype=jnp.int32), block(2, N_EP, TOK, 8, dtype=F32), block(8, 8, dtype=jnp.int32)),
            [pltpu.VMEM((N_EP, 16, TOK), F32), every] + sems(12) + sems(3), 12)
        dy_later, x_one = lax.optimization_barrier((dy_out, x_one))
        dy_all = (dy_out,) + tuple(lax.ppermute(dy_later, 'ep', [(k, k ^ flip) for k in range(N_EP)]) for flip in (1, 2))
        outs = expert_forward(0, off, x_one, weights_one)
        mid_tok, x_two, d_two = call(middle_kernel, 'middle', 1, (outs, mixed_one, dense_w2, rank, gate) + dy_all,
                                     (tok_block, padded, padded), COLLECT_SCRATCH + [own, every] + sems(12) + [own] + sems(2), 9)
        gx, grads, left, right = expert_backward(1, 0, 4, 2, off, x_two, d_two, weights_two)
        grad_mid, d_one, slabs, *done_two, keep_two, send_two = call(
            turn_kernel, 'turn', 2, (gx, dy_out, dense_w2, mid_tok, rank, gate, grads, left, right),
            (tok_block, padded, block(2, 2, 2, 2, 24, D)) + (block(2, ROWS_DP, FF),) * 3 + (block(*PACKED),) * 2,
            COLLECT_SCRATCH + sems(12) + HALVE_SCRATCH * 2 + ACROSS_SCRATCH + [own, every, pltpu.VMEM(grads_shape(2), BF16)], 17)
        got_two = along_x(send_two)
        gx_a, grads = expert_backward(0, 0, 2, 2, off, x_one, d_one, weights_one)
        keep_one, send_one = call(pair_kernel, 'pair', 4, (grads,), (block(*PACKED),) * 2, HALVE_SCRATCH, 6)
        got_two, d_one = lax.optimization_barrier((got_two, d_one))
        got_one = along_x(send_one)
        gx_b, grads, left, right = expert_backward(0, 2, 2, 1, off, x_one, d_one, weights_one)
        grad_tok, dense_one, dense_two, *reduced = call(
            exit_kernel, 'exit', 3, (gx_a, gx_b, grad_mid, dense_w1, tokens, slabs, rank, grads, left, right, keep_two, got_two) + tuple(done_two),
            (tok_block, block(24, D), block(24, D)) + (block(2, ROWS_DP, FF),) * 3 + (block(N_LOC, ROWS_DP, FF),) * 3,
            COLLECT_SCRATCH + HALVE_SCRATCH + ACROSS_SCRATCH + [pltpu.VMEM((2, 2, 2, 2, 24, D), BF16), pltpu.VMEM(grads_shape(1), BF16)] + dense_scratch() * 2, 15)
        grad_tok, dense_one, dense_two, *reduced = store_all(keep_one, got_one, (grad_tok, dense_one, dense_two) + tuple(reduced[3:]) + tuple(reduced[:3]))

        def shaped(gate_up_down):
            return gate_up_down[0], gate_up_down[1], jnp.swapaxes(gate_up_down[2], 1, 2)

        return (grad_tok, dense_one) + shaped(reduced[3:]) + (dense_two,) + shaped(reduced[:3])

    return jax.shard_map(local_step, mesh=mesh, in_specs=(tok_spec, tok_spec) + layer_specs + layer_specs,
                         out_specs=(tok_spec,) + grad_specs + grad_specs, check_vma=False)
```

```python
import functools

import jax
import jax.numpy as jnp
from jax import lax
from jax.experimental import pallas as pl
from jax.experimental.pallas import tpu as pltpu
from jax.sharding import PartitionSpec as P

BF16 = jnp.bfloat16
F32 = jnp.float32
N_EP = 4
N_LOC = 4
TOK = 512
D = 384
FF = 672
CAP = 256
SLOTS = 5 * CAP
HALF = TOK // 2
QUARTER = TOK // 4
SETS = (pl.ds(0, HALF), pl.ds(HALF, HALF))
ALL = pl.ds(0, TOK)
ROWS_DP = D // 4
VMEM = pl.BlockSpec(memory_space=pltpu.VMEM)
SMEM = pl.BlockSpec(memory_space=pltpu.SMEM)


def block(*shape, dtype=BF16):
    return jax.ShapeDtypeStruct(shape, dtype)


def mm(a, b, dims=((1,), (0,))):
    return lax.dot_general(a, b, (dims, ((), ())), preferred_element_type=F32)


NT = ((1,), (1,))
TN = ((0,), (0,))


def route_into(packs, rank_ref, gate_ref, off_ref, me):
    before = (lax.broadcasted_iota(jnp.int32, (TOK, TOK), 0) < lax.broadcasted_iota(jnp.int32, (TOK, TOK), 1)).astype(BF16)
    for layer in range(2):
        running = [jnp.int32(0)] * N_LOC
        last = [jnp.int32(0)] * N_LOC
        for src in range(N_EP):
            ids = packs[src, 4 * layer:4 * layer + 4, :]
            gates = packs[src, 8 + 4 * layer:12 + 4 * layer, :]
            member, gate = [], []
            for exp in range(N_LOC):
                match = ids == (me * N_LOC + exp).astype(F32)
                member.append(jnp.sum(match.astype(F32), axis=0, keepdims=True))
                gate.append(jnp.sum(jnp.where(match, gates, 0.0), axis=0, keepdims=True))
            member = jnp.concatenate(member, axis=0)
            gate = jnp.concatenate(gate + [jnp.zeros((4, TOK), F32)], axis=0)
            rank = mm(member.astype(BF16), before)
            rank = jnp.where(member > 0.5, rank, -1.0).astype(jnp.int32)
            rank_ref[layer, src, 0:4, :] = rank
            gate_ref[layer, src] = jnp.transpose(gate)
            for exp in range(N_LOC):
                count = jnp.max(rank[exp:exp + 1, :]) + 1
                off_ref[layer * N_LOC + exp, src] = running[exp]
                last[exp] = running[exp] + count
                running[exp] = running[exp] + (count + 15) // 16 * 16
        for exp in range(N_LOC):
            halves = (last[exp] + CAP // 2 - 1) // (CAP // 2)
            off_ref[layer * N_LOC + exp, 4] = halves // 2
            off_ref[layer * N_LOC + exp, 5] = halves % 2
            off_ref[layer * N_LOC + exp, 6] = halves * (CAP // 2)
            off_ref[layer * N_LOC + exp, 7] = jnp.maximum((halves + 1) // 2, 2)


def pick(layer, rank_ref, src, exp, toks=ALL):
    row = rank_ref[layer, src, pl.ds(exp, 1), toks]
    return (lax.broadcasted_iota(jnp.int32, (CAP, toks.size), 0) == row).astype(BF16)


def gate_column(layer, gate_ref, src, exp, toks=ALL):
    slab = gate_ref[layer, src, toks]
    lane = lax.broadcasted_iota(jnp.int32, slab.shape, 1)
    return jnp.sum(jnp.where(lane == exp, slab, 0.0), axis=1, keepdims=True)


def offset(off_ref, row, src):
    return pl.multiple_of(off_ref[row, src], 16)


def scatter_gated(layer, rank_ref, gate_ref, o_ref, src, toks):
    total = None
    for exp in range(N_LOC):
        term = gate_column(layer, gate_ref, src, exp, toks) * mm(pick(layer, rank_ref, src, exp, toks), o_ref[exp, src], TN)
        total = term if total is None else total + term
    return total.astype(BF16)


def scatter_plain(layer, rank_ref, g_refs, src, toks):
    sel = jnp.concatenate([pick(layer, rank_ref, src, exp, toks) for exp in range(N_LOC)], axis=0)
    per = N_LOC // len(g_refs)
    rows = [g_refs[exp // per][exp % per, src] for exp in range(N_LOC)]
    return mm(sel, jnp.concatenate(rows, axis=0), TN).astype(BF16)


def gather_rows(layer, rank_ref, pad_ref, src, block_ref, toks=ALL, gate_ref=None, more=False):
    @pl.loop(0, N_LOC)
    def _(exp):
        rows = block_ref[toks]
        if gate_ref is not None:
            rows = (gate_column(layer, gate_ref, src, exp, toks) * rows.astype(F32)).astype(BF16)
        picked = mm(pick(layer, rank_ref, src, exp, toks), rows)
        if more:
            picked = pad_ref[exp, src].astype(F32) + picked
        pad_ref[exp, src] = picked.astype(BF16)


def gather_others(spread, layer, rank_ref, pad_ref, every, gate_ref=None):
    for src in (1, 2):
        spread.arrived(src)
        gather_rows(layer, rank_ref, pad_ref, src, every.at[src], ALL, gate_ref)
    for k, toks in enumerate(SETS):
        spread.sets[k].arrived(3)
        gather_rows(layer, rank_ref, pad_ref, 3, every.at[3], toks, gate_ref, k == 1)


def packed(off_ref, row, pad_ref, exp, scr):
    for src in range(N_EP):
        scr[pl.ds(offset(off_ref, row, src), CAP), :] = pad_ref[exp, src]
    scr[pl.ds(offset(off_ref, row, 3) + CAP, CAP), :] = jnp.zeros((CAP, D), BF16)


def over_rows(off_ref, row, step):
    @pl.loop(0, off_ref[row, 4])
    def _(blk):
        step(pl.ds(pl.multiple_of(blk * CAP, CAP), CAP))

    @pl.when(off_ref[row, 5] == 1)
    def _():
        step(pl.ds(pl.multiple_of(off_ref[row, 4] * CAP, CAP), CAP // 2))


def tail_of(off_ref, row, size):
    return pl.ds(pl.multiple_of(off_ref[row, 6], CAP // 2), size)


def unpacked(off_ref, row, scr, out_ref, exp):
    for src in range(N_EP):
        out_ref[exp, src] = scr[pl.ds(offset(off_ref, row, src), CAP), :]


def forward_kernel(layer, off_ref, x_ref, wg_ref, wu_ref, wd_ref, out_ref, x_scr, o_scr):
    @pl.loop(0, N_LOC)
    def _(exp):
        row = layer * N_LOC + exp
        packed(off_ref, row, x_ref, exp, x_scr)

        def step(rows):
            x_blk = x_scr[rows, :]
            a_pre = mm(x_blk, wg_ref[exp], NT)
            b_pre = mm(x_blk, wu_ref[exp], NT)
            hidden = (jax.nn.silu(a_pre) * b_pre).astype(BF16)
            o_scr[rows, :] = mm(hidden, wd_ref[exp]).astype(BF16)

        over_rows(off_ref, row, step)
        o_scr[tail_of(off_ref, row, CAP), :] = jnp.zeros((CAP, D), BF16)
        unpacked(off_ref, row, o_scr, out_ref, exp)


def plain(kernel, name, ins, outs, scratch, grant, flops):
    return pl.pallas_call(
        kernel, out_shape=outs, in_specs=[SMEM] + [VMEM] * (len(ins) - 1), out_specs=jax.tree.map(lambda _: VMEM, outs),
        scratch_shapes=scratch, compiler_params=pltpu.CompilerParams(vmem_limit_bytes=grant * 1024 * 1024),
        cost_estimate=pl.CostEstimate(flops=flops, bytes_accessed=10_000_000, transcendentals=0), name=name)(*ins)


def expert_forward(layer, off, x_pad, weights):
    return plain(functools.partial(forward_kernel, layer), 'expert_forward', (off, x_pad) + weights, block(N_LOC, N_EP, CAP, D),
                 [pltpu.VMEM((SLOTS, D), BF16)] * 2, 8, 10_000_000_000)


def backward_kernel(layer, first, count, done, off_ref, x_ref, d_ref, wg_ref, wu_ref, wd_ref, out_ref, *refs):
    grad_ref = refs[0] if done else None
    left, right, gx_scr = refs[-3:]

    @pl.loop(first, first + count)
    def _(exp):
        row = layer * N_LOC + exp
        slot = jnp.maximum(exp - first - done, 0)
        x_scr, d_scr = left.at[slot, 0], left.at[slot, 1]
        packed(off_ref, row, x_ref, exp, x_scr)
        packed(off_ref, row, d_ref, exp, d_scr)

        def step(rows):
            x_blk = x_scr[rows, :]
            a_pre = mm(x_blk, wg_ref[exp], NT)
            grad_h = mm(d_scr[rows, :], wd_ref[exp], NT).astype(BF16).astype(F32)
            sigma = jax.nn.sigmoid(a_pre)
            swish = a_pre * sigma
            grad_b = (grad_h * swish).astype(BF16)
            right[slot, 1, rows, :] = grad_b
            slope = grad_h * (sigma + swish * (1.0 - sigma))
            b_pre = mm(x_blk, wu_ref[exp], NT)
            right[slot, 2, rows, :] = (swish * b_pre).astype(BF16)
            grad_a = (slope * b_pre).astype(BF16)
            right[slot, 0, rows, :] = grad_a
            gx_scr[rows, :] = (mm(grad_a, wg_ref[exp]) + mm(grad_b, wu_ref[exp])).astype(BF16)

        over_rows(off_ref, row, step)
        gx_scr[tail_of(off_ref, row, CAP), :] = jnp.zeros((CAP, D), BF16)
        unpacked(off_ref, row, gx_scr, out_ref, exp - first)
        depth, half = off_ref[row, 7], CAP // 2
        made_here = exp < first + done

        @pl.loop(off_ref[row, 4] * 2 + off_ref[row, 5], jnp.where(made_here, depth * 2, N_EP * 2))
        def _(k):
            rows = pl.ds(pl.multiple_of(k * half, half), half)
            right[slot, :, rows, :] = jnp.zeros((3, half, FF), BF16)
            left[slot, :, rows, :] = jnp.zeros((2, half, D), BF16)

        if done:
            for blocks in range(2, 5):
                pl.when(jnp.logical_and(made_here, depth == blocks))(
                    functools.partial(weight_grads, left, right, slot, grad_ref, exp - first, blocks * CAP))


def weight_grads(left, right, slot, grad_ref, exp, depth):
    @pl.loop(0, 3)
    def _(mat):
        grad = mm(left[slot, mat // 2, 0:depth, :], right[slot, mat, 0:depth, :], TN).astype(BF16)
        for owner in range(4):
            grad_ref[exp, mat, owner // 2, owner % 2] = grad[ROWS_DP * owner:ROWS_DP * owner + ROWS_DP]


def grads_shape(count):
    return (count, 3, 2, 2, ROWS_DP, FF)


def expert_backward(layer, first, count, done, off, x_pad, d_pad, weights):
    slots = max(count - done, 1)
    factors = ((slots, 2, SLOTS, D), (slots, 3, N_EP * CAP, FF))
    outs = (block(count, N_EP, CAP, D),) + ((block(*grads_shape(done)),) if done else ())
    scratch = [pltpu.VMEM((SLOTS, D), BF16)]
    if count > done:
        outs += tuple(block(*shape) for shape in factors)
    else:
        scratch = [pltpu.VMEM(shape, BF16) for shape in factors] + scratch
    return plain(functools.partial(backward_kernel, layer, first, count, done), 'expert_backward',
                 (off, x_pad, d_pad) + weights, outs, scratch, 12 if count == done else 6, 9_000_000_000 * count)


def remote(src, dst, sems, slot, target):
    send, recv = sems
    return pltpu.make_async_remote_copy(src_ref=src, dst_ref=dst, send_sem=send.at[slot], recv_sem=recv.at[slot],
                                        device_id=target, device_id_type=pl.DeviceIdType.MESH)


class Place:
    def __init__(self):
        ep, dp = lax.axis_index('ep'), lax.axis_index('dp')
        self.me = ep
        self.z, self.y = ep // 2, ep % 2
        self.x, self.c = dp // 2, dp % 2
        self.to_y, self.to_z = {'ep': self.z * 2 + 1 - self.y}, {'ep': (1 - self.z) * 2 + self.y}
        self.to_d = {'ep': (1 - self.z) * 2 + 1 - self.y}
        self.to_c, self.to_x = {'dp': self.x * 2 + 1 - self.c}, {'dp': (1 - self.x) * 2 + self.c}


def greet(targets):
    barrier = pltpu.get_barrier_semaphore()
    for target in targets:
        pl.semaphore_signal(barrier, inc=1, device_id=target, device_id_type=pl.DeviceIdType.MESH)
    return functools.partial(pl.semaphore_wait, barrier, len(targets))


class Spread:
    def __init__(self, at, own, every, sems, k):
        top, low = pl.ds(HALF * k, QUARTER), pl.ds(HALF * k + QUARTER, QUARTER)
        first = 6 * k
        self.direct = [remote(own.at[top], every.at[1, top], sems, first, at.to_y),
                       remote(own.at[low], every.at[2, low], sems, first + 1, at.to_z),
                       remote(own.at[low], every.at[1, low], sems, first + 2, at.to_y),
                       remote(own.at[top], every.at[2, top], sems, first + 3, at.to_z)]
        self.onward = [remote(every.at[1, top], every.at[3, top], sems, first + 4, at.to_z),
                       remote(every.at[2, low], every.at[3, low], sems, first + 5, at.to_y)]

    def start(self):
        for copy in self.direct:
            copy.start()

    def forward(self):
        for first, then in zip(self.direct, self.onward):
            first.wait_recv()
            then.start()

    def arrived(self, slot):
        for copy in ((), self.direct[2:3], self.direct[3:4], self.onward)[slot]:
            copy.wait_recv()

    def finish(self):
        for copy in self.direct + self.onward:
            copy.wait_send()


class Both:
    def __init__(self, first, second):
        self.sets = (first, second)

    def __getattr__(self, name):
        def each(*args):
            for one in self.sets:
                getattr(one, name)(*args)
        return each


class Collect:
    def __init__(self, at, part, got, mix_scr, sems, k):
        self.part, self.got, self.mix_scr, self.k = part, got, mix_scr, k
        self.top, self.low = pl.ds(HALF * k, QUARTER), pl.ds(HALF * k + QUARTER, QUARTER)
        self.first = first = 6 * k
        self.direct = [remote(part.at[3, self.top], got.at[first], sems, first, at.to_y),
                       remote(part.at[3, self.low], got.at[first + 1], sems, first + 1, at.to_z),
                       remote(part.at[1, self.top], got.at[first + 2], sems, first + 2, at.to_y),
                       remote(part.at[2, self.low], got.at[first + 3], sems, first + 3, at.to_z)]
        self.summed = [remote(mix_scr.at[2 * k], got.at[first + 4], sems, first + 4, at.to_z),
                       remote(mix_scr.at[2 * k + 1], got.at[first + 5], sems, first + 5, at.to_y)]

    def far(self):
        self.direct[0].start()
        self.direct[1].start()

    def near_y(self):
        self.direct[2].start()

    def near_z(self):
        self.direct[3].start()

    def forward(self):
        for step, (slot, rows) in enumerate(((2, self.top), (1, self.low))):
            self.direct[step].wait_recv()
            self.mix_scr[2 * self.k + step] = (self.part[slot, rows].astype(F32) + self.got[self.first + step].astype(F32)).astype(BF16)
            self.summed[step].start()

    def finish(self, base):
        for copy in self.direct[2:] + self.summed:
            copy.wait_recv()
        got, first = self.got, self.first
        top = self.part[0, self.top].astype(F32) + got[first + 2].astype(F32) + got[first + 4].astype(F32)
        low = self.part[0, self.low].astype(F32) + got[first + 3].astype(F32) + got[first + 5].astype(F32)
        return (base[SETS[self.k]].astype(F32) + jnp.concatenate([top, low], axis=0)).astype(BF16)

    def summed_gone(self):
        for copy in self.summed:
            copy.wait_send()

    def drain(self):
        for copy in self.direct:
            copy.wait_send()


def start_collect(at, part, got, mix_scr, sems, slot_sum, await_peers):
    both = Both(*[Collect(at, part, got, mix_scr, sems, k) for k in range(2)])
    for k, toks in enumerate(SETS):
        part[3, toks] = slot_sum(3, toks)
        if k == 0:
            await_peers()
        both.sets[k].far()
    sum_slot(part, 1, slot_sum)
    both.near_y()
    sum_slot(part, 2, slot_sum)
    both.near_z()
    return both


def sum_slot(part, slot, slot_sum):
    @pl.loop(0, 2)
    def _(k):
        toks = pl.ds(pl.multiple_of(k * HALF, HALF), HALF)
        part[slot, toks] = slot_sum(slot, toks)


def spread_of(at, own, every, sems):
    return Both(*[Spread(at, own, every, sems, k) for k in range(2)])


class Halve:
    def __init__(self, at, grads, got, sems):
        self.at, self.grads, self.got = at, grads, got
        self.pair = [remote(grads[k // 3].at[k % 3, :, 1 - at.c], got.at[k], sems, k, at.to_c) for k in range(6)]

    def start(self, exp):
        for copy in self.pair[3 * exp:3 * exp + 3]:
            copy.start()

    def wait(self, exp):
        for copy in self.pair[3 * exp:3 * exp + 3]:
            copy.wait_recv()

    def total(self, exp, side):
        return jnp.concatenate([self.grads[exp][mat, side, self.at.c].astype(F32) + self.got[3 * exp + mat, side].astype(F32)
                                for mat in range(3)], axis=1).astype(BF16)

    def drain(self):
        for copy in self.pair:
            copy.wait_send()


def store_expert(outs, exp, keep, got):
    total = (keep.astype(F32) + got.astype(F32)).astype(BF16)
    for mat, out in enumerate(outs):
        out[exp] = total[:, FF * mat:FF * mat + FF]


class Across:
    def __init__(self, at, halve, keep, send, got, sems):
        self.at, self.halve, self.keep, self.send, self.got = at, halve, keep, send, got
        self.along = [remote(send.at[exp], got.at[exp], sems, exp, at.to_x) for exp in range(2)]

    def forward(self, exp):
        self.halve.wait(exp)
        self.send[exp] = self.halve.total(exp, 1 - self.at.x)
        self.along[exp].start()
        self.keep[exp] = self.halve.total(exp, self.at.x)

    def finish(self, outs, first):
        for exp in range(2):
            self.along[exp].wait_recv()
            store_expert(outs, first + exp, self.keep[exp], self.got[exp])
        for copy in self.along:
            copy.wait_send()


def leave_totals(at, halve, keep, send):
    for exp in range(2):
        halve.wait(exp)
        send[exp] = halve.total(exp, 1 - at.x)
        keep[exp] = halve.total(exp, at.x)


def sems(count):
    return [pltpu.SemaphoreType.DMA((count,))] * 2


PACKED = (2, ROWS_DP, 3 * FF)
COLLECT_SCRATCH = [pltpu.VMEM((N_EP, TOK, D), BF16), pltpu.VMEM((12, QUARTER, D), BF16), pltpu.VMEM((4, QUARTER, D), BF16)] + sems(12)
HALVE_SCRATCH = [pltpu.VMEM((6, 2, ROWS_DP, FF), BF16)] + sems(6)
ACROSS_SCRATCH = [pltpu.VMEM(PACKED, BF16)] * 3 + sems(2)


ANY = pl.BlockSpec(memory_space=pl.ANY)


def call(kernel, name, ident, ins, outs, scratch, grant):
    return pl.pallas_call(
        kernel, out_shape=outs, scratch_shapes=scratch,
        in_specs=[SMEM if value.shape == (8, 8) else VMEM for value in ins],
        out_specs=jax.tree.map(lambda o: SMEM if o.shape == (8, 8) else VMEM, outs),
        compiler_params=pltpu.CompilerParams(collective_id=ident, has_side_effects=True, vmem_limit_bytes=grant * 1024 * 1024),
        cost_estimate=pl.CostEstimate(flops=10_000_000_000, bytes_accessed=4_000_000, transcendentals=0), name=name)(*ins)


def entry_kernel(own, pack_ref, x_pad, rank_ref, gate_ref, off_ref, packs, every, s_send, s_recv, p_send, p_recv):
    at = Place()
    greet([at.to_y, at.to_z])()
    small = [remote(pack_ref, packs.at[1], (p_send, p_recv), 0, at.to_y),
             remote(pack_ref, packs.at[2], (p_send, p_recv), 1, at.to_z),
             remote(packs.at[1], packs.at[3], (p_send, p_recv), 2, at.to_z)]
    small[0].start()
    small[1].start()
    spread = spread_of(at, own, every, (s_send, s_recv))
    spread.start()
    packs[0] = pack_ref[...]
    small[0].wait_recv()
    small[2].start()
    small[1].wait_recv()
    small[2].wait_recv()
    route_into(packs, rank_ref, gate_ref, off_ref, at.me)
    spread.forward()
    gather_rows(0, rank_ref, x_pad, 0, own)
    gather_others(spread, 0, rank_ref, x_pad, every)
    spread.finish()
    for copy in small:
        copy.wait_send()


def middle_kernel(o_ref, u_ref, dense_ref, rank_ref, gate_ref, dy_own, dy_y, dy_z, mid_ref, x_pad, d_pad,
                  part, got, mix_scr, c_send, c_recv, u_scr, every, s_send, s_recv, dy_d, d_send, d_recv):
    at = Place()
    await_peers = greet([at.to_y, at.to_z])
    onward = [remote(dy_y.at[SETS[0]], dy_d.at[SETS[0]], (d_send, d_recv), 0, at.to_z),
              remote(dy_z.at[SETS[1]], dy_d.at[SETS[1]], (d_send, d_recv), 1, at.to_y)]

    def begin():
        await_peers()
        for copy in onward:
            copy.start()

    def slot_sum(src, toks):
        return scatter_gated(0, rank_ref, gate_ref, o_ref, src, toks)

    collect = start_collect(at, part, got, mix_scr, (c_send, c_recv), slot_sum, begin)
    gather_rows(1, rank_ref, d_pad, 0, dy_own, ALL, gate_ref)
    collect.forward()
    sum_slot(part, 0, slot_sum)
    gather_rows(1, rank_ref, d_pad, 1, dy_y, ALL, gate_ref)
    spread = spread_of(at, u_scr, every, (s_send, s_recv))
    for k, rows in enumerate(SETS):
        mid = collect.sets[k].finish(u_ref)
        u_scr[rows] = (mid.astype(F32) + mm(mid, dense_ref[...])).astype(BF16)
        spread.sets[k].start()
        mid_ref[rows] = mid
    gather_rows(1, rank_ref, x_pad, 0, u_scr)
    gather_rows(1, rank_ref, d_pad, 2, dy_z, ALL, gate_ref)
    spread.forward()
    for copy in onward:
        copy.wait_recv()
    gather_rows(1, rank_ref, d_pad, 3, dy_d, ALL, gate_ref)
    collect.summed_gone()
    collect.drain()
    for copy in onward:
        copy.wait_send()
    gather_others(spread, 1, rank_ref, x_pad, every)
    spread.finish()


def dense_grad(x_ref, halves):
    return mm(x_ref[SETS[0]], halves[0], TN) + mm(x_ref[SETS[1]], halves[1], TN)


def write_slabs(slabs, value):
    for k in range(16):
        slabs[k // 8, k // 4 % 2, k // 2 % 2, k % 2] = value[24 * k:24 * k + 24].astype(BF16)


class DenseReduce:
    def __init__(self, at, slabs, got_c, sum_c, got_p, sum_p, got_x, sems):
        self.at, self.slabs, self.got_c, self.sum_c, self.got_p, self.sum_p, self.got_x = at, slabs, got_c, sum_c, got_p, sum_p, got_x
        self.pair = remote(slabs.at[:, 1 - at.c], got_c, sems, 0, at.to_c)
        self.plane = [remote(sum_c.at[:, z, y], got_p.at[k], sems, 1 + k, to) for k, (z, y, to) in enumerate((
            (at.z, 1 - at.y, at.to_y), (1 - at.z, at.y, at.to_z), (1 - at.z, 1 - at.y, at.to_d)))]
        self.along = remote(sum_p.at[1 - at.x], got_x, sems, 4, at.to_x)

    def start(self):
        self.pair.start()

    def to_plane(self):
        self.pair.wait_recv()
        for side in range(2):
            self.sum_c[side] = (self.slabs[side, self.at.c].astype(F32) + self.got_c[side].astype(F32)).astype(BF16)
        for copy in self.plane:
            copy.start()

    def to_x(self):
        for copy in self.plane:
            copy.wait_recv()
        for side in range(2):
            total = self.sum_c[side, self.at.z, self.at.y].astype(F32)
            for k in range(3):
                total = total + self.got_p[k, side].astype(F32)
            self.sum_p[side] = total.astype(BF16)
        self.along.start()

    def finish(self, out):
        self.along.wait_recv()
        out[...] = (self.sum_p[self.at.x].astype(F32) + self.got_x[...].astype(F32)).astype(BF16)
        for copy in [self.pair, self.along] + self.plane:
            copy.wait_send()


def dense_scratch():
    slab = lambda *lead: pltpu.VMEM(lead + (24, D), BF16)
    return [slab(2, 2, 2), slab(2, 2, 2), slab(3, 2), slab(2), slab()] + sems(5)


def turn_kernel(gx_ref, dy_ref, dense_ref, mid_ref, rank_ref, gate_ref, grads, left, right,
                grad_ref, d_pad, slabs, oa, ob, oc, later_keep, later_send,
                part, got, mix_scr, c_send, c_recv, s_send, s_recv, got_a, a_send, a_recv, got_b, b_send, b_recv,
                keep, send, got_x, x_send, x_recv, g_scr, every, later_grads):
    at = Place()
    await_peers = greet([at.to_y, at.to_z, at.to_c, at.to_x])
    now = Halve(at, (grads.at[0], grads.at[1]), got_a, (a_send, a_recv))
    later = Halve(at, (later_grads.at[0], later_grads.at[1]), got_b, (b_send, b_recv))

    def begin():
        await_peers()
        now.start(0)
        now.start(1)

    def slot_sum(src, toks):
        return scatter_plain(1, rank_ref, (gx_ref,), src, toks)

    collect = start_collect(at, part, got, mix_scr, (c_send, c_recv), slot_sum, begin)
    across = Across(at, now, keep, send, got_x, (x_send, x_recv))
    across.forward(0)
    collect.forward()
    across.forward(1)
    sum_slot(part, 0, slot_sum)
    for exp in range(2):
        weight_grads(left, right, exp, later_grads, exp, N_EP * CAP)
        later.start(exp)
    spread = spread_of(at, g_scr, every, (s_send, s_recv))
    halves = []
    for k, rows in enumerate(SETS):
        halves.append(collect.sets[k].finish(dy_ref))
        g_scr[rows] = (halves[k].astype(F32) + mm(halves[k], dense_ref[...], NT)).astype(BF16)
        spread.sets[k].start()
        grad_ref[rows] = g_scr[rows]
    gather_rows(0, rank_ref, d_pad, 0, g_scr, ALL, gate_ref)
    write_slabs(slabs, dense_grad(mid_ref, halves))
    spread.forward()
    leave_totals(at, later, later_keep, later_send)
    collect.summed_gone()
    collect.drain()
    now.drain()
    later.drain()
    across.finish((oa, ob, oc), 0)
    gather_others(spread, 0, rank_ref, d_pad, every, gate_ref)
    spread.finish()


def pair_kernel(grads, later_keep, later_send, got_b, b_send, b_recv):
    at = Place()
    greet([at.to_c])()
    later = Halve(at, (grads.at[0], grads.at[1]), got_b, (b_send, b_recv))
    later.start(0)
    later.start(1)
    leave_totals(at, later, later_keep, later_send)
    later.drain()


def exit_kernel(gx_a, gx_b, dy_ref, dense_ref, tok_ref, slabs_two, rank_ref, grads, left, right, two_keep, two_got, da, db, dc,
                dx_ref, dense_one, dense_two, oa, ob, oc, ta, tb, tc,
                part, got, mix_scr, c_send, c_recv, got_a, a_send, a_recv, keep, send, got_x, x_send, x_recv, slabs_one, last_grads, *dense):
    at = Place()
    await_peers = greet([at.to_y, at.to_z, at.to_d, at.to_c, at.to_x])
    now = Halve(at, (grads.at[0], last_grads.at[0]), got_a, (a_send, a_recv))
    half = len(dense) // 2
    first, second = [DenseReduce(at, slabs, *dense[k * half:k * half + 5], dense[k * half + 5:k * half + 7])
                     for k, slabs in enumerate((slabs_one, slabs_two))]

    def begin():
        await_peers()
        now.start(0)
        second.start()

    def slot_sum(src, toks):
        return scatter_plain(0, rank_ref, (gx_a, gx_b), src, toks)

    collect = start_collect(at, part, got, mix_scr, (c_send, c_recv), slot_sum, begin)
    across = Across(at, now, keep, send, got_x, (x_send, x_recv))
    across.forward(0)
    weight_grads(left, right, 0, last_grads, 0, N_EP * CAP)
    now.start(1)
    collect.forward()
    second.to_plane()
    across.forward(1)
    sum_slot(part, 0, slot_sum)
    for exp in range(2):
        store_expert((ta, tb, tc), 2 + exp, two_keep[exp], two_got[exp])
    for out, done in ((ta, da), (tb, db), (tc, dc)):
        out[0:2] = done[...]
    halves = [one.finish(dy_ref) for one in collect.sets]
    write_slabs(slabs_one, dense_grad(tok_ref, halves))
    first.start()
    second.to_x()
    for rows, half_rows in zip(SETS, halves):
        dx_ref[rows] = (half_rows.astype(F32) + mm(half_rows, dense_ref[...], NT)).astype(BF16)
    first.to_plane()
    collect.summed_gone()
    collect.drain()
    now.drain()
    first.to_x()
    across.finish((oa, ob, oc), 0)
    second.finish(dense_two)
    first.finish(dense_one)


def store_kernel(count, keep, got, *refs):
    values, outs, made, sem = refs[:count], refs[count:2 * count], refs[-2], refs[-1]
    copies = [pltpu.make_async_copy(values[k], outs[k] if k < count - 3 else outs[k].at[2:4], sem.at[k]) for k in range(count)]
    for copy in copies:
        copy.start()
    for exp in range(2):
        store_expert([made.at[mat] for mat in range(3)], exp, keep[exp], got[exp])
    for mat in range(3):
        copies.append(pltpu.make_async_copy(made.at[mat], outs[count - 3 + mat].at[0:2], sem.at[count + mat]))
        copies[-1].start()
    for copy in copies:
        copy.wait()


def store_all(keep, got, values):
    count = len(values)
    outs = [block(*value.shape) for value in values[:-3]] + [block(N_LOC, ROWS_DP, FF)] * 3
    return pl.pallas_call(
        functools.partial(store_kernel, count),
        out_shape=outs, in_specs=[VMEM] * (2 + count), out_specs=[ANY] * count,
        scratch_shapes=[pltpu.VMEM((3, 2, ROWS_DP, FF), BF16), pltpu.SemaphoreType.DMA((count + 3,))],
        compiler_params=pltpu.CompilerParams(vmem_limit_bytes=4 * 1024 * 1024),
        cost_estimate=pl.CostEstimate(flops=1_000_000_000, bytes_accessed=4_000_000, transcendentals=0), name='store')(keep, got, *values)


def stored(w_gate, w_up, w_down):
    return jnp.swapaxes(w_gate, 1, 2), jnp.swapaxes(w_up, 1, 2), w_down


def along_x(sent):
    return lax.ppermute(sent, 'dp', [(0, 2), (2, 0), (1, 3), (3, 1)])


def solution(mesh):
    tok_spec = P(('dp', 'ep'), None)
    exp_spec = P('ep', None, None)
    layer_specs = (P(None, None), tok_spec, tok_spec, exp_spec, exp_spec, exp_spec)
    grad_specs = (P(('dp', 'ep'), None), P('ep', 'dp', None), P('ep', 'dp', None), P('ep', None, 'dp'))

    def local_step(tokens, dy_out, dense_w1, route_idx1, route_gate1, w_gate1, w_up1, w_down1, dense_w2, route_idx2, route_gate2, w_gate2, w_up2, w_down2):
        weights_one, weights_two = stored(w_gate1, w_up1, w_down1), stored(w_gate2, w_up2, w_down2)
        tok_block, all_block = block(TOK, D), block(N_EP, TOK, D)
        padded = block(N_LOC, N_EP, CAP, D)
        every = pltpu.VMEM((N_EP, TOK, D), BF16)
        own = pltpu.VMEM((TOK, D), BF16)
        pack = jnp.concatenate([route_idx1.T.astype(F32), route_idx2.T.astype(F32), route_gate1.T, route_gate2.T], axis=0)
        mixed_one = (tokens.astype(F32) + jnp.dot(tokens, dense_w1, preferred_element_type=F32)).astype(BF16)
        x_one, rank, gate, off = call(
            entry_kernel, 'entry', 0, (mixed_one, pack),
            (padded, block(2, N_EP, 8, TOK, dtype=jnp.int32), block(2, N_EP, TOK, 8, dtype=F32), block(8, 8, dtype=jnp.int32)),
            [pltpu.VMEM((N_EP, 16, TOK), F32), every] + sems(12) + sems(3), 12)
        dy_later, x_one = lax.optimization_barrier((dy_out, x_one))
        dy_all = (dy_out,) + tuple(lax.ppermute(dy_later, 'ep', [(k, k ^ flip) for k in range(N_EP)]) for flip in (1, 2))
        outs = expert_forward(0, off, x_one, weights_one)
        mid_tok, x_two, d_two = call(middle_kernel, 'middle', 1, (outs, mixed_one, dense_w2, rank, gate) + dy_all,
                                     (tok_block, padded, padded), COLLECT_SCRATCH + [own, every] + sems(12) + [own] + sems(2), 9)
        gx, grads, left, right = expert_backward(1, 0, 4, 2, off, x_two, d_two, weights_two)
        grad_mid, d_one, slabs, *done_two, keep_two, send_two = call(
            turn_kernel, 'turn', 2, (gx, dy_out, dense_w2, mid_tok, rank, gate, grads, left, right),
            (tok_block, padded, block(2, 2, 2, 2, 24, D)) + (block(2, ROWS_DP, FF),) * 3 + (block(*PACKED),) * 2,
            COLLECT_SCRATCH + sems(12) + HALVE_SCRATCH * 2 + ACROSS_SCRATCH + [own, every, pltpu.VMEM(grads_shape(2), BF16)], 17)
        got_two = along_x(send_two)
        gx_a, grads = expert_backward(0, 0, 2, 2, off, x_one, d_one, weights_one)
        keep_one, send_one = call(pair_kernel, 'pair', 4, (grads,), (block(*PACKED),) * 2, HALVE_SCRATCH, 6)
        got_two, d_one = lax.optimization_barrier((got_two, d_one))
        got_one = along_x(send_one)
        gx_b, grads, left, right = expert_backward(0, 2, 2, 1, off, x_one, d_one, weights_one)
        grad_tok, dense_one, dense_two, *reduced = call(
            exit_kernel, 'exit', 3, (gx_a, gx_b, grad_mid, dense_w1, tokens, slabs, rank, grads, left, right, keep_two, got_two) + tuple(done_two),
            (tok_block, block(24, D), block(24, D)) + (block(2, ROWS_DP, FF),) * 3 + (block(N_LOC, ROWS_DP, FF),) * 3,
            COLLECT_SCRATCH + HALVE_SCRATCH + ACROSS_SCRATCH + [pltpu.VMEM((2, 2, 2, 2, 24, D), BF16), pltpu.VMEM(grads_shape(1), BF16)] + dense_scratch() * 2, 15)
        grad_tok, dense_one, dense_two, *reduced = store_all(keep_one, got_one, (grad_tok, dense_one, dense_two) + tuple(reduced[3:]) + tuple(reduced[:3]))

        def shaped(gate_up_down):
            return gate_up_down[0], gate_up_down[1], jnp.swapaxes(gate_up_down[2], 1, 2)

        return (grad_tok, dense_one) + shaped(reduced[3:]) + (dense_two,) + shaped(reduced[:3])

    return jax.shard_map(local_step, mesh=mesh, in_specs=(tok_spec, tok_spec) + layer_specs + layer_specs,
                         out_specs=(tok_spec,) + grad_specs + grad_specs, check_vma=False)
```

```python
import functools

import jax
import jax.numpy as jnp
from jax import lax
from jax.experimental import pallas as pl
from jax.experimental.pallas import tpu as pltpu
from jax.sharding import PartitionSpec as P

BF16 = jnp.bfloat16
F32 = jnp.float32
N_EP = 4
N_LOC = 4
TOK = 512
D = 384
FF = 672
CAP = 256
SLOTS = 5 * CAP
HALF = TOK // 2
QUARTER = TOK // 4
SETS = (pl.ds(0, HALF), pl.ds(HALF, HALF))
ALL = pl.ds(0, TOK)
ROWS_DP = D // 4
VMEM = pl.BlockSpec(memory_space=pltpu.VMEM)
SMEM = pl.BlockSpec(memory_space=pltpu.SMEM)


def block(*shape, dtype=BF16):
    return jax.ShapeDtypeStruct(shape, dtype)


def mm(a, b, dims=((1,), (0,))):
    return lax.dot_general(a, b, (dims, ((), ())), preferred_element_type=F32)


NT = ((1,), (1,))
TN = ((0,), (0,))


def route_into(packs, rank_ref, gate_ref, off_ref, me):
    before = (lax.broadcasted_iota(jnp.int32, (TOK, TOK), 0) < lax.broadcasted_iota(jnp.int32, (TOK, TOK), 1)).astype(BF16)
    for layer in range(2):
        running = [jnp.int32(0)] * N_LOC
        last = [jnp.int32(0)] * N_LOC
        for src in range(N_EP):
            ids = packs[src, 4 * layer:4 * layer + 4, :]
            gates = packs[src, 8 + 4 * layer:12 + 4 * layer, :]
            member, gate = [], []
            for exp in range(N_LOC):
                match = ids == (me * N_LOC + exp).astype(F32)
                member.append(jnp.sum(match.astype(F32), axis=0, keepdims=True))
                gate.append(jnp.sum(jnp.where(match, gates, 0.0), axis=0, keepdims=True))
            member = jnp.concatenate(member, axis=0)
            gate = jnp.concatenate(gate + [jnp.zeros((4, TOK), F32)], axis=0)
            rank = mm(member.astype(BF16), before)
            rank = jnp.where(member > 0.5, rank, -1.0).astype(jnp.int32)
            rank_ref[layer, src, 0:4, :] = rank
            gate_ref[layer, src] = jnp.transpose(gate)
            for exp in range(N_LOC):
                count = jnp.max(rank[exp:exp + 1, :]) + 1
                off_ref[layer * N_LOC + exp, src] = running[exp]
                last[exp] = running[exp] + count
                running[exp] = running[exp] + (count + 15) // 16 * 16
        for exp in range(N_LOC):
            halves = (last[exp] + CAP // 2 - 1) // (CAP // 2)
            off_ref[layer * N_LOC + exp, 4] = halves // 2
            off_ref[layer * N_LOC + exp, 5] = halves % 2
            off_ref[layer * N_LOC + exp, 6] = halves * (CAP // 2)
            off_ref[layer * N_LOC + exp, 7] = jnp.maximum((halves + 1) // 2, 2)


def pick(layer, rank_ref, src, exp, toks=ALL):
    row = rank_ref[layer, src, pl.ds(exp, 1), toks]
    return (lax.broadcasted_iota(jnp.int32, (CAP, toks.size), 0) == row).astype(BF16)


def gate_column(layer, gate_ref, src, exp, toks=ALL):
    slab = gate_ref[layer, src, toks]
    lane = lax.broadcasted_iota(jnp.int32, slab.shape, 1)
    return jnp.sum(jnp.where(lane == exp, slab, 0.0), axis=1, keepdims=True)


def offset(off_ref, row, src):
    return pl.multiple_of(off_ref[row, src], 16)


def scatter_gated(layer, rank_ref, gate_ref, o_ref, src, toks):
    total = None
    for exp in range(N_LOC):
        term = gate_column(layer, gate_ref, src, exp, toks) * mm(pick(layer, rank_ref, src, exp, toks), o_ref[exp, src], TN)
        total = term if total is None else total + term
    return total.astype(BF16)


def scatter_plain(layer, rank_ref, g_refs, src, toks):
    sel = jnp.concatenate([pick(layer, rank_ref, src, exp, toks) for exp in range(N_LOC)], axis=0)
    per = N_LOC // len(g_refs)
    rows = [g_refs[exp // per][exp % per, src] for exp in range(N_LOC)]
    return mm(sel, jnp.concatenate(rows, axis=0), TN).astype(BF16)


def gather_rows(layer, rank_ref, pad_ref, src, block_ref, toks=ALL, gate_ref=None, more=False):
    @pl.loop(0, N_LOC)
    def _(exp):
        rows = block_ref[toks]
        if gate_ref is not None:
            rows = (gate_column(layer, gate_ref, src, exp, toks) * rows.astype(F32)).astype(BF16)
        picked = mm(pick(layer, rank_ref, src, exp, toks), rows)
        if more:
            picked = pad_ref[exp, src].astype(F32) + picked
        pad_ref[exp, src] = picked.astype(BF16)


def gather_others(spread, layer, rank_ref, pad_ref, every, gate_ref=None):
    for src in (1, 2):
        spread.arrived(src)
        gather_rows(layer, rank_ref, pad_ref, src, every.at[src], ALL, gate_ref)
    for k, toks in enumerate(SETS):
        spread.sets[k].arrived(3)
        gather_rows(layer, rank_ref, pad_ref, 3, every.at[3], toks, gate_ref, k == 1)


def packed(off_ref, row, pad_ref, exp, scr):
    for src in range(N_EP):
        scr[pl.ds(offset(off_ref, row, src), CAP), :] = pad_ref[exp, src]
    scr[pl.ds(offset(off_ref, row, 3) + CAP, CAP), :] = jnp.zeros((CAP, D), BF16)


def over_rows(off_ref, row, step):
    @pl.loop(0, off_ref[row, 4])
    def _(blk):
        step(pl.ds(pl.multiple_of(blk * CAP, CAP), CAP))

    @pl.when(off_ref[row, 5] == 1)
    def _():
        step(pl.ds(pl.multiple_of(off_ref[row, 4] * CAP, CAP), CAP // 2))


def tail_of(off_ref, row, size):
    return pl.ds(pl.multiple_of(off_ref[row, 6], CAP // 2), size)


def unpacked(off_ref, row, scr, out_ref, exp):
    for src in range(N_EP):
        out_ref[exp, src] = scr[pl.ds(offset(off_ref, row, src), CAP), :]


def forward_kernel(layer, off_ref, x_ref, wg_ref, wu_ref, wd_ref, out_ref, x_scr, o_scr):
    @pl.loop(0, N_LOC)
    def _(exp):
        row = layer * N_LOC + exp
        packed(off_ref, row, x_ref, exp, x_scr)

        def step(rows):
            x_blk = x_scr[rows, :]
            a_pre = mm(x_blk, wg_ref[exp], NT)
            b_pre = mm(x_blk, wu_ref[exp], NT)
            hidden = (jax.nn.silu(a_pre) * b_pre).astype(BF16)
            o_scr[rows, :] = mm(hidden, wd_ref[exp]).astype(BF16)

        over_rows(off_ref, row, step)
        o_scr[tail_of(off_ref, row, CAP), :] = jnp.zeros((CAP, D), BF16)
        unpacked(off_ref, row, o_scr, out_ref, exp)


def plain(kernel, name, ins, outs, scratch, grant, flops):
    return pl.pallas_call(
        kernel, out_shape=outs, in_specs=[SMEM] + [VMEM] * (len(ins) - 1), out_specs=jax.tree.map(lambda _: VMEM, outs),
        scratch_shapes=scratch, compiler_params=pltpu.CompilerParams(vmem_limit_bytes=grant * 1024 * 1024),
        cost_estimate=pl.CostEstimate(flops=flops, bytes_accessed=10_000_000, transcendentals=0), name=name)(*ins)


def expert_forward(layer, off, x_pad, weights):
    return plain(functools.partial(forward_kernel, layer), 'expert_forward', (off, x_pad) + weights, block(N_LOC, N_EP, CAP, D),
                 [pltpu.VMEM((SLOTS, D), BF16)] * 2, 8, 10_000_000_000)


def backward_kernel(layer, first, count, done, off_ref, x_ref, d_ref, wg_ref, wu_ref, wd_ref, out_ref, *refs):
    grad_ref = refs[0] if done else None
    left, right, gx_scr = refs[-3:]

    @pl.loop(first, first + count)
    def _(exp):
        row = layer * N_LOC + exp
        slot = jnp.maximum(exp - first - done, 0)
        x_scr, d_scr = left.at[slot, 0], left.at[slot, 1]
        packed(off_ref, row, x_ref, exp, x_scr)
        packed(off_ref, row, d_ref, exp, d_scr)

        def step(rows):
            x_blk = x_scr[rows, :]
            a_pre = mm(x_blk, wg_ref[exp], NT)
            grad_h = mm(d_scr[rows, :], wd_ref[exp], NT).astype(BF16).astype(F32)
            sigma = jax.nn.sigmoid(a_pre)
            swish = a_pre * sigma
            grad_b = (grad_h * swish).astype(BF16)
            right[slot, 1, rows, :] = grad_b
            slope = grad_h * (sigma + swish * (1.0 - sigma))
            b_pre = mm(x_blk, wu_ref[exp], NT)
            right[slot, 2, rows, :] = (swish * b_pre).astype(BF16)
            grad_a = (slope * b_pre).astype(BF16)
            right[slot, 0, rows, :] = grad_a
            gx_scr[rows, :] = (mm(grad_a, wg_ref[exp]) + mm(grad_b, wu_ref[exp])).astype(BF16)

        over_rows(off_ref, row, step)
        gx_scr[tail_of(off_ref, row, CAP), :] = jnp.zeros((CAP, D), BF16)
        unpacked(off_ref, row, gx_scr, out_ref, exp - first)
        depth, half = off_ref[row, 7], CAP // 2
        made_here = exp < first + done

        @pl.loop(off_ref[row, 4] * 2 + off_ref[row, 5], jnp.where(made_here, depth * 2, N_EP * 2))
        def _(k):
            rows = pl.ds(pl.multiple_of(k * half, half), half)
            right[slot, :, rows, :] = jnp.zeros((3, half, FF), BF16)
            left[slot, :, rows, :] = jnp.zeros((2, half, D), BF16)

        if done:
            for blocks in range(2, 5):
                pl.when(jnp.logical_and(made_here, depth == blocks))(
                    functools.partial(weight_grads, left, right, slot, grad_ref, exp - first, blocks * CAP))


def weight_grads(left, right, slot, grad_ref, exp, depth):
    @pl.loop(0, 3)
    def _(mat):
        grad = mm(left[slot, mat // 2, 0:depth, :], right[slot, mat, 0:depth, :], TN).astype(BF16)
        for owner in range(4):
            grad_ref[exp, mat, owner // 2, owner % 2] = grad[ROWS_DP * owner:ROWS_DP * owner + ROWS_DP]


def grads_shape(count):
    return (count, 3, 2, 2, ROWS_DP, FF)


def expert_backward(layer, first, count, done, off, x_pad, d_pad, weights):
    slots = max(count - done, 1)
    factors = ((slots, 2, SLOTS, D), (slots, 3, N_EP * CAP, FF))
    outs = (block(count, N_EP, CAP, D),) + ((block(*grads_shape(done)),) if done else ())
    scratch = [pltpu.VMEM((SLOTS, D), BF16)]
    if count > done:
        outs += tuple(block(*shape) for shape in factors)
    else:
        scratch = [pltpu.VMEM(shape, BF16) for shape in factors] + scratch
    return plain(functools.partial(backward_kernel, layer, first, count, done), 'expert_backward',
                 (off, x_pad, d_pad) + weights, outs, scratch, 12 if count == done else 6, 9_000_000_000 * count)


def remote(src, dst, sems, slot, target):
    send, recv = sems
    return pltpu.make_async_remote_copy(src_ref=src, dst_ref=dst, send_sem=send.at[slot], recv_sem=recv.at[slot],
                                        device_id=target, device_id_type=pl.DeviceIdType.MESH)


class Place:
    def __init__(self):
        ep, dp = lax.axis_index('ep'), lax.axis_index('dp')
        self.me = ep
        self.z, self.y = ep // 2, ep % 2
        self.x, self.c = dp // 2, dp % 2
        self.to_y, self.to_z = {'ep': self.z * 2 + 1 - self.y}, {'ep': (1 - self.z) * 2 + self.y}
        self.to_d = {'ep': (1 - self.z) * 2 + 1 - self.y}
        self.to_c, self.to_x = {'dp': self.x * 2 + 1 - self.c}, {'dp': (1 - self.x) * 2 + self.c}


def greet(targets):
    barrier = pltpu.get_barrier_semaphore()
    for target in targets:
        pl.semaphore_signal(barrier, inc=1, device_id=target, device_id_type=pl.DeviceIdType.MESH)
    return functools.partial(pl.semaphore_wait, barrier, len(targets))


class Spread:
    def __init__(self, at, own, every, sems, k):
        top, low = pl.ds(HALF * k, QUARTER), pl.ds(HALF * k + QUARTER, QUARTER)
        first = 6 * k
        self.direct = [remote(own.at[top], every.at[1, top], sems, first, at.to_y),
                       remote(own.at[low], every.at[2, low], sems, first + 1, at.to_z),
                       remote(own.at[low], every.at[1, low], sems, first + 2, at.to_y),
                       remote(own.at[top], every.at[2, top], sems, first + 3, at.to_z)]
        self.onward = [remote(every.at[1, top], every.at[3, top], sems, first + 4, at.to_z),
                       remote(every.at[2, low], every.at[3, low], sems, first + 5, at.to_y)]

    def start(self):
        for copy in self.direct:
            copy.start()

    def forward(self):
        for first, then in zip(self.direct, self.onward):
            first.wait_recv()
            then.start()

    def arrived(self, slot):
        for copy in ((), self.direct[2:3], self.direct[3:4], self.onward)[slot]:
            copy.wait_recv()

    def finish(self):
        for copy in self.direct + self.onward:
            copy.wait_send()


class Both:
    def __init__(self, first, second):
        self.sets = (first, second)

    def __getattr__(self, name):
        def each(*args):
            for one in self.sets:
                getattr(one, name)(*args)
        return each


class Collect:
    def __init__(self, at, part, got, mix_scr, sems, k):
        self.part, self.got, self.mix_scr, self.k = part, got, mix_scr, k
        self.top, self.low = pl.ds(HALF * k, QUARTER), pl.ds(HALF * k + QUARTER, QUARTER)
        self.first = first = 6 * k
        self.direct = [remote(part.at[3, self.top], got.at[first], sems, first, at.to_y),
                       remote(part.at[3, self.low], got.at[first + 1], sems, first + 1, at.to_z),
                       remote(part.at[1, self.top], got.at[first + 2], sems, first + 2, at.to_y),
                       remote(part.at[2, self.low], got.at[first + 3], sems, first + 3, at.to_z)]
        self.summed = [remote(mix_scr.at[2 * k], got.at[first + 4], sems, first + 4, at.to_z),
                       remote(mix_scr.at[2 * k + 1], got.at[first + 5], sems, first + 5, at.to_y)]

    def far(self):
        self.direct[0].start()
        self.direct[1].start()

    def near_y(self):
        self.direct[2].start()

    def near_z(self):
        self.direct[3].start()

    def forward(self):
        for step, (slot, rows) in enumerate(((2, self.top), (1, self.low))):
            self.direct[step].wait_recv()
            self.mix_scr[2 * self.k + step] = (self.part[slot, rows].astype(F32) + self.got[self.first + step].astype(F32)).astype(BF16)
            self.summed[step].start()

    def finish(self, base):
        for copy in self.direct[2:] + self.summed:
            copy.wait_recv()
        got, first = self.got, self.first
        top = self.part[0, self.top].astype(F32) + got[first + 2].astype(F32) + got[first + 4].astype(F32)
        low = self.part[0, self.low].astype(F32) + got[first + 3].astype(F32) + got[first + 5].astype(F32)
        return (base[SETS[self.k]].astype(F32) + jnp.concatenate([top, low], axis=0)).astype(BF16)

    def summed_gone(self):
        for copy in self.summed:
            copy.wait_send()

    def drain(self):
        for copy in self.direct:
            copy.wait_send()


def start_collect(at, part, got, mix_scr, sems, slot_sum, await_peers):
    both = Both(*[Collect(at, part, got, mix_scr, sems, k) for k in range(2)])
    for k, toks in enumerate(SETS):
        part[3, toks] = slot_sum(3, toks)
        if k == 0:
            await_peers()
        both.sets[k].far()
    sum_slot(part, 1, slot_sum)
    both.near_y()
    sum_slot(part, 2, slot_sum)
    both.near_z()
    return both


def sum_slot(part, slot, slot_sum):
    @pl.loop(0, 2)
    def _(k):
        toks = pl.ds(pl.multiple_of(k * HALF, HALF), HALF)
        part[slot, toks] = slot_sum(slot, toks)


def spread_of(at, own, every, sems):
    return Both(*[Spread(at, own, every, sems, k) for k in range(2)])


class Halve:
    def __init__(self, at, grads, got, sems):
        self.at, self.grads, self.got = at, grads, got
        self.pair = [remote(grads[k // 3].at[k % 3, :, 1 - at.c], got.at[k], sems, k, at.to_c) for k in range(6)]

    def start(self, exp):
        for copy in self.pair[3 * exp:3 * exp + 3]:
            copy.start()

    def wait(self, exp):
        for copy in self.pair[3 * exp:3 * exp + 3]:
            copy.wait_recv()

    def total(self, exp, side):
        return jnp.concatenate([self.grads[exp][mat, side, self.at.c].astype(F32) + self.got[3 * exp + mat, side].astype(F32)
                                for mat in range(3)], axis=1).astype(BF16)

    def drain(self):
        for copy in self.pair:
            copy.wait_send()


def store_expert(outs, exp, keep, got):
    total = (keep.astype(F32) + got.astype(F32)).astype(BF16)
    for mat, out in enumerate(outs):
        out[exp] = total[:, FF * mat:FF * mat + FF]


class Across:
    def __init__(self, at, halve, keep, send, got, sems):
        self.at, self.halve, self.keep, self.send, self.got = at, halve, keep, send, got
        self.along = [remote(send.at[exp], got.at[exp], sems, exp, at.to_x) for exp in range(2)]

    def forward(self, exp):
        self.halve.wait(exp)
        self.send[exp] = self.halve.total(exp, 1 - self.at.x)
        self.along[exp].start()
        self.keep[exp] = self.halve.total(exp, self.at.x)

    def finish(self, outs, first):
        for exp in range(2):
            self.along[exp].wait_recv()
            store_expert(outs, first + exp, self.keep[exp], self.got[exp])
        for copy in self.along:
            copy.wait_send()


def leave_totals(at, halve, keep, send):
    for exp in range(2):
        halve.wait(exp)
        send[exp] = halve.total(exp, 1 - at.x)
        keep[exp] = halve.total(exp, at.x)


def sems(count):
    return [pltpu.SemaphoreType.DMA((count,))] * 2


PACKED = (2, ROWS_DP, 3 * FF)
COLLECT_SCRATCH = [pltpu.VMEM((N_EP, TOK, D), BF16), pltpu.VMEM((12, QUARTER, D), BF16), pltpu.VMEM((4, QUARTER, D), BF16)] + sems(12)
HALVE_SCRATCH = [pltpu.VMEM((6, 2, ROWS_DP, FF), BF16)] + sems(6)
ACROSS_SCRATCH = [pltpu.VMEM(PACKED, BF16)] * 3 + sems(2)


ANY = pl.BlockSpec(memory_space=pl.ANY)


def call(kernel, name, ident, ins, outs, scratch, grant):
    return pl.pallas_call(
        kernel, out_shape=outs, scratch_shapes=scratch,
        in_specs=[SMEM if value.shape == (8, 8) else VMEM for value in ins],
        out_specs=jax.tree.map(lambda o: SMEM if o.shape == (8, 8) else VMEM, outs),
        compiler_params=pltpu.CompilerParams(collective_id=ident, has_side_effects=True, vmem_limit_bytes=grant * 1024 * 1024),
        cost_estimate=pl.CostEstimate(flops=10_000_000_000, bytes_accessed=4_000_000, transcendentals=0), name=name)(*ins)


def entry_kernel(own, pack_ref, x_pad, rank_ref, gate_ref, off_ref, packs, every, s_send, s_recv, p_send, p_recv):
    at = Place()
    greet([at.to_y, at.to_z])()
    small = [remote(pack_ref, packs.at[1], (p_send, p_recv), 0, at.to_y),
             remote(pack_ref, packs.at[2], (p_send, p_recv), 1, at.to_z),
             remote(packs.at[1], packs.at[3], (p_send, p_recv), 2, at.to_z)]
    small[0].start()
    small[1].start()
    spread = spread_of(at, own, every, (s_send, s_recv))
    spread.start()
    packs[0] = pack_ref[...]
    small[0].wait_recv()
    small[2].start()
    small[1].wait_recv()
    small[2].wait_recv()
    route_into(packs, rank_ref, gate_ref, off_ref, at.me)
    spread.forward()
    gather_rows(0, rank_ref, x_pad, 0, own)
    gather_others(spread, 0, rank_ref, x_pad, every)
    spread.finish()
    for copy in small:
        copy.wait_send()


def middle_kernel(o_ref, u_ref, dense_ref, rank_ref, gate_ref, dy_own, dy_y, dy_z, mid_ref, x_pad, d_pad,
                  part, got, mix_scr, c_send, c_recv, u_scr, every, s_send, s_recv, dy_d, d_send, d_recv):
    at = Place()
    await_peers = greet([at.to_y, at.to_z])
    onward = [remote(dy_y.at[SETS[0]], dy_d.at[SETS[0]], (d_send, d_recv), 0, at.to_z),
              remote(dy_z.at[SETS[1]], dy_d.at[SETS[1]], (d_send, d_recv), 1, at.to_y)]

    def begin():
        await_peers()
        for copy in onward:
            copy.start()

    def slot_sum(src, toks):
        return scatter_gated(0, rank_ref, gate_ref, o_ref, src, toks)

    collect = start_collect(at, part, got, mix_scr, (c_send, c_recv), slot_sum, begin)
    gather_rows(1, rank_ref, d_pad, 0, dy_own, ALL, gate_ref)
    collect.forward()
    sum_slot(part, 0, slot_sum)
    gather_rows(1, rank_ref, d_pad, 1, dy_y, ALL, gate_ref)
    spread = spread_of(at, u_scr, every, (s_send, s_recv))
    for k, rows in enumerate(SETS):
        mid = collect.sets[k].finish(u_ref)
        u_scr[rows] = (mid.astype(F32) + mm(mid, dense_ref[...])).astype(BF16)
        spread.sets[k].start()
        mid_ref[rows] = mid
    gather_rows(1, rank_ref, x_pad, 0, u_scr)
    gather_rows(1, rank_ref, d_pad, 2, dy_z, ALL, gate_ref)
    spread.forward()
    for copy in onward:
        copy.wait_recv()
    gather_rows(1, rank_ref, d_pad, 3, dy_d, ALL, gate_ref)
    collect.summed_gone()
    collect.drain()
    for copy in onward:
        copy.wait_send()
    gather_others(spread, 1, rank_ref, x_pad, every)
    spread.finish()


def dense_grad(x_ref, halves):
    return mm(x_ref[SETS[0]], halves[0], TN) + mm(x_ref[SETS[1]], halves[1], TN)


def write_slabs(slabs, value):
    for k in range(16):
        slabs[k // 8, k // 4 % 2, k // 2 % 2, k % 2] = value[24 * k:24 * k + 24].astype(BF16)


class DenseReduce:
    def __init__(self, at, slabs, got_c, sum_c, got_p, sum_p, got_x, sems):
        self.at, self.slabs, self.got_c, self.sum_c, self.got_p, self.sum_p, self.got_x = at, slabs, got_c, sum_c, got_p, sum_p, got_x
        self.pair = remote(slabs.at[:, 1 - at.c], got_c, sems, 0, at.to_c)
        self.plane = [remote(sum_c.at[:, z, y], got_p.at[k], sems, 1 + k, to) for k, (z, y, to) in enumerate((
            (at.z, 1 - at.y, at.to_y), (1 - at.z, at.y, at.to_z), (1 - at.z, 1 - at.y, at.to_d)))]
        self.along = remote(sum_p.at[1 - at.x], got_x, sems, 4, at.to_x)

    def start(self):
        self.pair.start()

    def to_plane(self):
        self.pair.wait_recv()
        for side in range(2):
            self.sum_c[side] = (self.slabs[side, self.at.c].astype(F32) + self.got_c[side].astype(F32)).astype(BF16)
        for copy in self.plane:
            copy.start()

    def to_x(self):
        for copy in self.plane:
            copy.wait_recv()
        for side in range(2):
            total = self.sum_c[side, self.at.z, self.at.y].astype(F32)
            for k in range(3):
                total = total + self.got_p[k, side].astype(F32)
            self.sum_p[side] = total.astype(BF16)
        self.along.start()

    def finish(self, out):
        self.along.wait_recv()
        out[...] = (self.sum_p[self.at.x].astype(F32) + self.got_x[...].astype(F32)).astype(BF16)
        for copy in [self.pair, self.along] + self.plane:
            copy.wait_send()


def dense_scratch():
    slab = lambda *lead: pltpu.VMEM(lead + (24, D), BF16)
    return [slab(2, 2, 2), slab(2, 2, 2), slab(3, 2), slab(2), slab()] + sems(5)


def turn_kernel(gx_ref, dy_ref, dense_ref, mid_ref, rank_ref, gate_ref, grads, left, right,
                grad_ref, d_pad, slabs, oa, ob, oc, later_keep, later_send,
                part, got, mix_scr, c_send, c_recv, s_send, s_recv, got_a, a_send, a_recv, got_b, b_send, b_recv,
                keep, send, got_x, x_send, x_recv, g_scr, every, later_grads):
    at = Place()
    await_peers = greet([at.to_y, at.to_z, at.to_c, at.to_x])
    now = Halve(at, (grads.at[0], grads.at[1]), got_a, (a_send, a_recv))
    later = Halve(at, (later_grads.at[0], later_grads.at[1]), got_b, (b_send, b_recv))

    def begin():
        await_peers()
        now.start(0)
        now.start(1)

    def slot_sum(src, toks):
        return scatter_plain(1, rank_ref, (gx_ref,), src, toks)

    collect = start_collect(at, part, got, mix_scr, (c_send, c_recv), slot_sum, begin)
    across = Across(at, now, keep, send, got_x, (x_send, x_recv))
    across.forward(0)
    collect.forward()
    across.forward(1)
    sum_slot(part, 0, slot_sum)
    for exp in range(2):
        weight_grads(left, right, exp, later_grads, exp, N_EP * CAP)
        later.start(exp)
    spread = spread_of(at, g_scr, every, (s_send, s_recv))
    halves = []
    for k, rows in enumerate(SETS):
        halves.append(collect.sets[k].finish(dy_ref))
        g_scr[rows] = (halves[k].astype(F32) + mm(halves[k], dense_ref[...], NT)).astype(BF16)
        spread.sets[k].start()
        grad_ref[rows] = g_scr[rows]
    gather_rows(0, rank_ref, d_pad, 0, g_scr, ALL, gate_ref)
    write_slabs(slabs, dense_grad(mid_ref, halves))
    spread.forward()
    leave_totals(at, later, later_keep, later_send)
    collect.summed_gone()
    collect.drain()
    now.drain()
    later.drain()
    across.finish((oa, ob, oc), 0)
    gather_others(spread, 0, rank_ref, d_pad, every, gate_ref)
    spread.finish()


def pair_kernel(grads, later_keep, later_send, got_b, b_send, b_recv):
    at = Place()
    greet([at.to_c])()
    later = Halve(at, (grads.at[0], grads.at[1]), got_b, (b_send, b_recv))
    later.start(0)
    later.start(1)
    leave_totals(at, later, later_keep, later_send)
    later.drain()


def exit_kernel(gx_a, gx_b, dy_ref, dense_ref, tok_ref, slabs_two, rank_ref, grads, left, right, two_keep, two_got, da, db, dc,
                dx_ref, dense_one, dense_two, oa, ob, oc, ta, tb, tc,
                part, got, mix_scr, c_send, c_recv, got_a, a_send, a_recv, keep, send, got_x, x_send, x_recv, slabs_one, last_grads, *dense):
    at = Place()
    await_peers = greet([at.to_y, at.to_z, at.to_d, at.to_c, at.to_x])
    now = Halve(at, (grads.at[0], last_grads.at[0]), got_a, (a_send, a_recv))
    half = len(dense) // 2
    first, second = [DenseReduce(at, slabs, *dense[k * half:k * half + 5], dense[k * half + 5:k * half + 7])
                     for k, slabs in enumerate((slabs_one, slabs_two))]

    def begin():
        await_peers()
        now.start(0)
        second.start()

    def slot_sum(src, toks):
        return scatter_plain(0, rank_ref, (gx_a, gx_b), src, toks)

    collect = start_collect(at, part, got, mix_scr, (c_send, c_recv), slot_sum, begin)
    across = Across(at, now, keep, send, got_x, (x_send, x_recv))
    across.forward(0)
    weight_grads(left, right, 0, last_grads, 0, N_EP * CAP)
    now.start(1)
    collect.forward()
    second.to_plane()
    across.forward(1)
    sum_slot(part, 0, slot_sum)
    for exp in range(2):
        store_expert((ta, tb, tc), 2 + exp, two_keep[exp], two_got[exp])
    for out, done in ((ta, da), (tb, db), (tc, dc)):
        out[0:2] = done[...]
    halves = [one.finish(dy_ref) for one in collect.sets]
    write_slabs(slabs_one, dense_grad(tok_ref, halves))
    first.start()
    second.to_x()
    for rows, half_rows in zip(SETS, halves):
        dx_ref[rows] = (half_rows.astype(F32) + mm(half_rows, dense_ref[...], NT)).astype(BF16)
    first.to_plane()
    collect.summed_gone()
    collect.drain()
    now.drain()
    first.to_x()
    across.finish((oa, ob, oc), 0)
    second.finish(dense_two)
    first.finish(dense_one)


def store_kernel(count, keep, got, *refs):
    values, outs, made, sem = refs[:count], refs[count:2 * count], refs[-2], refs[-1]
    copies = [pltpu.make_async_copy(values[k], outs[k] if k < count - 3 else outs[k].at[2:4], sem.at[k]) for k in range(count)]
    for copy in copies:
        copy.start()
    for exp in range(2):
        store_expert([made.at[mat] for mat in range(3)], exp, keep[exp], got[exp])
    for mat in range(3):
        copies.append(pltpu.make_async_copy(made.at[mat], outs[count - 3 + mat].at[0:2], sem.at[count + mat]))
        copies[-1].start()
    for copy in copies:
        copy.wait()


def store_all(keep, got, values):
    count = len(values)
    outs = [block(*value.shape) for value in values[:-3]] + [block(N_LOC, ROWS_DP, FF)] * 3
    return pl.pallas_call(
        functools.partial(store_kernel, count),
        out_shape=outs, in_specs=[VMEM] * (2 + count), out_specs=[ANY] * count,
        scratch_shapes=[pltpu.VMEM((3, 2, ROWS_DP, FF), BF16), pltpu.SemaphoreType.DMA((count + 3,))],
        compiler_params=pltpu.CompilerParams(vmem_limit_bytes=4 * 1024 * 1024),
        cost_estimate=pl.CostEstimate(flops=1_000_000_000, bytes_accessed=4_000_000, transcendentals=0), name='store')(keep, got, *values)


def stored(w_gate, w_up, w_down):
    return jnp.swapaxes(w_gate, 1, 2), jnp.swapaxes(w_up, 1, 2), w_down


def along_x(sent):
    return lax.ppermute(sent, 'dp', [(0, 2), (2, 0), (1, 3), (3, 1)])


def solution(mesh):
    tok_spec = P(('dp', 'ep'), None)
    exp_spec = P('ep', None, None)
    layer_specs = (P(None, None), tok_spec, tok_spec, exp_spec, exp_spec, exp_spec)
    grad_specs = (P(('dp', 'ep'), None), P('ep', 'dp', None), P('ep', 'dp', None), P('ep', None, 'dp'))

    def local_step(tokens, dy_out, dense_w1, route_idx1, route_gate1, w_gate1, w_up1, w_down1, dense_w2, route_idx2, route_gate2, w_gate2, w_up2, w_down2):
        weights_one, weights_two = stored(w_gate1, w_up1, w_down1), stored(w_gate2, w_up2, w_down2)
        tok_block, all_block = block(TOK, D), block(N_EP, TOK, D)
        padded = block(N_LOC, N_EP, CAP, D)
        every = pltpu.VMEM((N_EP, TOK, D), BF16)
        own = pltpu.VMEM((TOK, D), BF16)
        place = lambda part, k: jnp.pad(part, ((0, 0), (4 * k, 12 - 4 * k)))
        pack = ((place(route_idx1, 0) + place(route_idx2, 1)).astype(F32) + (place(route_gate1, 2) + place(route_gate2, 3))).T
        mixed_one = (tokens.astype(F32) + jnp.dot(tokens, dense_w1, preferred_element_type=F32)).astype(BF16)
        x_one, rank, gate, off = call(
            entry_kernel, 'entry', 0, (mixed_one, pack),
            (padded, block(2, N_EP, 8, TOK, dtype=jnp.int32), block(2, N_EP, TOK, 8, dtype=F32), block(8, 8, dtype=jnp.int32)),
            [pltpu.VMEM((N_EP, 16, TOK), F32), every] + sems(12) + sems(3), 12)
        dy_later, x_one = lax.optimization_barrier((dy_out, x_one))
        dy_all = (dy_out,) + tuple(lax.ppermute(dy_later, 'ep', [(k, k ^ flip) for k in range(N_EP)]) for flip in (1, 2))
        outs = expert_forward(0, off, x_one, weights_one)
        mid_tok, x_two, d_two = call(middle_kernel, 'middle', 1, (outs, mixed_one, dense_w2, rank, gate) + dy_all,
                                     (tok_block, padded, padded), COLLECT_SCRATCH + [own, every] + sems(12) + [own] + sems(2), 9)
        gx, grads, left, right = expert_backward(1, 0, 4, 2, off, x_two, d_two, weights_two)
        grad_mid, d_one, slabs, *done_two, keep_two, send_two = call(
            turn_kernel, 'turn', 2, (gx, dy_out, dense_w2, mid_tok, rank, gate, grads, left, right),
            (tok_block, padded, block(2, 2, 2, 2, 24, D)) + (block(2, ROWS_DP, FF),) * 3 + (block(*PACKED),) * 2,
            COLLECT_SCRATCH + sems(12) + HALVE_SCRATCH * 2 + ACROSS_SCRATCH + [own, every, pltpu.VMEM(grads_shape(2), BF16)], 17)
        got_two = along_x(send_two)
        gx_a, grads = expert_backward(0, 0, 2, 2, off, x_one, d_one, weights_one)
        keep_one, send_one = call(pair_kernel, 'pair', 4, (grads,), (block(*PACKED),) * 2, HALVE_SCRATCH, 6)
        got_two, d_one = lax.optimization_barrier((got_two, d_one))
        got_one = along_x(send_one)
        gx_b, grads, left, right = expert_backward(0, 2, 2, 1, off, x_one, d_one, weights_one)
        grad_tok, dense_one, dense_two, *reduced = call(
            exit_kernel, 'exit', 3, (gx_a, gx_b, grad_mid, dense_w1, tokens, slabs, rank, grads, left, right, keep_two, got_two) + tuple(done_two),
            (tok_block, block(24, D), block(24, D)) + (block(2, ROWS_DP, FF),) * 3 + (block(N_LOC, ROWS_DP, FF),) * 3,
            COLLECT_SCRATCH + HALVE_SCRATCH + ACROSS_SCRATCH + [pltpu.VMEM((2, 2, 2, 2, 24, D), BF16), pltpu.VMEM(grads_shape(1), BF16)] + dense_scratch() * 2, 15)
        grad_tok, dense_one, dense_two, *reduced = store_all(keep_one, got_one, (grad_tok, dense_one, dense_two) + tuple(reduced[3:]) + tuple(reduced[:3]))

        def shaped(gate_up_down):
            return gate_up_down[0], gate_up_down[1], jnp.swapaxes(gate_up_down[2], 1, 2)

        return (grad_tok, dense_one) + shaped(reduced[3:]) + (dense_two,) + shaped(reduced[:3])

    return jax.shard_map(local_step, mesh=mesh, in_specs=(tok_spec, tok_spec) + layer_specs + layer_specs,
                         out_specs=(tok_spec,) + grad_specs + grad_specs, check_vma=False)
```
